256 devices in a mesh: seq: 32 (over x, z), head: 8 (over y, core).
Axes of the slice: x: 4, y: 4, z: 8, core: 2. Of those that a mesh axis runs over, the one named last changes fastest.
Arguments:
- queries: bfloat16 [32768, 4096], P('seq', 'head'), may hold values from -150 to 150
- keys: bfloat16 [32768, 4096], P('seq', 'head'), may hold values from -7 to 7
- values: bfloat16 [32768, 4096], P('seq', 'head'), may hold values from -6 to 6
- random_holder: int32 [32, 256, 3], P('head', 'seq'), may hold values from 0 to 31, all different within a row; in each aligned block of 8 rows (0 to 7, 8 to 15, ..., all dimensions but the last counted through in order) at most 2 rows name the same one
- random_offset: int32 [32, 256, 3], P('head', 'seq'), may hold values from 0 to 7
- keep: int32 [256], P('seq'), may hold values from 0 to 1, as said below
Outputs:
- packed: bfloat16 [32768, 4096], P('seq', 'head')
The draws below stay inside these ranges and needn't reach their ends.
Inputs may be any that keep to these rules, and one draw needn't show every extreme that they name: `random_holder`: for each head, the 8 query blocks of one index of seq name no index of seq more than 2 times over all their random entries; the 3 entries of one query block and head differ. `keep`: block j is kept where j % 8 == 0 or j % 8 == 7, and not kept where j % 8 == 1.
All inputs are finite; a program needn't handle non-finite values.
Results may differ from the reference program's by a relative error of at most 0.007.
Values may be sent and summed in bfloat16 or wider, within the bound.
A program may use at most 128 MiB of HBM per device.

```python
import math
import jax
import jax.numpy as jnp
import numpy as np
from jax import lax

H = 32
DH = 128
B = 128
G = 2
R = 3
BD = 8
NB = 256
L = 32768
MOST = 2
N_SEQ = 32


def paired_rows(key):
    base = jax.random.fold_in(key, 71)
    key_rows = jnp.clip(jax.random.normal(jax.random.fold_in(base, 1), (L, H * DH), jnp.float32), -6.0, 6.0)
    query_rows = jnp.clip(jax.random.normal(jax.random.fold_in(base, 2), (L, H * DH), jnp.float32), -6.0, 6.0)
    return (query_rows, key_rows)


def draw_queries(key, part):
    query_rows, key_rows = paired_rows(key)
    return query_rows.astype(jnp.bfloat16)


def draw_keys(key, part):
    query_rows, key_rows = paired_rows(key)
    return key_rows.astype(jnp.bfloat16)


def draw_keep(key, part):
    count = L // B
    rolled = jax.random.randint(jax.random.fold_in(key, 113), (count,), 0, 3)
    kept = (rolled == 0).astype(jnp.int32)
    position = jnp.arange(count, dtype=jnp.int32) % BD
    kept = jnp.where(position == 0, 1, kept)
    kept = jnp.where(position == BD - 1, 1, kept)
    kept = jnp.where(position == 1, 0, kept)
    return kept.astype(jnp.int32)


def plant(array, key, smallest, largest):
    extent = array.shape
    spot = [jax.random.randint(jax.random.fold_in(key, axis), (), 0, extent[axis]) for axis in range(len(extent))]
    array = array.at[tuple(spot)].set(smallest)
    longest = extent.index(max(extent))
    spot[longest] = (spot[longest] + 1) % extent[longest]
    return array.at[tuple(spot)].set(largest)


def levels(rng, shape, split, low, high):
    gain = 1.0
    for dim, shards_of in split:
        heights = jax.random.uniform(jax.random.fold_in(jax.random.fold_in(rng, 6), dim), (shards_of,), jnp.float32, low / len(split), high / len(split))
        gain = gain * jnp.repeat(jnp.exp(heights), shape[dim] // shards_of).reshape((-1,) + (1,) * (len(shape) - 1 - dim))
    return gain


def shared_out(rng, own, number, rows, number_of, top, limit, slope):
    sequence = jax.random.permutation(rng, number_of)
    heavy_load, usual = shares(number_of, rows * top, limit, slope, True), shares(number_of, rows * top, limit, slope, False)
    places = jnp.arange(number_of)

    def named(sizes, offset_by):
        used = int((sizes > 0).sum())
        fixed = max(1, used // 4)
        shifted = fixed + (places - fixed + offset_by * (used - fixed)) % max(1, number_of - fixed)
        return jnp.zeros((number_of,), jnp.int32).at[sequence[jnp.where(places < fixed, places, shifted)]].set(jnp.asarray(sizes, jnp.int32))

    sizes = jnp.where(number % 4 == 0, named(heavy_load, number // 4), named(usual, number - number // 4 - 1))
    mixed = jax.random.permutation(jax.random.fold_in(own, 3), number_of)
    source_of, sink = mixed[0:number_of // 2 * 2:2], mixed[1:number_of // 2 * 2:2]
    slack = jnp.minimum(sizes[source_of] - 1, limit - sizes[sink]) // 2
    slack = jnp.where((source_of == sequence[0]) | (sink == sequence[0]) | (sizes[sink] == 0), 0, jnp.maximum(slack, 0))
    shifted = jax.random.randint(jax.random.fold_in(own, 4), (number_of // 2,), 0, 1 << 20) % (slack + 1)
    sizes = sizes.at[source_of].add(-shifted).at[sink].add(shifted)
    labels = jnp.searchsorted(jnp.cumsum(sizes), jnp.arange(rows * top), side="right").astype(jnp.int32)
    table = labels.reshape(top, rows).T
    table = table[jax.random.permutation(jax.random.fold_in(own, 1), rows)]
    offset_by = jax.random.randint(jax.random.fold_in(own, 2), (rows, 1), 0, top)
    return jnp.take_along_axis(table, (jnp.arange(top)[None, :] + offset_by) % top, axis=1)


def shares(amount, total, limit, skew, full):
    weights = [(1 << 20) // math.isqrt(standing ** skew) + 1 for standing in range(1, amount + 1)]
    largest = limit if full else min(limit, max(-(-total // amount), total * weights[0] // sum(weights)))
    least = 1 if total - largest >= amount - 1 else 0
    counts, spare = [largest] + [least] * (amount - 1), total - largest - least * (amount - 1)
    while spare > 0:
        movable = [i for i in range(1, amount) if counts[i] < largest] or [i for i in range(1, amount) if counts[i] < limit]
        whole, left = sum([weights[i] for i in movable]), spare
        for i in movable:
            more = min(limit - counts[i], max(1, left * weights[i] // whole), spare)
            counts[i] = counts[i] + more
            spare = spare - more
    return np.array(counts)


def bell_draw(rng, dims, deviation, bound, split=(), kind=jnp.bfloat16):
    drawn = jax.random.normal(rng, dims, jnp.float32) * deviation
    if len(split) > 0:
        drawn = levels(rng, dims, split, -0.22, 0.18) * drawn
    return jnp.clip(drawn, min=-bound, max=bound).astype(kind)


def setup_inputs(seed: int = 0) -> dict:
    key_of = jax.random.split(jax.random.key(seed), 7)
    queries = draw_queries(jax.random.fold_in(key_of[6], 71), 0)
    keys = draw_keys(jax.random.fold_in(key_of[6], 71), 0)
    values = bell_draw(key_of[2], (L, H * DH), 1.0, 6.0, ((0, 32), (1, 8)))
    random_holder_keys = jax.random.split(jax.random.fold_in(key_of[3], 1), H * NB // BD)
    random_holder_turns = jax.random.permutation(jax.random.fold_in(key_of[3], 3), H * NB // BD)
    random_holder = jax.vmap(lambda own, number: shared_out(jax.random.fold_in(key_of[3], 2), own, number, BD, N_SEQ, R, MOST, 2))(random_holder_keys, random_holder_turns).reshape((H, NB, R))
    random_offset = plant(jax.random.randint(key_of[4], (H, NB, R), 0, BD), jax.random.fold_in(key_of[4], 1), 0, BD - 1).astype(jnp.int32)
    keep = draw_keep(jax.random.fold_in(key_of[6], 71), 0)
    return {"queries": queries, "keys": keys, "values": values, "random_holder": random_holder, "random_offset": random_offset, "keep": keep}


neg_big = -1.0e30


def reference(queries, keys, values, random_holder, random_offset, keep):
    score_scale = 1.0 / (DH ** 0.5)
    query_blocks = queries.reshape(NB, B, H, DH)
    key_blocks = keys.reshape(NB, B, H, DH)
    value_blocks = values.reshape(NB, B, H, DH)
    head_idx = jnp.arange(H, dtype=jnp.int32)[:, None]

    def one_block(block_idx):
        left = jnp.maximum(block_idx - 1, 0)
        right = jnp.minimum(block_idx + 1, NB - 1)
        common = jnp.concatenate((jnp.stack((left, block_idx, right)).astype(jnp.int32), jnp.arange(G, dtype=jnp.int32)))
        common_keys = jnp.transpose(key_blocks[common], (0, 2, 1, 3))
        common_values = jnp.transpose(value_blocks[common], (0, 2, 1, 3))
        chosen = (random_holder[:, block_idx] * BD + random_offset[:, block_idx]).astype(jnp.int32)
        rand_keys = jnp.transpose(key_blocks[chosen, :, head_idx, :], (1, 0, 2, 3))
        rand_values = jnp.transpose(value_blocks[chosen, :, head_idx, :], (1, 0, 2, 3))
        tile_keys = jnp.concatenate((common_keys, rand_keys), axis=0).astype(jnp.float32)
        tile_values = jnp.concatenate((common_values, rand_values), axis=0).astype(jnp.float32)
        live = jnp.concatenate((jnp.stack((block_idx > 0, block_idx >= 0, block_idx < NB - 1)), jnp.ones((G + R,), dtype=bool)))
        query_tile = jnp.transpose(query_blocks[block_idx], (1, 0, 2)).astype(jnp.float32)
        scores = jnp.einsum('hqd,thkd->thqk', query_tile, tile_keys) * score_scale
        row_max = jnp.max(scores, axis=-1)
        weights = jnp.exp(scores - row_max[..., None]).astype(jnp.bfloat16).astype(jnp.float32)
        row_sum = jnp.sum(weights, axis=-1)
        summed = jnp.einsum('thqk,thkd->thqd', weights, tile_values)
        live_b = live[:, None, None]
        overall = jnp.max(jnp.where(live_b, row_max, neg_big), axis=0)
        factor = jnp.where(live_b, jnp.exp(row_max - overall[None]), 0.0)
        numer = jnp.sum(factor[..., None] * summed, axis=0)
        denom = jnp.sum(factor * row_sum, axis=0)
        result = numer / denom[..., None]
        return jnp.transpose(result, (1, 0, 2)).reshape(B, H * DH).astype(jnp.bfloat16)

    attended = lax.map(one_block, jnp.arange(NB, dtype=jnp.int32))
    keep_i = keep.astype(jnp.int32)
    local_rank = (jnp.cumsum(keep_i) - keep_i).astype(jnp.int32)
    place = jnp.where(keep_i > 0, local_rank, NB).astype(jnp.int32)
    packed = jnp.zeros((NB + 1, B, H * DH), jnp.bfloat16).at[place].set(attended)
    return packed[:NB].reshape(L, H * DH)
```

```python
import functools
import math

import jax
import jax.numpy as jnp
from jax import lax
from jax.experimental import pallas as pl
from jax.experimental.pallas import tpu as pltpu
from jax.sharding import PartitionSpec as P

DH = 128
B = 128
G = 2
R = 3
NX = 4
NZ = 8
HD = 4
BD = 8
LCAP = 400

neg_big = -1e30
MESH = pl.DeviceIdType.MESH
SMEM_SPEC = pl.BlockSpec(memory_space=pltpu.SMEM)
VMEM_SPEC = pl.BlockSpec(memory_space=pltpu.VMEM)
score_scale = 1.0 / math.sqrt(DH)


def place():
    s = lax.axis_index("seq")
    return s, s // NZ, lax.rem(s, NZ), lax.axis_index("head")


def to_seq(s, h):
    return (s, h)


def params(cid=None, mib=48):
    if cid is None:
        return pltpu.CompilerParams(vmem_limit_bytes=mib << 20)
    return pltpu.CompilerParams(
        collective_id=cid, has_side_effects=True, vmem_limit_bytes=mib << 20
    )


def table_kernel(row, tab, send_sem, recv_sem):
    s, _, _, h = place()
    n = NX * NZ
    barrier = pltpu.get_barrier_semaphore()
    for d in range(1, n):
        pl.semaphore_signal(
            barrier, inc=1, device_id=(lax.rem(s + d, n), h), device_id_type=MESH
        )
    tab[s] = row[...]
    pl.semaphore_wait(barrier, n - 1)
    copies = []
    for d in range(1, n):
        copy = pltpu.make_async_remote_copy(
            src_ref=row,
            dst_ref=tab.at[s],
            send_sem=send_sem.at[d],
            recv_sem=recv_sem.at[d],
            device_id=(lax.rem(s + d, n), h),
            device_id_type=MESH,
        )
        copy.start()
        copies.append(copy)
    for copy in copies:
        copy.wait()


def gathered_table(row):
    n = NX * NZ
    return pl.pallas_call(
        table_kernel,
        out_shape=jax.ShapeDtypeStruct((n, 1, 128), jnp.int32),
        in_specs=[VMEM_SPEC],
        out_specs=VMEM_SPEC,
        scratch_shapes=[pltpu.SemaphoreType.DMA((n,)), pltpu.SemaphoreType.DMA((n,))],
        compiler_params=params(0, 16),
        name="table",
    )(row)


def plan_kernel(tab, send_idx, items, counts, blk, slot):
    s, x, z, _ = place()
    blk_dev = BD
    n_blocks = NX * NZ * BD

    def one(i, carry):
        rank, used, start = carry
        home = i // blk_dev
        k = tab[home, 0, HD * blk_dev * R + lax.rem(i, blk_dev)]
        used = jnp.where(lax.rem(i, blk_dev) == 0, 0, used)
        start = jnp.where(i == s * blk_dev, rank, start)
        mine = (k > 0) & (lax.rem(rank, NX) == x)
        at = jnp.where(mine, rank // NX, 64)
        blk[at] = i
        slot[at] = lax.rem(home, NZ) * 8 + (home // NZ) * 2 + used
        return rank + k, used + jnp.where(mine, 1, 0), start

    total, _, start = lax.fori_loop(0, n_blocks, one, (0, 0, 0))

    for c in range(8):
        send_idx[c] = 0
    filled = [jnp.int32(0)] * NX
    rank = start
    for j in range(blk_dev):
        k = tab[s, 0, HD * blk_dev * R + j]
        col = lax.rem(rank, NX)
        at = jnp.int32(8)
        for c in range(NX):
            hit = (k > 0) & (col == c)
            at = jnp.where(hit, c * 2 + filled[c], at)
            filled[c] = filled[c] + jnp.where(hit, 1, 0)
        send_idx[at] = j
        rank = rank + k

    def query(a, cnt):
        i = blk[a]
        home = i // blk_dev
        base = lax.rem(i, blk_dev) * R
        pos = (lax.rem(a // 2, NZ)) * 8 + (a // 16) * 2 + lax.rem(a, 2)
        word = slot[a] * 64 + pos
        cnt = list(cnt)

        def add(h, t, ok):
            w = ((t // 64) * 8 + lax.rem(t, blk_dev)) * 4096 + word
            items[h * LCAP + cnt[h]] = w
            cnt[h] = cnt[h] + jnp.where(ok, 1, 0)

        for dt in (-1, 0, 1):
            t = i + dt
            ok = (t >= 0) & (t < n_blocks) & (lax.rem(t // blk_dev, NZ) == z)
            t = jnp.clip(t, 0, n_blocks - 1)
            for h in range(HD):
                add(h, t, ok)
        for g in range(G):
            for h in range(HD):
                add(h, jnp.int32(g), z == 0)
        for h in range(HD):
            for r in range(R):
                t = tab[home, 0, h * blk_dev * R + base + r]
                add(h, t, lax.rem(t // blk_dev, NZ) == z)
        return tuple(cnt)

    n_mine = (total - x + NX - 1) // NX
    cnt = lax.fori_loop(0, n_mine, query, (jnp.int32(0),) * HD)
    for h in range(HD):
        counts[h] = cnt[h]
        for u in range(4):
            items[h * LCAP + cnt[h] + u] = jnp.int32(64)


def planned(tab):
    return pl.pallas_call(
        plan_kernel,
        out_shape=[
            jax.ShapeDtypeStruct((16,), jnp.int32),
            jax.ShapeDtypeStruct((HD * LCAP,), jnp.int32),
            jax.ShapeDtypeStruct((8,), jnp.int32),
        ],
        in_specs=[SMEM_SPEC],
        out_specs=[SMEM_SPEC] * 3,
        scratch_shapes=[pltpu.SMEM((72,), jnp.int32), pltpu.SMEM((72,), jnp.int32)],
        compiler_params=params(None, 16),
        name="plan",
    )(tab)


RING = [(k, h) for k in (1, 2, 3) for h in range(HD)]
RING_UP = RING + [(4, 0), (4, 1)]
RING_DOWN = RING + [(4, 2), (4, 3)]


def spread_kernel(idx, q, k, v, kv, qz, qs, sx, rx, so, ro, sf, rf, su, ru, sd, rd):
    s, x, z, hd = place()

    def at_x(d):
        return (lax.rem(x + d, NX) * NZ + z, hd)

    def at_z(d):
        return (x * NZ + lax.rem(z + d + NZ, NZ), hd)

    def xi(d):
        return lax.rem(x + d + NX, NX)

    def zi(d):
        return lax.rem(z + d + NZ, NZ)

    barrier = pltpu.get_barrier_semaphore()
    for d in (1, 2, 3):
        pl.semaphore_signal(barrier, inc=1, device_id=at_x(d), device_id_type=MESH)
    for d in (1, -1):
        pl.semaphore_signal(barrier, inc=1, device_id=at_z(d), device_id_type=MESH)

    def fill(c, carry):
        col, u = c // 2, lax.rem(c, 2)
        j = idx[c]
        for h in range(HD):
            qs[col, h, u] = q[j, :, h * DH : (h + 1) * DH]
        return carry

    lax.fori_loop(0, 8, fill, 0)
    for h in range(HD):
        for u in range(2):
            qz[h, z, x, u] = qs[x, h, u]
    pl.semaphore_wait(barrier, 5)

    q_out = []
    for d in (1, 2, 3):
        copy = pltpu.make_async_remote_copy(
            src_ref=qs.at[xi(d)],
            dst_ref=qz.at[:, z, x],
            send_sem=sx.at[d],
            recv_sem=rx.at[d],
            device_id=at_x(d),
            device_id_type=MESH,
        )
        copy.start()
        q_out.append(copy)

    own = []
    for h in range(HD):

        def prep(b, carry):
            rows = pl.ds(pl.multiple_of(b * B, B), B)
            kv[h, x, 0, b] = k[rows, h * DH : (h + 1) * DH]
            kv[h, x, 1, b] = v[rows, h * DH : (h + 1) * DH].T
            return carry

        lax.fori_loop(0, BD, prep, 0)
        for side, d in ((0, 1), (1, 3)):
            copy = pltpu.make_async_remote_copy(
                src_ref=kv.at[h, x],
                dst_ref=kv.at[h, x],
                send_sem=so.at[side, h],
                recv_sem=ro.at[side, h],
                device_id=at_x(d),
                device_id_type=MESH,
            )
            copy.start()
            own.append(copy)

    for d in (1, 2, 3):
        src = xi(-d)
        pltpu.make_async_remote_copy(
            src_ref=qz.at[:, z, src],
            dst_ref=qz.at[:, z, src],
            send_sem=sx.at[d],
            recv_sem=rx.at[d],
            device_id=at_x(d),
            device_id_type=MESH,
        ).wait_recv()

    rings = []

    def ring_piece(up, n):
        kk, h = (RING_UP if up else RING_DOWN)[n]
        step = -1 if up else 1
        row = zi(step * (kk - 1))
        return pltpu.make_async_remote_copy(
            src_ref=qz.at[h, row],
            dst_ref=qz.at[h, row],
            send_sem=(su if up else sd).at[n],
            recv_sem=(ru if up else rd).at[n],
            device_id=at_z(1 if up else -1),
            device_id_type=MESH,
        )

    def ring_arrival(up, n):
        kk, h = (RING_UP if up else RING_DOWN)[n]
        row = zi((-1 if up else 1) * kk)
        return pltpu.make_async_remote_copy(
            src_ref=qz.at[h, row],
            dst_ref=qz.at[h, row],
            send_sem=(su if up else sd).at[n],
            recv_sem=(ru if up else rd).at[n],
            device_id=at_z(1 if up else -1),
            device_id_type=MESH,
        )

    for n in range(4):
        for up in (True, False):
            copy = ring_piece(up, n)
            copy.start()
            rings.append(copy)

    fwd = []

    def forward_x(h):
        for side, d, part in ((0, 1, 0), (1, 3, 1)):
            src = xi(-d)
            pltpu.make_async_remote_copy(
                src_ref=kv.at[h, src],
                dst_ref=kv.at[h, src],
                send_sem=so.at[side, h],
                recv_sem=ro.at[side, h],
                device_id=at_x(d),
                device_id_type=MESH,
            ).wait_recv()
            copy = pltpu.make_async_remote_copy(
                src_ref=kv.at[h, src, part],
                dst_ref=kv.at[h, src, part],
                send_sem=sf.at[side, h],
                recv_sem=rf.at[side, h],
                device_id=at_x(d),
                device_id_type=MESH,
            )
            copy.start()
            fwd.append(copy)

    for n in range(14):
        for up in (True, False):
            kk, h = (RING_UP if up else RING_DOWN)[n]
            ring_arrival(up, n).wait_recv()
            table = RING_UP if up else RING_DOWN
            if (kk + 1, h) in table:
                copy = ring_piece(up, table.index((kk + 1, h)))
                copy.start()
                rings.append(copy)
        if n % 2 == 1 and n // 2 < HD:
            forward_x(n // 2)

    far = xi(2)
    for h in range(HD):
        for side, d, part in ((0, 1, 0), (1, 3, 1)):
            pltpu.make_async_remote_copy(
                src_ref=kv.at[h, far, part],
                dst_ref=kv.at[h, far, part],
                send_sem=sf.at[side, h],
                recv_sem=rf.at[side, h],
                device_id=at_x(d),
                device_id_type=MESH,
            ).wait_recv()
    for copy in q_out + own + rings + fwd:
        copy.wait_send()


def spread_all(idx, q, k, v):
    dma = pltpu.SemaphoreType.DMA
    return pl.pallas_call(
        spread_kernel,
        out_shape=[
            jax.ShapeDtypeStruct((HD, NX, 2, BD, B, DH), jnp.bfloat16),
            jax.ShapeDtypeStruct((HD, NZ, NX, 2, B, DH), jnp.bfloat16),
        ],
        in_specs=[SMEM_SPEC] + [VMEM_SPEC] * 3,
        out_specs=[VMEM_SPEC] * 2,
        scratch_shapes=[
            pltpu.VMEM((NX, HD, 2, B, DH), jnp.bfloat16),
            dma((4,)),
            dma((4,)),
            dma((2, HD)),
            dma((2, HD)),
            dma((2, HD)),
            dma((2, HD)),
            dma((14,)),
            dma((14,)),
            dma((14,)),
            dma((14,)),
        ],
        compiler_params=params(1),
        name="spread",
    )(idx, q, k, v)


UNROLL = 4


def part_kernel(ns, items, counts, kv, qz, out, lse, acc, top, den):
    h = pl.program_id(0)
    n_acc = NZ * ns

    def clear(a, carry):
        acc[a] = jnp.zeros((DH, B), jnp.float32)
        top[a] = jnp.full((1, B), neg_big, jnp.float32)
        den[a] = jnp.zeros((1, B), jnp.float32)
        return carry

    lax.fori_loop(0, n_acc + 1, clear, 0)

    def batch(n, carry):
        found = []
        for u in range(UNROLL):
            w = items[h * LCAP + n * UNROLL + u]
            pos = lax.rem(w, 64)
            a = (pos // 8) * ns + lax.rem(pos, 8)
            a = jnp.where(n * UNROLL + u < counts[h], a, n_acc)
            spot = lax.rem(w // 64, 64)
            tile = w // 4096
            keys = kv[0, tile // 8, 0, lax.rem(tile, 8)]
            vals = kv[0, tile // 8, 1, lax.rem(tile, 8)]
            qt = qz[0, spot // 8, lax.rem(spot, 8) // 2, lax.rem(spot, 2)]
            scores = lax.dot_general(
                keys, qt, (((1,), (1,)), ((), ())), preferred_element_type=jnp.float32
            )
            scores = scores * score_scale
            m = jnp.max(scores, axis=0, keepdims=True)
            p = jnp.exp(scores - m).astype(jnp.bfloat16)
            l = jnp.sum(p.astype(jnp.float32), axis=0, keepdims=True)
            o = jnp.dot(vals, p, preferred_element_type=jnp.float32)
            found.append((a, m, l, o))
        for a, m, l, o in found:
            old = top[a]
            new = jnp.maximum(old, m)
            f0, f1 = jnp.exp(old - new), jnp.exp(m - new)
            acc[a] = acc[a] * f0 + o * f1
            den[a] = den[a] * f0 + l * f1
            top[a] = new
        return carry

    lax.fori_loop(0, (counts[h] + UNROLL - 1) // UNROLL, batch, 0)

    def finish(a, carry):
        l = den[a]
        some = l > 0
        safe = jnp.where(some, l, 1.0)
        out[0, a // ns, lax.rem(a, ns)] = (acc[a] / safe).astype(jnp.bfloat16)
        lse[0, a // ns, lax.rem(a, ns)] = jnp.where(some, top[a] + jnp.log(safe), neg_big)
        return carry

    lax.fori_loop(0, n_acc, finish, 0)


def parts_of(ns, items, counts, kv, qz):
    n_acc = NZ * ns
    return pl.pallas_call(
        functools.partial(part_kernel, ns),
        grid=(HD,),
        out_shape=[
            jax.ShapeDtypeStruct((HD, NZ, ns, DH, B), jnp.bfloat16),
            jax.ShapeDtypeStruct((HD, NZ, ns, 1, B), jnp.float32),
        ],
        in_specs=[
            SMEM_SPEC,
            SMEM_SPEC,
            pl.BlockSpec((1, NX, 2, BD, B, DH), lambda h: (h, 0, 0, 0, 0, 0)),
            pl.BlockSpec((1, NZ, NX, 2, B, DH), lambda h: (h, 0, 0, 0, 0, 0)),
        ],
        out_specs=[
            pl.BlockSpec((1, NZ, ns, DH, B), lambda h: (h, 0, 0, 0, 0)),
            pl.BlockSpec((1, NZ, ns, 1, B), lambda h: (h, 0, 0, 0, 0)),
        ],
        scratch_shapes=[
            pltpu.VMEM((n_acc + 1, DH, B), jnp.float32),
            pltpu.VMEM((n_acc + 1, 1, B), jnp.float32),
            pltpu.VMEM((n_acc + 1, 1, B), jnp.float32),
        ],
        compiler_params=params(None, 40),
        name="parts",
    )(items, counts, kv, qz)


HOME_UP = [(4, 2), (4, 3)] + [(k, h) for k in (3, 2, 1) for h in range(HD)]
HOME_DOWN = [(4, 0), (4, 1)] + [(k, h) for k in (3, 2, 1) for h in range(HD)]


def merged(o0, l0, o1, l1):
    top = jnp.maximum(l0, l1)
    f0, f1 = jnp.exp(l0 - top), jnp.exp(l1 - top)
    both = f0 + f1
    o = (o0.astype(jnp.float32) * f0 + o1.astype(jnp.float32) * f1) / both
    return o, top + jnp.log(both)


def join_kernel(
    ns, o, lse, out, sou, slu, rou, rlu, sod, sld, rod, rld, fin, ssu, rsu, ssd, rsd, sx, rx
):
    s, x, z, hd = place()

    def at_x(d):
        return (lax.rem(x + d, NX) * NZ + z, hd)

    def at_z(d):
        return (x * NZ + lax.rem(z + d + NZ, NZ), hd)

    def zi(d):
        return lax.rem(z + d + NZ, NZ)

    barrier = pltpu.get_barrier_semaphore()
    for d in (1, 2, 3):
        pl.semaphore_signal(barrier, inc=1, device_id=at_x(d), device_id_type=MESH)
    for d in (1, -1):
        pl.semaphore_signal(barrier, inc=1, device_id=at_z(d), device_id_type=MESH)
    pl.semaphore_wait(barrier, 5)

    sent = []

    def copies(up, n, src_o, src_l):
        ro, rl = (rou, rlu) if up else (rod, rld)
        ss, rs = (ssu, rsu) if up else (ssd, rsd)
        return [
            pltpu.make_async_remote_copy(
                src_ref=src,
                dst_ref=dst.at[n],
                send_sem=ss.at[i, n],
                recv_sem=rs.at[i, n],
                device_id=at_z(1 if up else -1),
                device_id_type=MESH,
            )
            for i, (src, dst) in enumerate(((src_o, ro), (src_l, rl)))
        ]

    def send(up, n, src_o, src_l):
        for copy in copies(up, n, src_o, src_l):
            copy.start()
            sent.append(copy)

    def arrived(up, n):
        ro, rl = (rou, rlu) if up else (rod, rld)
        for copy in copies(up, n, ro.at[n], rl.at[n]):
            copy.wait_recv()

    for n in range(14):
        for up in (True, False):
            table = HOME_UP if up else HOME_DOWN
            kk, h = table[n]
            dest = zi(kk if up else -kk)
            if (kk + 1, h) not in table:
                send(up, n, o.at[h, dest], lse.at[h, dest])
                continue
            prev = table.index((kk + 1, h))
            arrived(up, prev)
            ro, rl = (rou, rlu) if up else (rod, rld)
            so, sl = (sou, slu) if up else (sod, sld)

            def step(i, carry, ro=ro, rl=rl, so=so, sl=sl, prev=prev, n=n, h=h, dest=dest):
                val, l = merged(o[h, dest, i], lse[h, dest, i], ro[prev, i], rl[prev, i])
                so[n, i] = val.astype(jnp.bfloat16)
                sl[n, i] = l
                return carry

            lax.fori_loop(0, ns, step, 0)
            send(up, n, so.at[n], sl.at[n])

    for h in range(HD):
        n = 10 + h
        arrived(True, n)
        arrived(False, n)

        def last(i, carry, h=h, n=n):
            a, la = merged(rou[n, i], rlu[n, i], rod[n, i], rld[n, i])
            val, _ = merged(o[h, z, i], lse[h, z, i], a, la)
            fin[i // 2, lax.rem(i, 2), :, h * DH : (h + 1) * DH] = val.T.astype(jnp.bfloat16)
            return carry

        lax.fori_loop(0, ns, last, 0)

    rows = ns // 2
    for r in range(NX):
        if r >= rows:

            @pl.when(x == r)
            def _():
                out[...] = jnp.zeros(out.shape, out.dtype)

            continue

        @pl.when(x == r)
        def _(r=r):
            out[:, x] = fin[r]

    def final(r, d):
        return pltpu.make_async_remote_copy(
            src_ref=fin.at[r],
            dst_ref=out.at[:, x],
            send_sem=sx.at[r],
            recv_sem=rx.at[d],
            device_id=(r * NZ + z, hd),
            device_id_type=MESH,
        )

    for d in (1, 2, 3):
        for r in range(rows):

            @pl.when(lax.rem(x + d, NX) == r)
            def _(r=r, d=d):
                final(r, d).start()

    for r in range(rows):

        @pl.when(x == r)
        def _(r=r):
            for d in (1, 2, 3):
                src = lax.rem(x - d + NX, NX)
                pltpu.make_async_remote_copy(
                    src_ref=fin.at[r],
                    dst_ref=out.at[:, src],
                    send_sem=sx.at[r],
                    recv_sem=rx.at[d],
                    device_id=at_x(d),
                    device_id_type=MESH,
                ).wait_recv()

    for d in (1, 2, 3):
        for r in range(rows):

            @pl.when(lax.rem(x + d, NX) == r)
            def _(r=r, d=d):
                final(r, d).wait_send()

    for copy in sent:
        copy.wait_send()


def joined(ns, o, lse):
    dma = pltpu.SemaphoreType.DMA
    piece_o = pltpu.VMEM((14, ns, DH, B), jnp.bfloat16)
    piece_l = pltpu.VMEM((14, ns, 1, B), jnp.float32)
    out = pl.pallas_call(
        functools.partial(join_kernel, ns),
        out_shape=jax.ShapeDtypeStruct((2, NX, B, HD * DH), jnp.bfloat16),
        in_specs=[VMEM_SPEC] * 2,
        out_specs=VMEM_SPEC,
        scratch_shapes=[
            piece_o, piece_l, piece_o, piece_l, piece_o, piece_l, piece_o, piece_l,
            pltpu.VMEM((ns // 2, 2, B, HD * DH), jnp.bfloat16),
            dma((2, 14)), dma((2, 14)), dma((2, 14)), dma((2, 14)),
            dma((4,)), dma((4,)),
        ],
        compiler_params=params(2 + ns // 8, 56),
        name="join%d" % ns,
    )(o, lse)
    return out.reshape(BD * B, HD * DH)


def body(queries, keys, values, random_holder, random_offset, keep):
    want = random_holder * BD + random_offset
    row = jnp.concatenate([want.reshape(-1), keep, jnp.zeros((24,), jnp.int32)])
    tab = gathered_table(row.reshape(1, 128))
    total = jnp.sum(tab[:, 0, HD * BD * R : HD * BD * R + BD])
    send_idx, items, counts = planned(tab)
    kv, qz = spread_all(send_idx, queries.reshape(BD, B, HD * DH), keys, values)

    def tail(ns):
        def run(items, counts, kv, qz):
            return joined(ns, *parts_of(ns, items, counts, kv, qz))

        return run

    return lax.cond(total <= 128, tail(4), tail(8), items, counts, kv, qz)


def solution(mesh):
    in_specs = (
        P("seq", "head"),
        P("seq", "head"),
        P("seq", "head"),
        P("head", "seq", None),
        P("head", "seq", None),
        P("seq"),
    )
    out_specs = P("seq", "head")
    return jax.shard_map(body, mesh=mesh, in_specs=in_specs, out_specs=out_specs, check_vma=False)
```

```python
import functools
import math

import jax
import jax.numpy as jnp
from jax import lax
from jax.experimental import pallas as pl
from jax.experimental.pallas import tpu as pltpu
from jax.sharding import PartitionSpec as P

DH = 128
B = 128
G = 2
R = 3
NX = 4
NZ = 8
HD = 4
BD = 8
LCAP = 400

neg_big = -1e30
MESH = pl.DeviceIdType.MESH
SMEM_SPEC = pl.BlockSpec(memory_space=pltpu.SMEM)
VMEM_SPEC = pl.BlockSpec(memory_space=pltpu.VMEM)
score_scale = 1.0 / math.sqrt(DH)


def place():
    s = lax.axis_index("seq")
    return s, s // NZ, lax.rem(s, NZ), lax.axis_index("head")


def to_seq(s, h):
    return (s, h)


def params(cid=None, mib=48):
    if cid is None:
        return pltpu.CompilerParams(vmem_limit_bytes=mib << 20)
    return pltpu.CompilerParams(
        collective_id=cid, has_side_effects=True, vmem_limit_bytes=mib << 20
    )


def first_kernel(row, k, v, tab, kv, ks, vs, send_sem, recv_sem, load, sk, rk, sf, rf):
    s, x, z, hd = place()
    n = NX * NZ
    loads = [
        pltpu.make_async_copy(k.at[:, :DH], ks, load.at[0]),
        pltpu.make_async_copy(v.at[:, :DH], vs, load.at[1]),
    ]
    for copy in loads:
        copy.start()
    barrier = pltpu.get_barrier_semaphore()
    for d in range(1, n):
        pl.semaphore_signal(
            barrier, inc=1, device_id=(lax.rem(s + d, n), hd), device_id_type=MESH
        )
    tab[s] = row[...]
    for copy in loads:
        copy.wait()

    def prep(b, carry):
        rows = pl.ds(pl.multiple_of(b * B, B), B)
        kv[x, 0, b] = ks[rows, :]
        kv[x, 1, b] = vs[rows, :].T
        return carry

    lax.fori_loop(0, BD, prep, 0)
    pl.semaphore_wait(barrier, n - 1)
    copies = []
    for d in range(1, n):
        copy = pltpu.make_async_remote_copy(
            src_ref=row,
            dst_ref=tab.at[s],
            send_sem=send_sem.at[d],
            recv_sem=recv_sem.at[d],
            device_id=(lax.rem(s + d, n), hd),
            device_id_type=MESH,
        )
        copy.start()
        copies.append(copy)

    gather = RowGather(kv, (sk, rk, sf, rf), x, z, hd)
    gather.own()
    gather.forward()
    gather.finish()
    for copy in copies:
        copy.wait()
    gather.close()


class RowGather:
    def __init__(self, kv, sems, x, z, hd):
        self.kv, self.sems, self.x, self.z, self.hd = kv, sems, x, z, hd
        self.sent = []

    def piece(self, which, side, part, holder):
        sk, rk, sf, rf = self.sems
        ss, rs = (sk, rk) if which == 0 else (sf, rf)
        d = 1 if side == 0 else 3
        return pltpu.make_async_remote_copy(
            src_ref=self.kv.at[holder, part],
            dst_ref=self.kv.at[holder, part],
            send_sem=ss.at[side, part],
            recv_sem=rs.at[side, part],
            device_id=(lax.rem(self.x + d, NX) * NZ + self.z, self.hd),
            device_id_type=MESH,
        )

    def start(self, copy):
        copy.start()
        self.sent.append(copy)

    def own(self):
        for order in (0, 1):
            for side in (0, 1):
                self.start(self.piece(0, side, order ^ side, self.x))

    def neighbour(self, side):
        return lax.rem(self.x + (3 if side == 0 else 1), NX)

    def forward(self):
        for side in (0, 1):
            self.piece(0, side, side, self.neighbour(side)).wait_recv()
            self.start(self.piece(1, side, side, self.neighbour(side)))

    def finish(self):
        for side in (0, 1):
            self.piece(0, side, 1 - side, self.neighbour(side)).wait_recv()
        for side in (0, 1):
            self.piece(1, side, side, lax.rem(self.x + 2, NX)).wait_recv()

    def close(self):
        for copy in self.sent:
            copy.wait_send()


def first_step(row, k, v):
    n = NX * NZ
    dma = pltpu.SemaphoreType.DMA
    any_spec = pl.BlockSpec(memory_space=pl.ANY)
    return pl.pallas_call(
        first_kernel,
        out_shape=[
            jax.ShapeDtypeStruct((n, 1, 128), jnp.int32),
            jax.ShapeDtypeStruct((NX, 2, BD, B, DH), jnp.bfloat16),
        ],
        in_specs=[VMEM_SPEC, any_spec, any_spec],
        out_specs=[VMEM_SPEC] * 2,
        scratch_shapes=[
            pltpu.VMEM((BD * B, DH), jnp.bfloat16),
            pltpu.VMEM((BD * B, DH), jnp.bfloat16),
            dma((n,)), dma((n,)), dma((2,)),
            dma((2, 2)), dma((2, 2)), dma((2, 2)), dma((2, 2)),
        ],
        compiler_params=params(0, 24),
        name="first",
    )(row, k, v)


TQ = 6
UN = 8
W_ANY = 128
W_ALL = 192
LFAST = 400


def fast_plan_kernel(tab, send_idx, comp, items, last, flag, blk, slot, cells):
    s, x, z, _ = place()
    n_home = NX * NZ
    flags = HD * BD * R
    for c in range(NX * NZ):
        cells[c] = 0

    def wipe(i, carry):
        for h in range(HD):
            for u in range(4):
                items[h * LFAST + i * 4 + u] = 0
        return carry

    lax.fori_loop(0, W_ALL // 4, wipe, 0)
    for i in range(HD * 64):
        last[i] = W_ALL
    for c in range(9):
        send_idx[c] = 0
        comp[c] = 0

    def one(home, carry):
        rank, start = carry
        zh, xh = home & (NZ - 1), home >> 3
        start = jnp.where(home == s, rank, start)
        used = jnp.int32(0)
        for b in range(BD):
            k = tab[home, 0, flags + b]
            col = rank & (NX - 1)
            cell = cells[col * NZ + zh]
            mine = (k > 0) & (col == x)
            at = jnp.where(mine, rank >> 2, 64)
            blk[at] = home * BD + b
            slot[at] = zh * 8 + cell
            comp[jnp.where(mine & (zh == z), cell, 8)] = xh * 2 + used
            used = used + jnp.where(mine, 1, 0)
            cells[col * NZ + zh] = cell + k
            rank = rank + k
        return rank, start

    total, start = lax.fori_loop(0, n_home, one, (jnp.int32(0), jnp.int32(0)))
    most = jnp.int32(0)
    for c in range(NX * NZ):
        most = jnp.maximum(most, cells[c])
    flag[0] = jnp.where((total <= 128) & (most <= TQ), 1, 0)

    filled = [jnp.int32(0)] * NX
    rank = start
    for j in range(BD):
        k = tab[s, 0, flags + j]
        col = rank & (NX - 1)
        at = jnp.int32(8)
        for c in range(NX):
            hit = (k > 0) & (col == c)
            at = jnp.where(hit, c * 2 + filled[c], at)
            filled[c] = filled[c] + jnp.where(hit, 1, 0)
        send_idx[at] = j
        rank = rank + k

    def query(a, cnt):
        i = blk[a]
        home, b = i >> 3, i & (BD - 1)
        word = slot[a]
        begin = cnt
        cnt = list(cnt)
        lists = [h * LFAST for h in range(HD)]

        def add(h, w, one):
            items[lists[h] + cnt[h]] = w + jnp.where(cnt[h] == begin[h], 1 << 20, 0)
            cnt[h] = cnt[h] + one

        for dt in (-1, 0, 1):
            t = i + dt
            near = t >> 3
            ok = (t >= 0) & (t < n_home * BD) & ((near & (NZ - 1)) == z)
            w = word + (((t >> 6) & 3) * 8 + (t & 7)) * 64
            one = jnp.where(ok, 1, 0)
            for h in range(HD):
                add(h, w, one)
        one = jnp.where(z == 0, 1, 0)
        for g in range(G):
            for h in range(HD):
                add(h, word + g * 64, one)
        for h in range(HD):
            for r in range(R):
                t = tab[home, 0, h * BD * R + b * R + r]
                w = word + ((t >> 6) * 8 + (t & 7)) * 64
                add(h, w, jnp.where(((t >> 3) & (NZ - 1)) == z, 1, 0))
        for h in range(HD):
            last[h * 64 + a] = jnp.where(cnt[h] > begin[h], cnt[h] - 1, W_ALL)
        return tuple(cnt)

    n_mine = (total - x + NX - 1) >> 2
    cnt = lax.fori_loop(0, n_mine, query, (jnp.int32(0),) * HD)
    for h in range(HD):
        items[h * LFAST + cnt[h]] = 0


def fast_planned(tab):
    i32 = lambda n: jax.ShapeDtypeStruct((n,), jnp.int32)
    return pl.pallas_call(
        fast_plan_kernel,
        out_shape=[i32(16), i32(16), i32(HD * LFAST), i32(HD * 64), i32(8)],
        in_specs=[SMEM_SPEC],
        out_specs=[SMEM_SPEC] * 5,
        scratch_shapes=[
            pltpu.SMEM((72,), jnp.int32),
            pltpu.SMEM((72,), jnp.int32),
            pltpu.SMEM((NX * NZ,), jnp.int32),
        ],
        compiler_params=params(None, 16),
        name="fastplan",
    )(tab)


NS = 4
EXP2 = score_scale * math.log2(math.e)
Q_UP = [(k, h) for h in range(HD) for k in (1, 2, 3)] + [(4, 0), (4, 2)]
Q_DOWN = [(k, h) for h in range(HD) for k in (1, 2, 3)] + [(4, 1), (4, 3)]
M_UP = [(k, h) for h in range(HD) for k in (3, 2, 1)] + [(4, 1), (4, 3)]
M_DOWN = [(k, h) for h in range(HD) for k in (3, 2, 1)] + [(4, 0), (4, 2)]


def main_kernel(idx, comp, items, last, q_any, k_any, v_any, kv_first, out, *rest):
    kvs, qrs, qzs, cos, cls = rest[0:3], rest[3:7], rest[7:11], rest[11:15], rest[15:19]
    (qv, kbuf, vbuf, qs, res, rel, st_o, st_m, st_l, mo, ml, ro, rl, fin) = rest[19:33]
    (load, sqx, rqx, skv, rkv, sfw, rfw, sq, rq, sm, rm, sx, rx) = rest[33:]
    s, x, z, hd = place()
    kv_of = (kv_first,) + tuple(kvs)

    def at_x(d):
        return (lax.rem(x + d, NX) * NZ + z, hd)

    def at_z(d):
        return (x * NZ + lax.rem(z + d + NZ, NZ), hd)

    def xi(d):
        return lax.rem(x + d + NX, NX)

    def zi(d):
        return lax.rem(z + d + NZ, NZ)

    loads = [
        pltpu.make_async_copy(src, dst, load.at[i])
        for i, (src, dst) in enumerate(((q_any, qv), (k_any, kbuf), (v_any, vbuf)))
    ]
    for copy in loads:
        copy.start()
    barrier = pltpu.get_barrier_semaphore()
    for d in (1, 2, 3):
        pl.semaphore_signal(barrier, inc=1, device_id=at_x(d), device_id_type=MESH)
    for d in (1, -1):
        pl.semaphore_signal(barrier, inc=1, device_id=at_z(d), device_id_type=MESH)

    loads[0].wait()

    def fill(c, carry):
        col, u = c // 2, lax.rem(c, 2)
        j = idx[c]
        for h in range(HD):
            qs[col, h, u] = qv[j, :, h * DH : (h + 1) * DH]
        return carry

    lax.fori_loop(0, 8, fill, 0)
    for h in range(HD):
        for u in range(2):
            qrs[h][x, u] = qs[x, h, u]
    pl.semaphore_wait(barrier, 5)

    sent = []

    def start(copy):
        copy.start()
        sent.append(copy)

    def q_move(h, d, src):
        return pltpu.make_async_remote_copy(
            src_ref=qs.at[src, h],
            dst_ref=qrs[h].at[x],
            send_sem=sqx.at[d, h],
            recv_sem=rqx.at[d, h],
            device_id=at_x(d),
            device_id_type=MESH,
        )

    for h in range(HD):
        for d in (1, 3, 2):
            start(q_move(h, d, xi(d)))

    loads[1].wait()
    loads[2].wait()
    gathers = [None]
    for h in range(1, HD):
        g = RowGather(kvs[h - 1], (skv.at[h], rkv.at[h], sfw.at[h], rfw.at[h]), x, z, hd)
        gathers.append(g)

    def prepare(h):
        def prep(b, carry):
            rows = pl.ds(pl.multiple_of(b * B, B), B)
            kvs[h - 1][x, 0, b] = kbuf[rows, h * DH : (h + 1) * DH]
            kvs[h - 1][x, 1, b] = vbuf[rows, h * DH : (h + 1) * DH].T
            return carry

        lax.fori_loop(0, BD, prep, 0)

    prepare(1)
    gathers[1].own()

    def q_copy(up, kk, h, row):
        n = (Q_UP if up else Q_DOWN).index((kk, h))
        return pltpu.make_async_remote_copy(
            src_ref=qzs[h].at[row],
            dst_ref=qzs[h].at[row],
            send_sem=sq.at[0 if up else 1, n],
            recv_sem=rq.at[0 if up else 1, n],
            device_id=at_z(1 if up else -1),
            device_id_type=MESH,
        )

    def q_send(up, kk, h):
        if (kk, h) in (Q_UP if up else Q_DOWN):
            start(q_copy(up, kk, h, zi((-1 if up else 1) * (kk - 1))))

    def q_ready(h):
        for d in (1, 2, 3):
            src = xi(-d)
            pltpu.make_async_remote_copy(
                src_ref=qrs[h].at[src],
                dst_ref=qrs[h].at[src],
                send_sem=sqx.at[d, h],
                recv_sem=rqx.at[d, h],
                device_id=at_x(d),
                device_id_type=MESH,
            ).wait_recv()
        for c in range(TQ):
            w = comp[c]
            qzs[h][z, c] = qrs[h][w >> 1, w & 1]

    def q_begin(h):
        for up in (True, False):
            q_send(up, 1, h)

    def q_step(kk, h):
        for up in (True, False):
            if (kk, h) in (Q_UP if up else Q_DOWN):
                q_copy(up, kk, h, zi((-1 if up else 1) * kk)).wait_recv()
                q_send(up, kk + 1, h)

    nb = jnp.where(z == 0, W_ALL // UN // 4, W_ANY // UN // 4)

    def chunk(h, part):
        kv, qz = kv_of[h], qzs[h]

        def batch(n, carry):
            m0, l0, o0 = st_m[...], st_l[...], st_o[...]
            words = [items[h * LFAST + n * UN + u] for u in range(UN)]
            scores = []
            for w in words:
                spot, tile = w & 63, (w >> 6) & 31
                scores.append(
                    lax.dot_general(
                        kv[tile >> 3, 0, tile & 7],
                        qz[spot >> 3, spot & 7],
                        (((1,), (1,)), ((), ())),
                        preferred_element_type=jnp.float32,
                    )
                )
            tops, weights = [], []
            for sc in scores:
                raw = jnp.max(sc, axis=0, keepdims=True)
                tops.append(raw)
                weights.append(jnp.exp2((sc - raw) * EXP2).astype(jnp.bfloat16))
            sums = []
            for w, p in zip(words, weights):
                tile = (w >> 6) & 31
                rows = jnp.concatenate([kv[tile >> 3, 1, tile & 7], ones], axis=0)
                sums.append(jnp.dot(rows, p, preferred_element_type=jnp.float32))
            for u, w in enumerate(words):
                old = jnp.where((w >> 20) > 0, neg_big, m0)
                top = jnp.maximum(old, tops[u])
                f0, f1 = jnp.exp2((old - top) * EXP2), jnp.exp2((tops[u] - top) * EXP2)
                m0 = top
                l0 = l0 * f0 + sums[u][DH : DH + 1] * f1
                o0 = o0 * f0 + sums[u][:DH] * f1
                at = n * UN + u
                res[at] = o0
                rel[at] = jnp.concatenate([m0, l0], axis=0)
            st_m[...], st_l[...], st_o[...] = m0, l0, o0
            return carry

        ones = jnp.ones((16, B), jnp.bfloat16)
        lax.fori_loop(part * nb, (part + 1) * nb, batch, 0)

    def collect(h):
        for a in range(NZ * NS):
            w = last[h * 64 + a]
            zp, i = (a >> 1) & 7, (a >> 4) * 2 + (a & 1)
            l = rel[w, 1:2]
            cos[h][zp, i] = (res[w] * (1.0 / l)).astype(jnp.bfloat16)
            cls[h][zp, i] = rel[w, 0:1] * score_scale + jnp.log(l)

    def m_copies(up, kk, h, src_o, src_l):
        n = (M_UP if up else M_DOWN).index((kk, h))
        side = 0 if up else 1
        return [
            pltpu.make_async_remote_copy(
                src_ref=src,
                dst_ref=dst.at[side, n],
                send_sem=sm.at[i, side, n],
                recv_sem=rm.at[i, side, n],
                device_id=at_z(1 if up else -1),
                device_id_type=MESH,
            )
            for i, (src, dst) in enumerate(((src_o, ro), (src_l, rl)))
        ]

    def m_arrived(up, kk, h):
        n = (M_UP if up else M_DOWN).index((kk, h))
        side = 0 if up else 1
        for copy in m_copies(up, kk, h, ro.at[side, n], rl.at[side, n]):
            copy.wait_recv()
        return side, n

    def m_step(kk, h):
        for up in (True, False):
            table = M_UP if up else M_DOWN
            if (kk, h) not in table:
                continue
            dest = zi(kk if up else -kk)
            if (kk + 1, h) not in table:
                for copy in m_copies(up, kk, h, cos[h].at[dest], cls[h].at[dest]):
                    start(copy)
                continue
            side, prev = m_arrived(up, kk + 1, h)
            n = table.index((kk, h))
            for i in range(NS):
                val, l = merged(cos[h][dest, i], cls[h][dest, i], ro[side, prev, i], rl[side, prev, i])
                mo[side, n, i] = val.astype(jnp.bfloat16)
                ml[side, n, i] = l
            for copy in m_copies(up, kk, h, mo.at[side, n], ml.at[side, n]):
                start(copy)

    def m_begin(h):
        collect(h)
        m_step(4, h)
        for up in (True, False):
            table = M_UP if up else M_DOWN
            if (4, h) not in table:
                dest = zi(3 if up else -3)
                for copy in m_copies(up, 3, h, cos[h].at[dest], cls[h].at[dest]):
                    start(copy)

    def m_second(h):
        for up in (True, False):
            table = M_UP if up else M_DOWN
            if (4, h) in table:
                dest = zi(3 if up else -3)
                side, prev = m_arrived(up, 4, h)
                n = table.index((3, h))
                for i in range(NS):
                    val, l = merged(cos[h][dest, i], cls[h][dest, i], ro[side, prev, i], rl[side, prev, i])
                    mo[side, n, i] = val.astype(jnp.bfloat16)
                    ml[side, n, i] = l
                for copy in m_copies(up, 3, h, mo.at[side, n], ml.at[side, n]):
                    start(copy)

    def final(h, r, d):
        return pltpu.make_async_remote_copy(
            src_ref=fin.at[h, r],
            dst_ref=out.at[:, x, :, h * DH : (h + 1) * DH],
            send_sem=sx.at[h, r],
            recv_sem=rx.at[h, d],
            device_id=(r * NZ + z, hd),
            device_id_type=MESH,
        )

    rows = NS // 2

    def m_end(h):
        su, nu = m_arrived(True, 1, h)
        sd, nd = m_arrived(False, 1, h)
        for i in range(NS):
            a, la = merged(ro[su, nu, i], rl[su, nu, i], ro[sd, nd, i], rl[sd, nd, i])
            val, _ = merged(cos[h][z, i], cls[h][z, i], a, la)
            fin[h, i // 2, i % 2] = val.T.astype(jnp.bfloat16)
        for r in range(rows):

            @pl.when(x == r)
            def _(r=r):
                for u in range(2):
                    out[u, x, :, h * DH : (h + 1) * DH] = fin[h, r, u]

            for d in (1, 2, 3):

                @pl.when(lax.rem(x + d, NX) == r)
                def _(r=r, d=d):
                    final(h, r, d).start()

    @pl.when(x >= rows)
    def _():
        out[...] = jnp.zeros(out.shape, out.dtype)

    res[W_ALL] = jnp.zeros((DH, B), jnp.float32)
    rel[W_ALL, 0:1] = jnp.full((1, B), neg_big, jnp.float32)
    rel[W_ALL, 1:2] = jnp.ones((1, B), jnp.float32)
    st_o[...] = jnp.zeros((DH, B), jnp.float32)
    st_m[...] = jnp.full((1, B), neg_big, jnp.float32)
    st_l[...] = jnp.zeros((1, B), jnp.float32)

    for h in (0, 1):
        q_ready(h)
        q_begin(h)
    prepare(2)
    prepare(3)
    q_ready(2)
    q_ready(3)
    q_step(1, 0)
    q_step(1, 1)
    q_step(2, 0)
    q_step(2, 1)
    gathers[1].forward()
    gathers[2].own()
    q_step(3, 0)
    q_step(3, 1)
    q_begin(2)
    q_begin(3)
    q_step(4, 0)
    chunk(0, 0)
    q_step(1, 2)
    chunk(0, 1)
    q_step(4, 1)
    q_step(1, 3)
    chunk(0, 2)
    gathers[2].forward()
    gathers[3].own()
    q_step(2, 2)
    chunk(0, 3)
    m_begin(0)
    q_step(2, 3)
    gathers[1].finish()
    chunk(1, 0)
    q_step(3, 2)
    chunk(1, 1)
    q_step(3, 3)
    m_second(0)
    chunk(1, 2)
    q_step(4, 2)
    q_step(4, 3)
    chunk(1, 3)
    m_begin(1)
    m_step(2, 0)
    gathers[3].forward()
    gathers[2].finish()
    chunk(2, 0)
    m_second(1)
    chunk(2, 1)
    m_step(1, 0)
    m_step(2, 1)
    chunk(2, 2)
    chunk(2, 3)
    m_begin(2)
    m_step(1, 1)
    m_end(0)
    gathers[3].finish()
    chunk(3, 0)
    m_second(2)
    m_end(1)
    chunk(3, 1)
    m_step(2, 2)
    chunk(3, 2)
    chunk(3, 3)
    m_begin(3)
    m_step(1, 2)
    m_second(3)
    m_end(2)
    m_step(2, 3)
    m_step(1, 3)
    m_end(3)

    for h in range(HD):
        for r in range(rows):

            @pl.when(x == r)
            def _(h=h, r=r):
                for d in (1, 2, 3):
                    src = lax.rem(x - d + NX, NX)
                    pltpu.make_async_remote_copy(
                        src_ref=fin.at[h, r],
                        dst_ref=out.at[:, src, :, h * DH : (h + 1) * DH],
                        send_sem=sx.at[h, r],
                        recv_sem=rx.at[h, d],
                        device_id=at_x(d),
                        device_id_type=MESH,
                    ).wait_recv()

            for d in (1, 2, 3):

                @pl.when(lax.rem(x + d, NX) == r)
                def _(h=h, r=r, d=d):
                    final(h, r, d).wait_send()

    for g in gathers[1:]:
        g.close()
    for copy in sent:
        copy.wait_send()


def main_step(idx, comp, items, last, q, k, v, kv_first):
    dma = pltpu.SemaphoreType.DMA
    any_spec = pl.BlockSpec(memory_space=pl.ANY)
    bf, f32 = jnp.bfloat16, jnp.float32
    out = pl.pallas_call(
        main_kernel,
        out_shape=jax.ShapeDtypeStruct((2, NX, B, HD * DH), bf),
        in_specs=[SMEM_SPEC] * 4 + [any_spec] * 3 + [VMEM_SPEC],
        out_specs=VMEM_SPEC,
        scratch_shapes=[pltpu.VMEM((NX, 2, BD, B, DH), bf)] * 3
        + [pltpu.VMEM((NX, 2, B, DH), bf)] * HD
        + [pltpu.VMEM((NZ, TQ, B, DH), bf)] * HD
        + [pltpu.VMEM((NZ, NS, DH, B), bf)] * HD
        + [pltpu.VMEM((NZ, NS, 1, B), f32)] * HD
        + [
            pltpu.VMEM((BD, B, HD * DH), bf),
            pltpu.VMEM((BD * B, HD * DH), bf),
            pltpu.VMEM((BD * B, HD * DH), bf),
            pltpu.VMEM((NX, HD, 2, B, DH), bf),
            pltpu.VMEM((W_ALL + 1, DH, B), f32),
            pltpu.VMEM((W_ALL + 1, 2, B), f32),
            pltpu.VMEM((DH, B), f32),
            pltpu.VMEM((1, B), f32),
            pltpu.VMEM((1, B), f32),
            pltpu.VMEM((2, 14, NS, DH, B), bf),
            pltpu.VMEM((2, 14, NS, 1, B), f32),
            pltpu.VMEM((2, 14, NS, DH, B), bf),
            pltpu.VMEM((2, 14, NS, 1, B), f32),
            pltpu.VMEM((HD, NS // 2, 2, B, DH), bf),
        ]
        + [
            dma((3,)),
            dma((4, HD)), dma((4, HD)),
            dma((HD, 2, 2)), dma((HD, 2, 2)), dma((HD, 2, 2)), dma((HD, 2, 2)),
            dma((2, 14)), dma((2, 14)),
            dma((2, 2, 14)), dma((2, 2, 14)),
            dma((HD, NS // 2)), dma((HD, 4)),
        ],
        compiler_params=params(1, 58),
        name="main",
    )(idx, comp, items, last, q, k, v, kv_first)
    return out.reshape(BD * B, HD * DH)


def plan_kernel(tab, send_idx, items, counts, blk, slot):
    s, x, z, _ = place()
    blk_dev = BD
    n_blocks = NX * NZ * BD

    def one(i, carry):
        rank, used, start = carry
        home = i // blk_dev
        k = tab[home, 0, HD * blk_dev * R + lax.rem(i, blk_dev)]
        used = jnp.where(lax.rem(i, blk_dev) == 0, 0, used)
        start = jnp.where(i == s * blk_dev, rank, start)
        mine = (k > 0) & (lax.rem(rank, NX) == x)
        at = jnp.where(mine, rank // NX, 64)
        blk[at] = i
        slot[at] = lax.rem(home, NZ) * 8 + (home // NZ) * 2 + used
        return rank + k, used + jnp.where(mine, 1, 0), start

    total, _, start = lax.fori_loop(0, n_blocks, one, (0, 0, 0))

    for c in range(8):
        send_idx[c] = 0
    filled = [jnp.int32(0)] * NX
    rank = start
    for j in range(blk_dev):
        k = tab[s, 0, HD * blk_dev * R + j]
        col = lax.rem(rank, NX)
        at = jnp.int32(8)
        for c in range(NX):
            hit = (k > 0) & (col == c)
            at = jnp.where(hit, c * 2 + filled[c], at)
            filled[c] = filled[c] + jnp.where(hit, 1, 0)
        send_idx[at] = j
        rank = rank + k

    def query(a, cnt):
        i = blk[a]
        home = i // blk_dev
        base = lax.rem(i, blk_dev) * R
        pos = (lax.rem(a // 2, NZ)) * 8 + (a // 16) * 2 + lax.rem(a, 2)
        word = slot[a] * 64 + pos
        cnt = list(cnt)

        def add(h, t, ok):
            w = ((t // 64) * 8 + lax.rem(t, blk_dev)) * 4096 + word
            items[h * LCAP + cnt[h]] = w
            cnt[h] = cnt[h] + jnp.where(ok, 1, 0)

        for dt in (-1, 0, 1):
            t = i + dt
            ok = (t >= 0) & (t < n_blocks) & (lax.rem(t // blk_dev, NZ) == z)
            t = jnp.clip(t, 0, n_blocks - 1)
            for h in range(HD):
                add(h, t, ok)
        for g in range(G):
            for h in range(HD):
                add(h, jnp.int32(g), z == 0)
        for h in range(HD):
            for r in range(R):
                t = tab[home, 0, h * blk_dev * R + base + r]
                add(h, t, lax.rem(t // blk_dev, NZ) == z)
        return tuple(cnt)

    n_mine = (total - x + NX - 1) // NX
    cnt = lax.fori_loop(0, n_mine, query, (jnp.int32(0),) * HD)
    for h in range(HD):
        counts[h] = cnt[h]
        for u in range(4):
            items[h * LCAP + cnt[h] + u] = jnp.int32(64)


def planned(tab):
    return pl.pallas_call(
        plan_kernel,
        out_shape=[
            jax.ShapeDtypeStruct((16,), jnp.int32),
            jax.ShapeDtypeStruct((HD * LCAP,), jnp.int32),
            jax.ShapeDtypeStruct((8,), jnp.int32),
        ],
        in_specs=[SMEM_SPEC],
        out_specs=[SMEM_SPEC] * 3,
        scratch_shapes=[pltpu.SMEM((72,), jnp.int32), pltpu.SMEM((72,), jnp.int32)],
        compiler_params=params(None, 16),
        name="plan",
    )(tab)


RING = [(k, h) for k in (1, 2, 3) for h in range(HD)]
RING_UP = RING + [(4, 0), (4, 1)]
RING_DOWN = RING + [(4, 2), (4, 3)]


def spread_kernel(idx, q, k, v, kv, qz, qs, sx, rx, so, ro, sf, rf, su, ru, sd, rd):
    s, x, z, hd = place()

    def at_x(d):
        return (lax.rem(x + d, NX) * NZ + z, hd)

    def at_z(d):
        return (x * NZ + lax.rem(z + d + NZ, NZ), hd)

    def xi(d):
        return lax.rem(x + d + NX, NX)

    def zi(d):
        return lax.rem(z + d + NZ, NZ)

    barrier = pltpu.get_barrier_semaphore()
    for d in (1, 2, 3):
        pl.semaphore_signal(barrier, inc=1, device_id=at_x(d), device_id_type=MESH)
    for d in (1, -1):
        pl.semaphore_signal(barrier, inc=1, device_id=at_z(d), device_id_type=MESH)

    def fill(c, carry):
        col, u = c // 2, lax.rem(c, 2)
        j = idx[c]
        for h in range(HD):
            qs[col, h, u] = q[j, :, h * DH : (h + 1) * DH]
        return carry

    lax.fori_loop(0, 8, fill, 0)
    for h in range(HD):
        for u in range(2):
            qz[h, z, x, u] = qs[x, h, u]
    pl.semaphore_wait(barrier, 5)

    q_out = []
    for d in (1, 2, 3):
        copy = pltpu.make_async_remote_copy(
            src_ref=qs.at[xi(d)],
            dst_ref=qz.at[:, z, x],
            send_sem=sx.at[d],
            recv_sem=rx.at[d],
            device_id=at_x(d),
            device_id_type=MESH,
        )
        copy.start()
        q_out.append(copy)

    own = []
    for h in range(HD):

        def prep(b, carry):
            rows = pl.ds(pl.multiple_of(b * B, B), B)
            kv[h, x, 0, b] = k[rows, h * DH : (h + 1) * DH]
            kv[h, x, 1, b] = v[rows, h * DH : (h + 1) * DH].T
            return carry

        lax.fori_loop(0, BD, prep, 0)
        for side, d in ((0, 1), (1, 3)):
            copy = pltpu.make_async_remote_copy(
                src_ref=kv.at[h, x],
                dst_ref=kv.at[h, x],
                send_sem=so.at[side, h],
                recv_sem=ro.at[side, h],
                device_id=at_x(d),
                device_id_type=MESH,
            )
            copy.start()
            own.append(copy)

    for d in (1, 2, 3):
        src = xi(-d)
        pltpu.make_async_remote_copy(
            src_ref=qz.at[:, z, src],
            dst_ref=qz.at[:, z, src],
            send_sem=sx.at[d],
            recv_sem=rx.at[d],
            device_id=at_x(d),
            device_id_type=MESH,
        ).wait_recv()

    rings = []

    def ring_piece(up, n):
        kk, h = (RING_UP if up else RING_DOWN)[n]
        step = -1 if up else 1
        row = zi(step * (kk - 1))
        return pltpu.make_async_remote_copy(
            src_ref=qz.at[h, row],
            dst_ref=qz.at[h, row],
            send_sem=(su if up else sd).at[n],
            recv_sem=(ru if up else rd).at[n],
            device_id=at_z(1 if up else -1),
            device_id_type=MESH,
        )

    def ring_arrival(up, n):
        kk, h = (RING_UP if up else RING_DOWN)[n]
        row = zi((-1 if up else 1) * kk)
        return pltpu.make_async_remote_copy(
            src_ref=qz.at[h, row],
            dst_ref=qz.at[h, row],
            send_sem=(su if up else sd).at[n],
            recv_sem=(ru if up else rd).at[n],
            device_id=at_z(1 if up else -1),
            device_id_type=MESH,
        )

    for n in range(4):
        for up in (True, False):
            copy = ring_piece(up, n)
            copy.start()
            rings.append(copy)

    fwd = []

    def forward_x(h):
        for side, d, part in ((0, 1, 0), (1, 3, 1)):
            src = xi(-d)
            pltpu.make_async_remote_copy(
                src_ref=kv.at[h, src],
                dst_ref=kv.at[h, src],
                send_sem=so.at[side, h],
                recv_sem=ro.at[side, h],
                device_id=at_x(d),
                device_id_type=MESH,
            ).wait_recv()
            copy = pltpu.make_async_remote_copy(
                src_ref=kv.at[h, src, part],
                dst_ref=kv.at[h, src, part],
                send_sem=sf.at[side, h],
                recv_sem=rf.at[side, h],
                device_id=at_x(d),
                device_id_type=MESH,
            )
            copy.start()
            fwd.append(copy)

    for n in range(14):
        for up in (True, False):
            kk, h = (RING_UP if up else RING_DOWN)[n]
            ring_arrival(up, n).wait_recv()
            table = RING_UP if up else RING_DOWN
            if (kk + 1, h) in table:
                copy = ring_piece(up, table.index((kk + 1, h)))
                copy.start()
                rings.append(copy)
        if n % 2 == 1 and n // 2 < HD:
            forward_x(n // 2)

    far = xi(2)
    for h in range(HD):
        for side, d, part in ((0, 1, 0), (1, 3, 1)):
            pltpu.make_async_remote_copy(
                src_ref=kv.at[h, far, part],
                dst_ref=kv.at[h, far, part],
                send_sem=sf.at[side, h],
                recv_sem=rf.at[side, h],
                device_id=at_x(d),
                device_id_type=MESH,
            ).wait_recv()
    for copy in q_out + own + rings + fwd:
        copy.wait_send()


def spread_all(idx, q, k, v):
    dma = pltpu.SemaphoreType.DMA
    return pl.pallas_call(
        spread_kernel,
        out_shape=[
            jax.ShapeDtypeStruct((HD, NX, 2, BD, B, DH), jnp.bfloat16),
            jax.ShapeDtypeStruct((HD, NZ, NX, 2, B, DH), jnp.bfloat16),
        ],
        in_specs=[SMEM_SPEC] + [VMEM_SPEC] * 3,
        out_specs=[VMEM_SPEC] * 2,
        scratch_shapes=[
            pltpu.VMEM((NX, HD, 2, B, DH), jnp.bfloat16),
            dma((4,)),
            dma((4,)),
            dma((2, HD)),
            dma((2, HD)),
            dma((2, HD)),
            dma((2, HD)),
            dma((14,)),
            dma((14,)),
            dma((14,)),
            dma((14,)),
        ],
        compiler_params=params(2),
        name="spread",
    )(idx, q, k, v)


UNROLL = 4


def part_kernel(ns, items, counts, kv, qz, out, lse, acc, top, den):
    h = pl.program_id(0)
    n_acc = NZ * ns

    def clear(a, carry):
        acc[a] = jnp.zeros((DH, B), jnp.float32)
        top[a] = jnp.full((1, B), neg_big, jnp.float32)
        den[a] = jnp.zeros((1, B), jnp.float32)
        return carry

    lax.fori_loop(0, n_acc + 1, clear, 0)

    def batch(n, carry):
        found = []
        for u in range(UNROLL):
            w = items[h * LCAP + n * UNROLL + u]
            pos = lax.rem(w, 64)
            a = (pos // 8) * ns + lax.rem(pos, 8)
            a = jnp.where(n * UNROLL + u < counts[h], a, n_acc)
            spot = lax.rem(w // 64, 64)
            tile = w // 4096
            keys = kv[0, tile // 8, 0, lax.rem(tile, 8)]
            vals = kv[0, tile // 8, 1, lax.rem(tile, 8)]
            qt = qz[0, spot // 8, lax.rem(spot, 8) // 2, lax.rem(spot, 2)]
            scores = lax.dot_general(
                keys, qt, (((1,), (1,)), ((), ())), preferred_element_type=jnp.float32
            )
            scores = scores * score_scale
            m = jnp.max(scores, axis=0, keepdims=True)
            p = jnp.exp(scores - m).astype(jnp.bfloat16)
            l = jnp.sum(p.astype(jnp.float32), axis=0, keepdims=True)
            o = jnp.dot(vals, p, preferred_element_type=jnp.float32)
            found.append((a, m, l, o))
        for a, m, l, o in found:
            old = top[a]
            new = jnp.maximum(old, m)
            f0, f1 = jnp.exp(old - new), jnp.exp(m - new)
            acc[a] = acc[a] * f0 + o * f1
            den[a] = den[a] * f0 + l * f1
            top[a] = new
        return carry

    lax.fori_loop(0, (counts[h] + UNROLL - 1) // UNROLL, batch, 0)

    def finish(a, carry):
        l = den[a]
        some = l > 0
        safe = jnp.where(some, l, 1.0)
        out[0, a // ns, lax.rem(a, ns)] = (acc[a] / safe).astype(jnp.bfloat16)
        lse[0, a // ns, lax.rem(a, ns)] = jnp.where(some, top[a] + jnp.log(safe), neg_big)
        return carry

    lax.fori_loop(0, n_acc, finish, 0)


def parts_of(ns, items, counts, kv, qz):
    n_acc = NZ * ns
    return pl.pallas_call(
        functools.partial(part_kernel, ns),
        grid=(HD,),
        out_shape=[
            jax.ShapeDtypeStruct((HD, NZ, ns, DH, B), jnp.bfloat16),
            jax.ShapeDtypeStruct((HD, NZ, ns, 1, B), jnp.float32),
        ],
        in_specs=[
            SMEM_SPEC,
            SMEM_SPEC,
            pl.BlockSpec((1, NX, 2, BD, B, DH), lambda h: (h, 0, 0, 0, 0, 0)),
            pl.BlockSpec((1, NZ, NX, 2, B, DH), lambda h: (h, 0, 0, 0, 0, 0)),
        ],
        out_specs=[
            pl.BlockSpec((1, NZ, ns, DH, B), lambda h: (h, 0, 0, 0, 0)),
            pl.BlockSpec((1, NZ, ns, 1, B), lambda h: (h, 0, 0, 0, 0)),
        ],
        scratch_shapes=[
            pltpu.VMEM((n_acc + 1, DH, B), jnp.float32),
            pltpu.VMEM((n_acc + 1, 1, B), jnp.float32),
            pltpu.VMEM((n_acc + 1, 1, B), jnp.float32),
        ],
        compiler_params=params(None, 40),
        name="parts",
    )(items, counts, kv, qz)


HOME_UP = [(4, 2), (4, 3)] + [(k, h) for k in (3, 2, 1) for h in range(HD)]
HOME_DOWN = [(4, 0), (4, 1)] + [(k, h) for k in (3, 2, 1) for h in range(HD)]


def merged(o0, l0, o1, l1):
    top = jnp.maximum(l0, l1)
    f0, f1 = jnp.exp(l0 - top), jnp.exp(l1 - top)
    both = f0 + f1
    o = (o0.astype(jnp.float32) * f0 + o1.astype(jnp.float32) * f1) / both
    return o, top + jnp.log(both)


def join_kernel(
    ns, o, lse, out, sou, slu, rou, rlu, sod, sld, rod, rld, fin, ssu, rsu, ssd, rsd, sx, rx
):
    s, x, z, hd = place()

    def at_x(d):
        return (lax.rem(x + d, NX) * NZ + z, hd)

    def at_z(d):
        return (x * NZ + lax.rem(z + d + NZ, NZ), hd)

    def zi(d):
        return lax.rem(z + d + NZ, NZ)

    barrier = pltpu.get_barrier_semaphore()
    for d in (1, 2, 3):
        pl.semaphore_signal(barrier, inc=1, device_id=at_x(d), device_id_type=MESH)
    for d in (1, -1):
        pl.semaphore_signal(barrier, inc=1, device_id=at_z(d), device_id_type=MESH)
    pl.semaphore_wait(barrier, 5)

    sent = []

    def copies(up, n, src_o, src_l):
        ro, rl = (rou, rlu) if up else (rod, rld)
        ss, rs = (ssu, rsu) if up else (ssd, rsd)
        return [
            pltpu.make_async_remote_copy(
                src_ref=src,
                dst_ref=dst.at[n],
                send_sem=ss.at[i, n],
                recv_sem=rs.at[i, n],
                device_id=at_z(1 if up else -1),
                device_id_type=MESH,
            )
            for i, (src, dst) in enumerate(((src_o, ro), (src_l, rl)))
        ]

    def send(up, n, src_o, src_l):
        for copy in copies(up, n, src_o, src_l):
            copy.start()
            sent.append(copy)

    def arrived(up, n):
        ro, rl = (rou, rlu) if up else (rod, rld)
        for copy in copies(up, n, ro.at[n], rl.at[n]):
            copy.wait_recv()

    for n in range(14):
        for up in (True, False):
            table = HOME_UP if up else HOME_DOWN
            kk, h = table[n]
            dest = zi(kk if up else -kk)
            if (kk + 1, h) not in table:
                send(up, n, o.at[h, dest], lse.at[h, dest])
                continue
            prev = table.index((kk + 1, h))
            arrived(up, prev)
            ro, rl = (rou, rlu) if up else (rod, rld)
            so, sl = (sou, slu) if up else (sod, sld)

            def step(i, carry, ro=ro, rl=rl, so=so, sl=sl, prev=prev, n=n, h=h, dest=dest):
                val, l = merged(o[h, dest, i], lse[h, dest, i], ro[prev, i], rl[prev, i])
                so[n, i] = val.astype(jnp.bfloat16)
                sl[n, i] = l
                return carry

            lax.fori_loop(0, ns, step, 0)
            send(up, n, so.at[n], sl.at[n])

    for h in range(HD):
        n = 10 + h
        arrived(True, n)
        arrived(False, n)

        def last(i, carry, h=h, n=n):
            a, la = merged(rou[n, i], rlu[n, i], rod[n, i], rld[n, i])
            val, _ = merged(o[h, z, i], lse[h, z, i], a, la)
            fin[i // 2, lax.rem(i, 2), :, h * DH : (h + 1) * DH] = val.T.astype(jnp.bfloat16)
            return carry

        lax.fori_loop(0, ns, last, 0)

    rows = ns // 2
    for r in range(NX):
        if r >= rows:

            @pl.when(x == r)
            def _():
                out[...] = jnp.zeros(out.shape, out.dtype)

            continue

        @pl.when(x == r)
        def _(r=r):
            out[:, x] = fin[r]

    def final(r, d):
        return pltpu.make_async_remote_copy(
            src_ref=fin.at[r],
            dst_ref=out.at[:, x],
            send_sem=sx.at[r],
            recv_sem=rx.at[d],
            device_id=(r * NZ + z, hd),
            device_id_type=MESH,
        )

    for d in (1, 2, 3):
        for r in range(rows):

            @pl.when(lax.rem(x + d, NX) == r)
            def _(r=r, d=d):
                final(r, d).start()

    for r in range(rows):

        @pl.when(x == r)
        def _(r=r):
            for d in (1, 2, 3):
                src = lax.rem(x - d + NX, NX)
                pltpu.make_async_remote_copy(
                    src_ref=fin.at[r],
                    dst_ref=out.at[:, src],
                    send_sem=sx.at[r],
                    recv_sem=rx.at[d],
                    device_id=at_x(d),
                    device_id_type=MESH,
                ).wait_recv()

    for d in (1, 2, 3):
        for r in range(rows):

            @pl.when(lax.rem(x + d, NX) == r)
            def _(r=r, d=d):
                final(r, d).wait_send()

    for copy in sent:
        copy.wait_send()


def joined(ns, o, lse):
    dma = pltpu.SemaphoreType.DMA
    piece_o = pltpu.VMEM((14, ns, DH, B), jnp.bfloat16)
    piece_l = pltpu.VMEM((14, ns, 1, B), jnp.float32)
    out = pl.pallas_call(
        functools.partial(join_kernel, ns),
        out_shape=jax.ShapeDtypeStruct((2, NX, B, HD * DH), jnp.bfloat16),
        in_specs=[VMEM_SPEC] * 2,
        out_specs=VMEM_SPEC,
        scratch_shapes=[
            piece_o, piece_l, piece_o, piece_l, piece_o, piece_l, piece_o, piece_l,
            pltpu.VMEM((ns // 2, 2, B, HD * DH), jnp.bfloat16),
            dma((2, 14)), dma((2, 14)), dma((2, 14)), dma((2, 14)),
            dma((4,)), dma((4,)),
        ],
        compiler_params=params(3, 56),
        name="join%d" % ns,
    )(o, lse)
    return out.reshape(BD * B, HD * DH)


def body(queries, keys, values, random_holder, random_offset, keep):
    want = random_holder * BD + random_offset
    row = jnp.concatenate([want.reshape(-1), keep, jnp.zeros((24,), jnp.int32)])
    tab, kv_first = first_step(row.reshape(1, 128), keys, values)
    q = queries.reshape(BD, B, HD * DH)
    idx, comp, items, last, flag = fast_planned(tab)

    def fast(idx, comp, items, last, tab, q, keys, values, kv_first):
        return main_step(idx, comp, items, last, q, keys, values, kv_first)

    def wide(idx, comp, items, last, tab, q, keys, values, kv_first):
        send_idx, items, counts = planned(tab)
        kv, qz = spread_all(send_idx, q, keys, values)
        return joined(8, *parts_of(8, items, counts, kv, qz))

    return lax.cond(
        flag[0] > 0, fast, wide, idx, comp, items, last, tab, q, keys, values, kv_first
    )


def solution(mesh):
    in_specs = (
        P("seq", "head"),
        P("seq", "head"),
        P("seq", "head"),
        P("head", "seq", None),
        P("head", "seq", None),
        P("seq"),
    )
    out_specs = P("seq", "head")
    return jax.shard_map(body, mesh=mesh, in_specs=in_specs, out_specs=out_specs, check_vma=False)
```

```python
import functools
import math

import jax
import jax.numpy as jnp
from jax import lax
from jax.experimental import pallas as pl
from jax.experimental.pallas import tpu as pltpu
from jax.sharding import PartitionSpec as P

DH = 128
B = 128
G = 2
R = 3
NX = 4
NZ = 8
HD = 4
BD = 8
LCAP = 400

neg_big = -1e30
MESH = pl.DeviceIdType.MESH
SMEM_SPEC = pl.BlockSpec(memory_space=pltpu.SMEM)
VMEM_SPEC = pl.BlockSpec(memory_space=pltpu.VMEM)
score_scale = 1.0 / math.sqrt(DH)


def place():
    s = lax.axis_index("seq")
    return s, s // NZ, lax.rem(s, NZ), lax.axis_index("head")


def to_seq(s, h):
    return (s, h)


def params(cid=None, mib=48):
    if cid is None:
        return pltpu.CompilerParams(vmem_limit_bytes=mib << 20)
    return pltpu.CompilerParams(
        collective_id=cid, has_side_effects=True, vmem_limit_bytes=mib << 20
    )


def table_kernel(row, tab, send_sem, recv_sem):
    s, _, _, h = place()
    n = NX * NZ
    barrier = pltpu.get_barrier_semaphore()
    for d in range(1, n):
        pl.semaphore_signal(
            barrier, inc=1, device_id=(lax.rem(s + d, n), h), device_id_type=MESH
        )
    tab[s] = row[...]
    pl.semaphore_wait(barrier, n - 1)
    copies = []
    for d in range(1, n):
        copy = pltpu.make_async_remote_copy(
            src_ref=row,
            dst_ref=tab.at[s],
            send_sem=send_sem.at[d],
            recv_sem=recv_sem.at[d],
            device_id=(lax.rem(s + d, n), h),
            device_id_type=MESH,
        )
        copy.start()
        copies.append(copy)
    for copy in copies:
        copy.wait()


def gathered_table(row):
    n = NX * NZ
    return pl.pallas_call(
        table_kernel,
        out_shape=jax.ShapeDtypeStruct((n, 1, 128), jnp.int32),
        in_specs=[VMEM_SPEC],
        out_specs=VMEM_SPEC,
        scratch_shapes=[pltpu.SemaphoreType.DMA((n,)), pltpu.SemaphoreType.DMA((n,))],
        compiler_params=params(0, 16),
        name="table",
    )(row)


class RowGather:
    def __init__(self, kv, sems, x, z, hd):
        self.kv, self.sems, self.x, self.z, self.hd = kv, sems, x, z, hd
        self.sent = []

    def piece(self, which, side, part, holder):
        sk, rk, sf, rf = self.sems
        ss, rs = (sk, rk) if which == 0 else (sf, rf)
        d = 1 if side == 0 else 3
        return pltpu.make_async_remote_copy(
            src_ref=self.kv.at[holder, part],
            dst_ref=self.kv.at[holder, part],
            send_sem=ss.at[side, part],
            recv_sem=rs.at[side, part],
            device_id=(lax.rem(self.x + d, NX) * NZ + self.z, self.hd),
            device_id_type=MESH,
        )

    def start(self, copy):
        copy.start()
        self.sent.append(copy)

    def own(self):
        for order in (0, 1):
            for side in (0, 1):
                self.start(self.piece(0, side, order ^ side, self.x))

    def neighbour(self, side):
        return lax.rem(self.x + (3 if side == 0 else 1), NX)

    def forward(self):
        for side in (0, 1):
            self.piece(0, side, side, self.neighbour(side)).wait_recv()
            self.start(self.piece(1, side, side, self.neighbour(side)))

    def finish(self):
        for side in (0, 1):
            self.piece(0, side, 1 - side, self.neighbour(side)).wait_recv()
        for side in (0, 1):
            self.piece(1, side, side, lax.rem(self.x + 2, NX)).wait_recv()

    def close(self):
        for copy in self.sent:
            copy.wait_send()


UN = 8
W_ANY = 128
W_ALL = 192
LFAST = 400


def fast_plan_kernel(tab, tabv, send_idx, comp, items, last, flag, blk, slot, cells):
    s, x, z, _ = place()
    n_home = NX * NZ
    flags = HD * BD * R

    lane = lax.broadcasted_iota(jnp.int32, (n_home, 128), 1)
    kept = jnp.where((lane >= flags) & (lane < flags + BD), tabv[:, 0, :], 0).astype(jnp.float32)
    before = (
        lax.broadcasted_iota(jnp.int32, (128, 128), 0)
        < lax.broadcasted_iota(jnp.int32, (128, 128), 1)
    ).astype(jnp.float32)
    above = (
        lax.broadcasted_iota(jnp.int32, (n_home, n_home), 1)
        < lax.broadcasted_iota(jnp.int32, (n_home, n_home), 0)
    ).astype(jnp.float32)
    in_row = jnp.dot(kept, before, preferred_element_type=jnp.float32)
    rows = jnp.sum(kept, axis=1, keepdims=True)
    upper = jnp.dot(above, jnp.broadcast_to(rows, (n_home, 128)), preferred_element_type=jnp.float32)
    ranks = (in_row + upper).astype(jnp.int32)
    most = jnp.zeros((NZ, 1), jnp.float32)
    for c in range(NX):
        n = jnp.sum(jnp.where((ranks & (NX - 1)) == c, kept, 0.0), axis=1, keepdims=True)
        most = jnp.maximum(most, n[0:8] + n[8:16] + n[16:24] + n[24:32])
    most = jnp.max(most)

    for c in range(NZ):
        cells[c] = 0

    def wipe(i, carry):
        for h in range(HD):
            for u in range(8):
                items[h * LFAST + i * 8 + u] = 0
        return carry

    lax.fori_loop(0, W_ALL // 8, wipe, 0)
    for h in range(HD):
        for i in range(32):
            last[h * 64 + i] = W_ALL
    for c in range(9):
        send_idx[c] = 0
        comp[c] = 0

    def one(home, carry):
        rank, start = carry
        zh, xh = home & (NZ - 1), home >> 3
        start = jnp.where(home == s, rank, start)
        used = xh * 2
        cell = cells[zh]
        here = zh == z
        for b in range(BD):
            k = tab[home, 0, flags + b]
            mine = (k > 0) & ((rank & (NX - 1)) == x)
            at = jnp.where(mine, rank >> 2, 64)
            blk[at] = home * BD + b
            slot[at] = zh * 8 + cell
            comp[jnp.where(mine & here, cell, 8)] = used
            add = jnp.where(mine, 1, 0)
            used = used + add
            cell = cell + add
            rank = rank + k
        cells[zh] = cell
        return rank, start

    total, start = lax.fori_loop(0, n_home, one, (jnp.int32(0), jnp.int32(0)))
    fits = jnp.where(most <= 5.0, 2, jnp.where(most <= 6.0, 1, 0))
    flag[0] = jnp.where(total <= 128, fits, 0)

    filled = [jnp.int32(0)] * NX
    rank = start
    for j in range(BD):
        k = tab[s, 0, flags + j]
        col = rank & (NX - 1)
        at = jnp.int32(8)
        for c in range(NX):
            hit = (k > 0) & (col == c)
            at = jnp.where(hit, c * 2 + filled[c], at)
            filled[c] = filled[c] + jnp.where(hit, 1, 0)
        send_idx[at] = j
        rank = rank + k

    def query(a, cnt):
        i = blk[a]
        home, b = i >> 3, i & (BD - 1)
        word = slot[a]
        begin = [c + h * LFAST for h, c in enumerate(cnt)]
        cnt = list(begin)

        def add(h, w, one):
            items[cnt[h]] = w + jnp.where(cnt[h] == begin[h], 1 << 20, 0)
            cnt[h] = cnt[h] + one

        for dt in (-1, 0, 1):
            t = i + dt
            near = t >> 3
            ok = (t >= 0) & (t < n_home * BD) & ((near & (NZ - 1)) == z)
            w = word + (((t >> 6) & 3) * 8 + (t & 7)) * 64
            one = jnp.where(ok, 1, 0)
            for h in range(HD):
                add(h, w, one)
        for h in range(HD):
            for r in range(R):
                t = tab[home, 0, h * BD * R + b * R + r]
                w = word + ((t >> 6) * 8 + (t & 7)) * 64
                add(h, w, jnp.where(((t >> 3) & (NZ - 1)) == z, 1, 0))

        def with_shared(*cnt):
            cnt = list(cnt)
            for h in range(HD):
                for g in range(G):
                    items[cnt[h]] = word + g * 64 + jnp.where(cnt[h] == begin[h], 1 << 20, 0)
                    cnt[h] = cnt[h] + 1
            return tuple(cnt)

        cnt = lax.cond(z == 0, with_shared, lambda *cnt: tuple(cnt), *cnt)
        for h in range(HD):
            last[h * 64 + a] = jnp.where(cnt[h] > begin[h], cnt[h] - 1 - h * LFAST, W_ALL)
        return tuple(c - h * LFAST for h, c in enumerate(cnt))

    n_mine = (total - x + NX - 1) >> 2
    cnt = lax.fori_loop(0, n_mine, query, (jnp.int32(0),) * HD)
    for h in range(HD):
        items[h * LFAST + cnt[h]] = 0


def fast_planned(tab):
    i32 = lambda n: jax.ShapeDtypeStruct((n,), jnp.int32)
    return pl.pallas_call(
        fast_plan_kernel,
        out_shape=[i32(16), i32(16), i32(HD * LFAST), i32(HD * 64), i32(8)],
        in_specs=[SMEM_SPEC, VMEM_SPEC],
        out_specs=[SMEM_SPEC] * 5,
        scratch_shapes=[
            pltpu.SMEM((72,), jnp.int32),
            pltpu.SMEM((72,), jnp.int32),
            pltpu.SMEM((NZ,), jnp.int32),
        ],
        compiler_params=params(None, 16),
        name="fastplan",
    )(tab, tab)


NS = 4
EXP2 = score_scale * math.log2(math.e)
Q_UP = [(k, h) for h in range(HD) for k in (1, 2, 3)] + [(4, 0), (4, 2)]
Q_DOWN = [(k, h) for h in range(HD) for k in (1, 2, 3)] + [(4, 1), (4, 3)]
M_UP = [(k, h) for h in range(HD) for k in (3, 2, 1)] + [(4, 1), (4, 3)]
M_DOWN = [(k, h) for h in range(HD) for k in (3, 2, 1)] + [(4, 0), (4, 2)]


def main_kernel(tq, idx, comp, items, last, q_any, k_any, v_any, out, *rest):
    kvs, qrs, qzs, cos, cls = rest[0:4], rest[4:8], rest[8:12], rest[12:16], rest[16:20]
    (qv, kbuf, vbuf, qs, res, rel, st_o, st_m, st_l, mo, ml, ro, rl, fin) = rest[20:34]
    (load, sqx, rqx, skv, rkv, sfw, rfw, sq, rq, sm, rm, sx, rx) = rest[34:]
    s, x, z, hd = place()

    def at_x(d):
        return (lax.rem(x + d, NX) * NZ + z, hd)

    def at_z(d):
        return (x * NZ + lax.rem(z + d + NZ, NZ), hd)

    def xi(d):
        return lax.rem(x + d + NX, NX)

    def zi(d):
        return lax.rem(z + d + NZ, NZ)

    loads = [
        pltpu.make_async_copy(src, dst, load.at[i])
        for i, (src, dst) in enumerate(((q_any, qv), (k_any, kbuf), (v_any, vbuf)))
    ]
    for copy in loads:
        copy.start()
    barrier = pltpu.get_barrier_semaphore()
    for d in (1, 2, 3):
        pl.semaphore_signal(barrier, inc=1, device_id=at_x(d), device_id_type=MESH)
    for d in (1, -1):
        pl.semaphore_signal(barrier, inc=1, device_id=at_z(d), device_id_type=MESH)

    loads[0].wait()

    def fill(c, carry):
        col, u = c // 2, lax.rem(c, 2)
        j = idx[c]
        for h in range(HD):
            qs[col, h, u] = qv[j, :, h * DH : (h + 1) * DH]
        return carry

    lax.fori_loop(0, 8, fill, 0)
    for h in range(HD):
        for u in range(2):
            qrs[h][x, u] = qs[x, h, u]
    pl.semaphore_wait(barrier, 5)

    sent = []

    def start(copy):
        copy.start()
        sent.append(copy)

    def q_move(h, d, src):
        return pltpu.make_async_remote_copy(
            src_ref=qs.at[src, h],
            dst_ref=qrs[h].at[x],
            send_sem=sqx.at[d, h],
            recv_sem=rqx.at[d, h],
            device_id=at_x(d),
            device_id_type=MESH,
        )

    for h in range(HD):
        for d in (1, 3, 2):
            start(q_move(h, d, xi(d)))

    loads[1].wait()
    loads[2].wait()
    gathers = []
    for h in range(HD):
        g = RowGather(kvs[h], (skv.at[h], rkv.at[h], sfw.at[h], rfw.at[h]), x, z, hd)
        gathers.append(g)

    def prepare(h):
        def prep(b, carry):
            rows = pl.ds(pl.multiple_of(b * B, B), B)
            kvs[h][x, 0, b] = kbuf[rows, h * DH : (h + 1) * DH]
            kvs[h][x, 1, b] = vbuf[rows, h * DH : (h + 1) * DH].T
            return carry

        lax.fori_loop(0, BD, prep, 0)

    prepare(0)
    gathers[0].own()

    def q_copy(up, kk, h, row):
        n = (Q_UP if up else Q_DOWN).index((kk, h))
        return pltpu.make_async_remote_copy(
            src_ref=qzs[h].at[row],
            dst_ref=qzs[h].at[row],
            send_sem=sq.at[0 if up else 1, n],
            recv_sem=rq.at[0 if up else 1, n],
            device_id=at_z(1 if up else -1),
            device_id_type=MESH,
        )

    def q_send(up, kk, h):
        if (kk, h) in (Q_UP if up else Q_DOWN):
            start(q_copy(up, kk, h, zi((-1 if up else 1) * (kk - 1))))

    def q_ready(h):
        for d in (1, 2, 3):
            src = xi(-d)
            pltpu.make_async_remote_copy(
                src_ref=qrs[h].at[src],
                dst_ref=qrs[h].at[src],
                send_sem=sqx.at[d, h],
                recv_sem=rqx.at[d, h],
                device_id=at_x(d),
                device_id_type=MESH,
            ).wait_recv()
        for c in range(tq):
            w = comp[c]
            qzs[h][z, c] = qrs[h][w >> 1, w & 1]

    def q_begin(h):
        for up in (True, False):
            q_send(up, 1, h)

    def q_step(kk, h):
        for up in (True, False):
            if (kk, h) in (Q_UP if up else Q_DOWN):
                q_copy(up, kk, h, zi((-1 if up else 1) * kk)).wait_recv()
                q_send(up, kk + 1, h)

    nb = jnp.where(z == 0, W_ALL // UN // 4, W_ANY // UN // 4)

    def chunk(h, part):
        kv, qz = kvs[h], qzs[h]

        def batch(n, carry):
            m0, l0, o0 = st_m[...], st_l[...], st_o[...]
            words = [items[h * LFAST + n * UN + u] for u in range(UN)]
            scores = []
            for w in words:
                spot, tile = w & 63, (w >> 6) & 31
                scores.append(
                    lax.dot_general(
                        kv[tile >> 3, 0, tile & 7],
                        qz[spot >> 3, spot & 7],
                        (((1,), (1,)), ((), ())),
                        preferred_element_type=jnp.float32,
                    )
                )
            tops, weights = [], []
            for sc in scores:
                raw = jnp.max(sc, axis=0, keepdims=True)
                tops.append(raw)
                weights.append(jnp.exp2((sc - raw) * EXP2).astype(jnp.bfloat16))
            sums = []
            for w, p in zip(words, weights):
                tile = (w >> 6) & 31
                rows = jnp.concatenate([kv[tile >> 3, 1, tile & 7], ones], axis=0)
                sums.append(jnp.dot(rows, p, preferred_element_type=jnp.float32))
            for u, w in enumerate(words):
                old = jnp.where((w >> 20) > 0, neg_big, m0)
                top = jnp.maximum(old, tops[u])
                f0, f1 = jnp.exp2((old - top) * EXP2), jnp.exp2((tops[u] - top) * EXP2)
                m0 = top
                l0 = l0 * f0 + sums[u][DH : DH + 1] * f1
                o0 = o0 * f0 + sums[u][:DH] * f1
                at = n * UN + u
                res[at] = o0
                rel[at] = jnp.concatenate([m0, l0], axis=0)
            st_m[...], st_l[...], st_o[...] = m0, l0, o0
            return carry

        ones = jnp.ones((16, B), jnp.bfloat16)
        lax.fori_loop(part * nb, (part + 1) * nb, batch, 0)

    def collect(h):
        for a in range(NZ * NS):
            w = last[h * 64 + a]
            zp, i = (a >> 1) & 7, (a >> 4) * 2 + (a & 1)
            l = rel[w, 1:2]
            cos[h][zp, i] = (res[w] * (1.0 / l)).astype(jnp.bfloat16)
            cls[h][zp, i] = rel[w, 0:1] * score_scale + jnp.log(l)

    def m_copies(up, kk, h, src_o, src_l):
        n = (M_UP if up else M_DOWN).index((kk, h))
        side = 0 if up else 1
        return [
            pltpu.make_async_remote_copy(
                src_ref=src,
                dst_ref=dst.at[side, n],
                send_sem=sm.at[i, side, n],
                recv_sem=rm.at[i, side, n],
                device_id=at_z(1 if up else -1),
                device_id_type=MESH,
            )
            for i, (src, dst) in enumerate(((src_o, ro), (src_l, rl)))
        ]

    def m_arrived(up, kk, h):
        n = (M_UP if up else M_DOWN).index((kk, h))
        side = 0 if up else 1
        for copy in m_copies(up, kk, h, ro.at[side, n], rl.at[side, n]):
            copy.wait_recv()
        return side, n

    def m_step(kk, h):
        for up in (True, False):
            table = M_UP if up else M_DOWN
            if (kk, h) not in table:
                continue
            dest = zi(kk if up else -kk)
            if (kk + 1, h) not in table:
                for copy in m_copies(up, kk, h, cos[h].at[dest], cls[h].at[dest]):
                    start(copy)
                continue
            side, prev = m_arrived(up, kk + 1, h)
            n = table.index((kk, h))
            for i in range(NS):
                val, l = merged(cos[h][dest, i], cls[h][dest, i], ro[side, prev, i], rl[side, prev, i])
                mo[side, n, i] = val.astype(jnp.bfloat16)
                ml[side, n, i] = l
            for copy in m_copies(up, kk, h, mo.at[side, n], ml.at[side, n]):
                start(copy)

    def m_begin(h):
        collect(h)
        m_step(4, h)
        for up in (True, False):
            table = M_UP if up else M_DOWN
            if (4, h) not in table:
                dest = zi(3 if up else -3)
                for copy in m_copies(up, 3, h, cos[h].at[dest], cls[h].at[dest]):
                    start(copy)

    def m_second(h):
        for up in (True, False):
            table = M_UP if up else M_DOWN
            if (4, h) in table:
                dest = zi(3 if up else -3)
                side, prev = m_arrived(up, 4, h)
                n = table.index((3, h))
                for i in range(NS):
                    val, l = merged(cos[h][dest, i], cls[h][dest, i], ro[side, prev, i], rl[side, prev, i])
                    mo[side, n, i] = val.astype(jnp.bfloat16)
                    ml[side, n, i] = l
                for copy in m_copies(up, 3, h, mo.at[side, n], ml.at[side, n]):
                    start(copy)

    def final(h, r, d):
        return pltpu.make_async_remote_copy(
            src_ref=fin.at[h, r],
            dst_ref=out.at[:, x, :, h * DH : (h + 1) * DH],
            send_sem=sx.at[h, r],
            recv_sem=rx.at[h, d],
            device_id=(r * NZ + z, hd),
            device_id_type=MESH,
        )

    rows = NS // 2

    def m_end(h):
        su, nu = m_arrived(True, 1, h)
        sd, nd = m_arrived(False, 1, h)
        for i in range(NS):
            a, la = merged(ro[su, nu, i], rl[su, nu, i], ro[sd, nd, i], rl[sd, nd, i])
            val, _ = merged(cos[h][z, i], cls[h][z, i], a, la)
            fin[h, i // 2, i % 2] = val.T.astype(jnp.bfloat16)
        for r in range(rows):

            @pl.when(x == r)
            def _(r=r):
                for u in range(2):
                    out[u, x, :, h * DH : (h + 1) * DH] = fin[h, r, u]

            for d in (1, 2, 3):

                @pl.when(lax.rem(x + d, NX) == r)
                def _(r=r, d=d):
                    final(h, r, d).start()

    @pl.when(x >= rows)
    def _():
        out[...] = jnp.zeros(out.shape, out.dtype)

    res[W_ALL] = jnp.zeros((DH, B), jnp.float32)
    rel[W_ALL, 0:1] = jnp.full((1, B), neg_big, jnp.float32)
    rel[W_ALL, 1:2] = jnp.ones((1, B), jnp.float32)
    st_o[...] = jnp.zeros((DH, B), jnp.float32)
    st_m[...] = jnp.full((1, B), neg_big, jnp.float32)
    st_l[...] = jnp.zeros((1, B), jnp.float32)

    for h in (0, 1):
        q_ready(h)
        q_begin(h)
    prepare(1)
    q_ready(2)
    q_ready(3)
    q_step(1, 0)
    q_step(1, 1)
    gathers[0].forward()
    gathers[1].own()
    prepare(2)
    prepare(3)
    q_step(2, 0)
    q_step(2, 1)
    q_step(3, 0)
    q_step(3, 1)
    q_begin(2)
    q_begin(3)
    q_step(4, 0)
    gathers[0].finish()
    chunk(0, 0)
    q_step(1, 2)
    chunk(0, 1)
    q_step(4, 1)
    gathers[1].forward()
    gathers[2].own()
    q_step(1, 3)
    chunk(0, 2)
    q_step(2, 2)
    chunk(0, 3)
    m_begin(0)
    q_step(2, 3)
    gathers[1].finish()
    chunk(1, 0)
    q_step(3, 2)
    chunk(1, 1)
    gathers[2].forward()
    gathers[3].own()
    q_step(3, 3)
    m_second(0)
    chunk(1, 2)
    q_step(4, 2)
    q_step(4, 3)
    chunk(1, 3)
    m_begin(1)
    m_step(2, 0)
    gathers[2].finish()
    chunk(2, 0)
    m_second(1)
    chunk(2, 1)
    gathers[3].forward()
    m_step(1, 0)
    m_step(2, 1)
    chunk(2, 2)
    chunk(2, 3)
    m_begin(2)
    m_step(1, 1)
    m_end(0)
    gathers[3].finish()
    chunk(3, 0)
    m_second(2)
    m_end(1)
    chunk(3, 1)
    m_step(2, 2)
    chunk(3, 2)
    chunk(3, 3)
    m_begin(3)
    m_step(1, 2)
    m_second(3)
    m_end(2)
    m_step(2, 3)
    m_step(1, 3)
    m_end(3)

    for h in range(HD):
        for r in range(rows):

            @pl.when(x == r)
            def _(h=h, r=r):
                for d in (1, 2, 3):
                    src = lax.rem(x - d + NX, NX)
                    pltpu.make_async_remote_copy(
                        src_ref=fin.at[h, r],
                        dst_ref=out.at[:, src, :, h * DH : (h + 1) * DH],
                        send_sem=sx.at[h, r],
                        recv_sem=rx.at[h, d],
                        device_id=at_x(d),
                        device_id_type=MESH,
                    ).wait_recv()

            for d in (1, 2, 3):

                @pl.when(lax.rem(x + d, NX) == r)
                def _(h=h, r=r, d=d):
                    final(h, r, d).wait_send()

    for g in gathers:
        g.close()
    for copy in sent:
        copy.wait_send()


def main_step(tq, idx, comp, items, last, q, k, v):
    dma = pltpu.SemaphoreType.DMA
    any_spec = pl.BlockSpec(memory_space=pl.ANY)
    bf, f32 = jnp.bfloat16, jnp.float32
    out = pl.pallas_call(
        functools.partial(main_kernel, tq),
        out_shape=jax.ShapeDtypeStruct((2, NX, B, HD * DH), bf),
        in_specs=[SMEM_SPEC] * 4 + [any_spec] * 3,
        out_specs=VMEM_SPEC,
        scratch_shapes=[pltpu.VMEM((NX, 2, BD, B, DH), bf)] * HD
        + [pltpu.VMEM((NX, 2, B, DH), bf)] * HD
        + [pltpu.VMEM((NZ, tq, B, DH), bf)] * HD
        + [pltpu.VMEM((NZ, NS, DH, B), bf)] * HD
        + [pltpu.VMEM((NZ, NS, 1, B), f32)] * HD
        + [
            pltpu.VMEM((BD, B, HD * DH), bf),
            pltpu.VMEM((BD * B, HD * DH), bf),
            pltpu.VMEM((BD * B, HD * DH), bf),
            pltpu.VMEM((NX, HD, 2, B, DH), bf),
            pltpu.VMEM((W_ALL + 1, DH, B), f32),
            pltpu.VMEM((W_ALL + 1, 2, B), f32),
            pltpu.VMEM((DH, B), f32),
            pltpu.VMEM((1, B), f32),
            pltpu.VMEM((1, B), f32),
            pltpu.VMEM((2, 14, NS, DH, B), bf),
            pltpu.VMEM((2, 14, NS, 1, B), f32),
            pltpu.VMEM((2, 14, NS, DH, B), bf),
            pltpu.VMEM((2, 14, NS, 1, B), f32),
            pltpu.VMEM((HD, NS // 2, 2, B, DH), bf),
        ]
        + [
            dma((3,)),
            dma((4, HD)), dma((4, HD)),
            dma((HD, 2, 2)), dma((HD, 2, 2)), dma((HD, 2, 2)), dma((HD, 2, 2)),
            dma((2, 14)), dma((2, 14)),
            dma((2, 2, 14)), dma((2, 2, 14)),
            dma((HD, NS // 2)), dma((HD, 4)),
        ],
        compiler_params=params(tq, 58),
        name="main%d" % tq,
    )(idx, comp, items, last, q, k, v)
    return out.reshape(BD * B, HD * DH)


def plan_kernel(tab, send_idx, items, counts, blk, slot):
    s, x, z, _ = place()
    blk_dev = BD
    n_blocks = NX * NZ * BD

    def one(i, carry):
        rank, used, start = carry
        home = i // blk_dev
        k = tab[home, 0, HD * blk_dev * R + lax.rem(i, blk_dev)]
        used = jnp.where(lax.rem(i, blk_dev) == 0, 0, used)
        start = jnp.where(i == s * blk_dev, rank, start)
        mine = (k > 0) & (lax.rem(rank, NX) == x)
        at = jnp.where(mine, rank // NX, 64)
        blk[at] = i
        slot[at] = lax.rem(home, NZ) * 8 + (home // NZ) * 2 + used
        return rank + k, used + jnp.where(mine, 1, 0), start

    total, _, start = lax.fori_loop(0, n_blocks, one, (0, 0, 0))

    for c in range(8):
        send_idx[c] = 0
    filled = [jnp.int32(0)] * NX
    rank = start
    for j in range(blk_dev):
        k = tab[s, 0, HD * blk_dev * R + j]
        col = lax.rem(rank, NX)
        at = jnp.int32(8)
        for c in range(NX):
            hit = (k > 0) & (col == c)
            at = jnp.where(hit, c * 2 + filled[c], at)
            filled[c] = filled[c] + jnp.where(hit, 1, 0)
        send_idx[at] = j
        rank = rank + k

    def query(a, cnt):
        i = blk[a]
        home = i // blk_dev
        base = lax.rem(i, blk_dev) * R
        pos = (lax.rem(a // 2, NZ)) * 8 + (a // 16) * 2 + lax.rem(a, 2)
        word = slot[a] * 64 + pos
        cnt = list(cnt)

        def add(h, t, ok):
            w = ((t // 64) * 8 + lax.rem(t, blk_dev)) * 4096 + word
            items[h * LCAP + cnt[h]] = w
            cnt[h] = cnt[h] + jnp.where(ok, 1, 0)

        for dt in (-1, 0, 1):
            t = i + dt
            ok = (t >= 0) & (t < n_blocks) & (lax.rem(t // blk_dev, NZ) == z)
            t = jnp.clip(t, 0, n_blocks - 1)
            for h in range(HD):
                add(h, t, ok)
        for g in range(G):
            for h in range(HD):
                add(h, jnp.int32(g), z == 0)
        for h in range(HD):
            for r in range(R):
                t = tab[home, 0, h * blk_dev * R + base + r]
                add(h, t, lax.rem(t // blk_dev, NZ) == z)
        return tuple(cnt)

    n_mine = (total - x + NX - 1) // NX
    cnt = lax.fori_loop(0, n_mine, query, (jnp.int32(0),) * HD)
    for h in range(HD):
        counts[h] = cnt[h]
        for u in range(4):
            items[h * LCAP + cnt[h] + u] = jnp.int32(64)


def planned(tab):
    return pl.pallas_call(
        plan_kernel,
        out_shape=[
            jax.ShapeDtypeStruct((16,), jnp.int32),
            jax.ShapeDtypeStruct((HD * LCAP,), jnp.int32),
            jax.ShapeDtypeStruct((8,), jnp.int32),
        ],
        in_specs=[SMEM_SPEC],
        out_specs=[SMEM_SPEC] * 3,
        scratch_shapes=[pltpu.SMEM((72,), jnp.int32), pltpu.SMEM((72,), jnp.int32)],
        compiler_params=params(None, 16),
        name="plan",
    )(tab)


RING = [(k, h) for k in (1, 2, 3) for h in range(HD)]
RING_UP = RING + [(4, 0), (4, 1)]
RING_DOWN = RING + [(4, 2), (4, 3)]


def spread_kernel(idx, q, k, v, kv, qz, qs, sx, rx, so, ro, sf, rf, su, ru, sd, rd):
    s, x, z, hd = place()

    def at_x(d):
        return (lax.rem(x + d, NX) * NZ + z, hd)

    def at_z(d):
        return (x * NZ + lax.rem(z + d + NZ, NZ), hd)

    def xi(d):
        return lax.rem(x + d + NX, NX)

    def zi(d):
        return lax.rem(z + d + NZ, NZ)

    barrier = pltpu.get_barrier_semaphore()
    for d in (1, 2, 3):
        pl.semaphore_signal(barrier, inc=1, device_id=at_x(d), device_id_type=MESH)
    for d in (1, -1):
        pl.semaphore_signal(barrier, inc=1, device_id=at_z(d), device_id_type=MESH)

    def fill(c, carry):
        col, u = c // 2, lax.rem(c, 2)
        j = idx[c]
        for h in range(HD):
            qs[col, h, u] = q[j, :, h * DH : (h + 1) * DH]
        return carry

    lax.fori_loop(0, 8, fill, 0)
    for h in range(HD):
        for u in range(2):
            qz[h, z, x, u] = qs[x, h, u]
    pl.semaphore_wait(barrier, 5)

    q_out = []
    for d in (1, 2, 3):
        copy = pltpu.make_async_remote_copy(
            src_ref=qs.at[xi(d)],
            dst_ref=qz.at[:, z, x],
            send_sem=sx.at[d],
            recv_sem=rx.at[d],
            device_id=at_x(d),
            device_id_type=MESH,
        )
        copy.start()
        q_out.append(copy)

    own = []
    for h in range(HD):

        def prep(b, carry):
            rows = pl.ds(pl.multiple_of(b * B, B), B)
            kv[h, x, 0, b] = k[rows, h * DH : (h + 1) * DH]
            kv[h, x, 1, b] = v[rows, h * DH : (h + 1) * DH].T
            return carry

        lax.fori_loop(0, BD, prep, 0)
        for side, d in ((0, 1), (1, 3)):
            copy = pltpu.make_async_remote_copy(
                src_ref=kv.at[h, x],
                dst_ref=kv.at[h, x],
                send_sem=so.at[side, h],
                recv_sem=ro.at[side, h],
                device_id=at_x(d),
                device_id_type=MESH,
            )
            copy.start()
            own.append(copy)

    for d in (1, 2, 3):
        src = xi(-d)
        pltpu.make_async_remote_copy(
            src_ref=qz.at[:, z, src],
            dst_ref=qz.at[:, z, src],
            send_sem=sx.at[d],
            recv_sem=rx.at[d],
            device_id=at_x(d),
            device_id_type=MESH,
        ).wait_recv()

    rings = []

    def ring_piece(up, n):
        kk, h = (RING_UP if up else RING_DOWN)[n]
        step = -1 if up else 1
        row = zi(step * (kk - 1))
        return pltpu.make_async_remote_copy(
            src_ref=qz.at[h, row],
            dst_ref=qz.at[h, row],
            send_sem=(su if up else sd).at[n],
            recv_sem=(ru if up else rd).at[n],
            device_id=at_z(1 if up else -1),
            device_id_type=MESH,
        )

    def ring_arrival(up, n):
        kk, h = (RING_UP if up else RING_DOWN)[n]
        row = zi((-1 if up else 1) * kk)
        return pltpu.make_async_remote_copy(
            src_ref=qz.at[h, row],
            dst_ref=qz.at[h, row],
            send_sem=(su if up else sd).at[n],
            recv_sem=(ru if up else rd).at[n],
            device_id=at_z(1 if up else -1),
            device_id_type=MESH,
        )

    for n in range(4):
        for up in (True, False):
            copy = ring_piece(up, n)
            copy.start()
            rings.append(copy)

    fwd = []

    def forward_x(h):
        for side, d, part in ((0, 1, 0), (1, 3, 1)):
            src = xi(-d)
            pltpu.make_async_remote_copy(
                src_ref=kv.at[h, src],
                dst_ref=kv.at[h, src],
                send_sem=so.at[side, h],
                recv_sem=ro.at[side, h],
                device_id=at_x(d),
                device_id_type=MESH,
            ).wait_recv()
            copy = pltpu.make_async_remote_copy(
                src_ref=kv.at[h, src, part],
                dst_ref=kv.at[h, src, part],
                send_sem=sf.at[side, h],
                recv_sem=rf.at[side, h],
                device_id=at_x(d),
                device_id_type=MESH,
            )
            copy.start()
            fwd.append(copy)

    for n in range(14):
        for up in (True, False):
            kk, h = (RING_UP if up else RING_DOWN)[n]
            ring_arrival(up, n).wait_recv()
            table = RING_UP if up else RING_DOWN
            if (kk + 1, h) in table:
                copy = ring_piece(up, table.index((kk + 1, h)))
                copy.start()
                rings.append(copy)
        if n % 2 == 1 and n // 2 < HD:
            forward_x(n // 2)

    far = xi(2)
    for h in range(HD):
        for side, d, part in ((0, 1, 0), (1, 3, 1)):
            pltpu.make_async_remote_copy(
                src_ref=kv.at[h, far, part],
                dst_ref=kv.at[h, far, part],
                send_sem=sf.at[side, h],
                recv_sem=rf.at[side, h],
                device_id=at_x(d),
                device_id_type=MESH,
            ).wait_recv()
    for copy in q_out + own + rings + fwd:
        copy.wait_send()


def spread_all(idx, q, k, v):
    dma = pltpu.SemaphoreType.DMA
    return pl.pallas_call(
        spread_kernel,
        out_shape=[
            jax.ShapeDtypeStruct((HD, NX, 2, BD, B, DH), jnp.bfloat16),
            jax.ShapeDtypeStruct((HD, NZ, NX, 2, B, DH), jnp.bfloat16),
        ],
        in_specs=[SMEM_SPEC] + [VMEM_SPEC] * 3,
        out_specs=[VMEM_SPEC] * 2,
        scratch_shapes=[
            pltpu.VMEM((NX, HD, 2, B, DH), jnp.bfloat16),
            dma((4,)),
            dma((4,)),
            dma((2, HD)),
            dma((2, HD)),
            dma((2, HD)),
            dma((2, HD)),
            dma((14,)),
            dma((14,)),
            dma((14,)),
            dma((14,)),
        ],
        compiler_params=params(2),
        name="spread",
    )(idx, q, k, v)


UNROLL = 4


def part_kernel(ns, items, counts, kv, qz, out, lse, acc, top, den):
    h = pl.program_id(0)
    n_acc = NZ * ns

    def clear(a, carry):
        acc[a] = jnp.zeros((DH, B), jnp.float32)
        top[a] = jnp.full((1, B), neg_big, jnp.float32)
        den[a] = jnp.zeros((1, B), jnp.float32)
        return carry

    lax.fori_loop(0, n_acc + 1, clear, 0)

    def batch(n, carry):
        found = []
        for u in range(UNROLL):
            w = items[h * LCAP + n * UNROLL + u]
            pos = lax.rem(w, 64)
            a = (pos // 8) * ns + lax.rem(pos, 8)
            a = jnp.where(n * UNROLL + u < counts[h], a, n_acc)
            spot = lax.rem(w // 64, 64)
            tile = w // 4096
            keys = kv[0, tile // 8, 0, lax.rem(tile, 8)]
            vals = kv[0, tile // 8, 1, lax.rem(tile, 8)]
            qt = qz[0, spot // 8, lax.rem(spot, 8) // 2, lax.rem(spot, 2)]
            scores = lax.dot_general(
                keys, qt, (((1,), (1,)), ((), ())), preferred_element_type=jnp.float32
            )
            scores = scores * score_scale
            m = jnp.max(scores, axis=0, keepdims=True)
            p = jnp.exp(scores - m).astype(jnp.bfloat16)
            l = jnp.sum(p.astype(jnp.float32), axis=0, keepdims=True)
            o = jnp.dot(vals, p, preferred_element_type=jnp.float32)
            found.append((a, m, l, o))
        for a, m, l, o in found:
            old = top[a]
            new = jnp.maximum(old, m)
            f0, f1 = jnp.exp(old - new), jnp.exp(m - new)
            acc[a] = acc[a] * f0 + o * f1
            den[a] = den[a] * f0 + l * f1
            top[a] = new
        return carry

    lax.fori_loop(0, (counts[h] + UNROLL - 1) // UNROLL, batch, 0)

    def finish(a, carry):
        l = den[a]
        some = l > 0
        safe = jnp.where(some, l, 1.0)
        out[0, a // ns, lax.rem(a, ns)] = (acc[a] / safe).astype(jnp.bfloat16)
        lse[0, a // ns, lax.rem(a, ns)] = jnp.where(some, top[a] + jnp.log(safe), neg_big)
        return carry

    lax.fori_loop(0, n_acc, finish, 0)


def parts_of(ns, items, counts, kv, qz):
    n_acc = NZ * ns
    return pl.pallas_call(
        functools.partial(part_kernel, ns),
        grid=(HD,),
        out_shape=[
            jax.ShapeDtypeStruct((HD, NZ, ns, DH, B), jnp.bfloat16),
            jax.ShapeDtypeStruct((HD, NZ, ns, 1, B), jnp.float32),
        ],
        in_specs=[
            SMEM_SPEC,
            SMEM_SPEC,
            pl.BlockSpec((1, NX, 2, BD, B, DH), lambda h: (h, 0, 0, 0, 0, 0)),
            pl.BlockSpec((1, NZ, NX, 2, B, DH), lambda h: (h, 0, 0, 0, 0, 0)),
        ],
        out_specs=[
            pl.BlockSpec((1, NZ, ns, DH, B), lambda h: (h, 0, 0, 0, 0)),
            pl.BlockSpec((1, NZ, ns, 1, B), lambda h: (h, 0, 0, 0, 0)),
        ],
        scratch_shapes=[
            pltpu.VMEM((n_acc + 1, DH, B), jnp.float32),
            pltpu.VMEM((n_acc + 1, 1, B), jnp.float32),
            pltpu.VMEM((n_acc + 1, 1, B), jnp.float32),
        ],
        compiler_params=params(None, 40),
        name="parts",
    )(items, counts, kv, qz)


HOME_UP = [(4, 2), (4, 3)] + [(k, h) for k in (3, 2, 1) for h in range(HD)]
HOME_DOWN = [(4, 0), (4, 1)] + [(k, h) for k in (3, 2, 1) for h in range(HD)]


def merged(o0, l0, o1, l1):
    top = jnp.maximum(l0, l1)
    f0, f1 = jnp.exp(l0 - top), jnp.exp(l1 - top)
    both = f0 + f1
    o = (o0.astype(jnp.float32) * f0 + o1.astype(jnp.float32) * f1) / both
    return o, top + jnp.log(both)


def join_kernel(
    ns, o, lse, out, sou, slu, rou, rlu, sod, sld, rod, rld, fin, ssu, rsu, ssd, rsd, sx, rx
):
    s, x, z, hd = place()

    def at_x(d):
        return (lax.rem(x + d, NX) * NZ + z, hd)

    def at_z(d):
        return (x * NZ + lax.rem(z + d + NZ, NZ), hd)

    def zi(d):
        return lax.rem(z + d + NZ, NZ)

    barrier = pltpu.get_barrier_semaphore()
    for d in (1, 2, 3):
        pl.semaphore_signal(barrier, inc=1, device_id=at_x(d), device_id_type=MESH)
    for d in (1, -1):
        pl.semaphore_signal(barrier, inc=1, device_id=at_z(d), device_id_type=MESH)
    pl.semaphore_wait(barrier, 5)

    sent = []

    def copies(up, n, src_o, src_l):
        ro, rl = (rou, rlu) if up else (rod, rld)
        ss, rs = (ssu, rsu) if up else (ssd, rsd)
        return [
            pltpu.make_async_remote_copy(
                src_ref=src,
                dst_ref=dst.at[n],
                send_sem=ss.at[i, n],
                recv_sem=rs.at[i, n],
                device_id=at_z(1 if up else -1),
                device_id_type=MESH,
            )
            for i, (src, dst) in enumerate(((src_o, ro), (src_l, rl)))
        ]

    def send(up, n, src_o, src_l):
        for copy in copies(up, n, src_o, src_l):
            copy.start()
            sent.append(copy)

    def arrived(up, n):
        ro, rl = (rou, rlu) if up else (rod, rld)
        for copy in copies(up, n, ro.at[n], rl.at[n]):
            copy.wait_recv()

    for n in range(14):
        for up in (True, False):
            table = HOME_UP if up else HOME_DOWN
            kk, h = table[n]
            dest = zi(kk if up else -kk)
            if (kk + 1, h) not in table:
                send(up, n, o.at[h, dest], lse.at[h, dest])
                continue
            prev = table.index((kk + 1, h))
            arrived(up, prev)
            ro, rl = (rou, rlu) if up else (rod, rld)
            so, sl = (sou, slu) if up else (sod, sld)

            def step(i, carry, ro=ro, rl=rl, so=so, sl=sl, prev=prev, n=n, h=h, dest=dest):
                val, l = merged(o[h, dest, i], lse[h, dest, i], ro[prev, i], rl[prev, i])
                so[n, i] = val.astype(jnp.bfloat16)
                sl[n, i] = l
                return carry

            lax.fori_loop(0, ns, step, 0)
            send(up, n, so.at[n], sl.at[n])

    for h in range(HD):
        n = 10 + h
        arrived(True, n)
        arrived(False, n)

        def last(i, carry, h=h, n=n):
            a, la = merged(rou[n, i], rlu[n, i], rod[n, i], rld[n, i])
            val, _ = merged(o[h, z, i], lse[h, z, i], a, la)
            fin[i // 2, lax.rem(i, 2), :, h * DH : (h + 1) * DH] = val.T.astype(jnp.bfloat16)
            return carry

        lax.fori_loop(0, ns, last, 0)

    rows = ns // 2
    for r in range(NX):
        if r >= rows:

            @pl.when(x == r)
            def _():
                out[...] = jnp.zeros(out.shape, out.dtype)

            continue

        @pl.when(x == r)
        def _(r=r):
            out[:, x] = fin[r]

    def final(r, d):
        return pltpu.make_async_remote_copy(
            src_ref=fin.at[r],
            dst_ref=out.at[:, x],
            send_sem=sx.at[r],
            recv_sem=rx.at[d],
            device_id=(r * NZ + z, hd),
            device_id_type=MESH,
        )

    for d in (1, 2, 3):
        for r in range(rows):

            @pl.when(lax.rem(x + d, NX) == r)
            def _(r=r, d=d):
                final(r, d).start()

    for r in range(rows):

        @pl.when(x == r)
        def _(r=r):
            for d in (1, 2, 3):
                src = lax.rem(x - d + NX, NX)
                pltpu.make_async_remote_copy(
                    src_ref=fin.at[r],
                    dst_ref=out.at[:, src],
                    send_sem=sx.at[r],
                    recv_sem=rx.at[d],
                    device_id=at_x(d),
                    device_id_type=MESH,
                ).wait_recv()

    for d in (1, 2, 3):
        for r in range(rows):

            @pl.when(lax.rem(x + d, NX) == r)
            def _(r=r, d=d):
                final(r, d).wait_send()

    for copy in sent:
        copy.wait_send()


def joined(ns, o, lse):
    dma = pltpu.SemaphoreType.DMA
    piece_o = pltpu.VMEM((14, ns, DH, B), jnp.bfloat16)
    piece_l = pltpu.VMEM((14, ns, 1, B), jnp.float32)
    out = pl.pallas_call(
        functools.partial(join_kernel, ns),
        out_shape=jax.ShapeDtypeStruct((2, NX, B, HD * DH), jnp.bfloat16),
        in_specs=[VMEM_SPEC] * 2,
        out_specs=VMEM_SPEC,
        scratch_shapes=[
            piece_o, piece_l, piece_o, piece_l, piece_o, piece_l, piece_o, piece_l,
            pltpu.VMEM((ns // 2, 2, B, HD * DH), jnp.bfloat16),
            dma((2, 14)), dma((2, 14)), dma((2, 14)), dma((2, 14)),
            dma((4,)), dma((4,)),
        ],
        compiler_params=params(3, 56),
        name="join%d" % ns,
    )(o, lse)
    return out.reshape(BD * B, HD * DH)


def body(queries, keys, values, random_holder, random_offset, keep):
    want = random_holder * BD + random_offset
    row = jnp.concatenate([want.reshape(-1), keep, jnp.zeros((24,), jnp.int32)])
    tab = gathered_table(row.reshape(1, 128))
    q = queries.reshape(BD, B, HD * DH)
    idx, comp, items, last, flag = fast_planned(tab)

    def fast(tq):
        def run(idx, comp, items, last, tab, q, keys, values):
            return main_step(tq, idx, comp, items, last, q, keys, values)

        return run

    def wide(idx, comp, items, last, tab, q, keys, values):
        send_idx, items, counts = planned(tab)
        kv, qz = spread_all(send_idx, q, keys, values)
        return joined(8, *parts_of(8, items, counts, kv, qz))

    return lax.switch(
        flag[0], (wide, fast(6), fast(5)), idx, comp, items, last, tab, q, keys, values
    )


def solution(mesh):
    in_specs = (
        P("seq", "head"),
        P("seq", "head"),
        P("seq", "head"),
        P("head", "seq", None),
        P("head", "seq", None),
        P("seq"),
    )
    out_specs = P("seq", "head")
    return jax.shard_map(body, mesh=mesh, in_specs=in_specs, out_specs=out_specs, check_vma=False)
```

```python
import math

import jax
import jax.numpy as jnp
from jax import lax
from jax.experimental import pallas as pl
from jax.experimental.pallas import tpu as pltpu
from jax.sharding import PartitionSpec as P

DH = 128
B = 128
G = 2
R = 3
NX = 4
NZ = 8
HD = 4
BD = 8
TQ = 6
NS = 4
UN = 8
W_ANY = 128
W_ALL = 192
STEP = 32 * NX

neg_big = -1e30
MESH = pl.DeviceIdType.MESH
SMEM_SPEC = pl.BlockSpec(memory_space=pltpu.SMEM)
VMEM_SPEC = pl.BlockSpec(memory_space=pltpu.VMEM)
score_scale = 1.0 / math.sqrt(DH)


def place():
    s = lax.axis_index("seq")
    return s, s // NZ, lax.rem(s, NZ), lax.axis_index("head")


def to_seq(s, h):
    return (s, h)


def params(cid=None, mib=48):
    if cid is None:
        return pltpu.CompilerParams(vmem_limit_bytes=mib << 20)
    return pltpu.CompilerParams(
        collective_id=cid, has_side_effects=True, vmem_limit_bytes=mib << 20
    )


class RowGather:
    def __init__(self, kv, sems, x, z, hd):
        self.kv, self.sems, self.x, self.z, self.hd = kv, sems, x, z, hd
        self.sent = []

    def piece(self, which, side, part, holder):
        sk, rk, sf, rf = self.sems
        ss, rs = (sk, rk) if which == 0 else (sf, rf)
        d = 1 if side == 0 else 3
        return pltpu.make_async_remote_copy(
            src_ref=self.kv.at[holder, part],
            dst_ref=self.kv.at[holder, part],
            send_sem=ss.at[side, part],
            recv_sem=rs.at[side, part],
            device_id=(lax.rem(self.x + d, NX) * NZ + self.z, self.hd),
            device_id_type=MESH,
        )

    def start(self, copy):
        copy.start()
        self.sent.append(copy)

    def own(self):
        for order in (0, 1):
            for side in (0, 1):
                self.start(self.piece(0, side, order ^ side, self.x))

    def neighbour(self, side):
        return lax.rem(self.x + (3 if side == 0 else 1), NX)

    def forward(self):
        for side in (0, 1):
            self.piece(0, side, side, self.neighbour(side)).wait_recv()
            self.start(self.piece(1, side, side, self.neighbour(side)))

    def finish(self):
        for side in (0, 1):
            self.piece(0, side, 1 - side, self.neighbour(side)).wait_recv()
        for side in (0, 1):
            self.piece(1, side, side, lax.rem(self.x + 2, NX)).wait_recv()

    def close(self):
        for copy in self.sent:
            copy.wait_send()


def merged(o0, l0, o1, l1):
    top = jnp.maximum(l0, l1)
    f0, f1 = jnp.exp(l0 - top), jnp.exp(l1 - top)
    both = f0 + f1
    o = (o0.astype(jnp.float32) * f0 + o1.astype(jnp.float32) * f1) / both
    return o, top + jnp.log(both)


def plan(tab, window, part, s, x, z, sendm, lastm, itemm, info):
    n_home, wide = NX * NZ, 128
    flags = HD * BD * R
    f32, i32, bf = jnp.float32, jnp.int32, jnp.bfloat16

    def iota(rows, cols, axis):
        return lax.broadcasted_iota(i32, (rows, cols), axis)

    def times(a, b):
        return jnp.dot(a.astype(bf), b.astype(bf), preferred_element_type=f32)

    t = tab[:, 0, :]
    lane = iota(n_home, wide, 1)
    home = iota(n_home, wide, 0)
    kept = jnp.where((lane >= flags) & (lane < flags + BD), t, 0).astype(f32)
    in_row = times(kept, (iota(wide, wide, 0) < iota(wide, wide, 1)).astype(f32))
    count = jnp.broadcast_to(jnp.sum(kept, axis=1, keepdims=True), (n_home, wide))
    upper = times(iota(n_home, n_home, 1) < iota(n_home, n_home, 0), count)
    ranks = (in_row + upper).astype(i32)
    first_rank = upper.astype(i32)

    most = jnp.zeros((NZ, 1), f32)
    for c in range(NX):
        n = jnp.sum(jnp.where((ranks & (NX - 1)) == c, kept, 0.0), axis=1, keepdims=True)
        most = jnp.maximum(most, n[0:8] + n[8:16] + n[16:24] + n[24:32])
    most = jnp.max(most, axis=0, keepdims=True)
    total = jnp.sum(count[:, 0:1], axis=0, keepdims=True)
    row8 = iota(8, wide, 0)
    info[...] = jnp.where(
        row8 == 0, jnp.broadcast_to(total, (8, wide)), jnp.broadcast_to(most, (8, wide))
    ).astype(i32)

    row, line = home & (NZ - 1), home >> 3
    blocks = []
    mine_count = jnp.zeros((n_home, wide), f32)
    for b in range(BD):
        at = flags + b
        k = jnp.broadcast_to(kept[:, at : at + 1], (n_home, wide)) > 0
        r = jnp.broadcast_to(ranks[:, at : at + 1], (n_home, wide))
        here = k & ((r >> 7) == window)
        turn = jnp.where(((r - first_rank) >= 4) & (((r - 4) >> 7) == window), 1, 0)
        mine = here & ((r & (NX - 1)) == x)
        blocks.append((r, here, turn, mine))
        mine_count = mine_count + jnp.where(mine, 1.0, 0.0)
    same_row = (iota(n_home, n_home, 0) & (NZ - 1)) == (iota(n_home, n_home, 1) & (NZ - 1))
    cell = times(same_row & (iota(n_home, n_home, 1) < iota(n_home, n_home, 0)), mine_count)
    cell = cell.astype(i32) - part * TQ

    send = jnp.zeros((n_home, wide), i32)
    take = jnp.zeros((n_home, wide), i32)
    hots, data = [], []
    for b, (r, here, turn, mine) in enumerate(blocks):
        send = send + jnp.where(here & (lane == (r & (NX - 1)) * 2 + turn), b, 0)
        chosen = mine & (cell >= 0) & (cell < TQ)
        take = take + jnp.where(chosen & (row == z) & (lane == cell), line * 2 + turn, 0)
        hots.append(jnp.where(chosen & (((r >> 2) & 31) == lane), 1.0, 0.0))
        moved = t if b == 0 else pltpu.roll(t, wide - R * b, 1)
        moved = jnp.where(lane == 120, home * BD + b, moved)
        moved = jnp.where(lane == 121, row * 8 + cell, moved)
        data.append(jnp.where(lane == 122, 1, moved).astype(f32))
        cell = cell + jnp.where(mine, 1, 0)
    sendm[...] = send
    take = jnp.sum(take.astype(f32), axis=0, keepdims=True).astype(i32)

    hot = jnp.concatenate(hots, axis=0).astype(bf)
    known = jnp.concatenate(data, axis=0).astype(bf)
    of = lax.dot_general(hot, known, (((0,), (0,)), ((), ())), preferred_element_type=f32)
    of = of[:32]

    src, to = iota(wide, wide, 0), iota(wide, wide, 1)
    kind = to & 7
    wanted = jnp.where(kind < 3, 120, jnp.where(kind < 5, -1, (to >> 3) * (BD * R) + kind - 5))
    tile = times(of, (src == wanted).astype(f32)).astype(i32)
    spot = times(of, (src == 121).astype(f32)).astype(i32)
    valid = times(of, (src == 122).astype(f32)) > 0.5
    m = iota(32, wide, 1)
    kind = m & 7
    tile = tile + jnp.where(kind < 3, kind - 1, jnp.where(kind < 5, kind - 3, 0))
    ok = valid & (m < 32) & (tile >= 0) & (tile < n_home * BD)
    ok = ok & (((tile >> 3) & (NZ - 1)) == z)
    hit = jnp.where(ok, 1.0, 0.0)
    word = spot + ((((tile >> 6) & 3) * 8) + (tile & 7)) * 64
    same_head = (src >> 3) == (to >> 3)
    ahead = times(hit, (same_head & (src < to)).astype(f32))
    whole = times(hit, same_head.astype(f32))
    above = times(
        times(iota(32, 32, 1) < iota(32, 32, 0), hit), same_head.astype(f32)
    )
    order = jnp.where(ok, (ahead + above).astype(i32), -1)
    word = word + jnp.where(ahead < 0.5, 1 << 20, 0)
    lastm[...] = jnp.where(whole > 0.5, (above + whole).astype(i32) - 1, W_ALL)

    slots = iota(32, 2 * wide, 1)
    for h in range(HD):
        found = jnp.zeros((32, 2 * wide), i32)
        for k in range(8):
            c = h * 8 + k
            spots = jnp.broadcast_to(order[:, c : c + 1], (32, 2 * wide))
            words = jnp.broadcast_to(word[:, c : c + 1], (32, 2 * wide))
            found = found + jnp.where(spots == slots, words, 0)
        found = (found[0:8] + found[8:16]) + (found[16:24] + found[24:32])
        found = found[0:4] + found[4:8]
        found = found[0:2] + found[2:4]
        itemm[h : h + 1] = found[0:1] + found[1:2]
    itemm[4:5] = jnp.concatenate([take, take], axis=1)


EXP2 = score_scale * math.log2(math.e)
Q_UP = [(k, h) for h in range(HD) for k in (1, 2, 3)] + [(4, 0), (4, 2)]
Q_DOWN = [(k, h) for h in range(HD) for k in (1, 2, 3)] + [(4, 1), (4, 3)]
M_UP = [(k, h) for h in range(HD) for k in (3, 2, 1)] + [(4, 1), (4, 3)]
M_DOWN = [(k, h) for h in range(HD) for k in (3, 2, 1)] + [(4, 0), (4, 2)]


def main_kernel(turn, table_row, q_any, k_any, v_any, out, info, *rest):
    kvs, qrs, qzs, cos, cls = rest[0:4], rest[4:8], rest[8:12], rest[12:16], rest[16:20]
    (qv, kbuf, vbuf, qs, sc, res, rel, st_o, st_m, st_l, mo, ml, ro, rl, fin) = rest[20:35]
    (tab, sendm, lastm, itemm, sends, lasts, items) = rest[35:42]
    (load, stab, rtab, sqx, rqx, skv, rkv, sfw, rfw, sq, rq, sm, rm, sx, rx) = rest[42:]
    s, x, z, hd = place()
    n_seq = NX * NZ

    def at_x(d):
        return (lax.rem(x + d, NX) * NZ + z, hd)

    def at_z(d):
        return (x * NZ + lax.rem(z + d + NZ, NZ), hd)

    def xi(d):
        return lax.rem(x + d + NX, NX)

    def zi(d):
        return lax.rem(z + d + NZ, NZ)

    loads = [
        pltpu.make_async_copy(src, dst, load.at[i])
        for i, (src, dst) in enumerate(((q_any, qv), (k_any, kbuf), (v_any, vbuf)))
    ]
    for copy in loads:
        copy.start()
    barrier = pltpu.get_barrier_semaphore()
    for d in range(1, n_seq):
        pl.semaphore_signal(
            barrier, inc=1, device_id=(lax.rem(s + d, n_seq), hd), device_id_type=MESH
        )
    tab[s] = table_row[...]
    loads[1].wait()
    loads[2].wait()

    sent = []

    def start(copy):
        copy.start()
        sent.append(copy)

    gathers = []
    for h in range(HD):
        g = RowGather(kvs[h], (skv.at[h], rkv.at[h], sfw.at[h], rfw.at[h]), x, z, hd)
        gathers.append(g)

    def prepare(h):
        def prep(b, carry):
            rows = pl.ds(pl.multiple_of(b * B, B), B)
            kvs[h][x, 0, b] = kbuf[rows, h * DH : (h + 1) * DH]
            kvs[h][x, 1, b] = vbuf[rows, h * DH : (h + 1) * DH].T
            return carry

        lax.fori_loop(0, BD, prep, 0)


    prepare(0)
    pl.semaphore_wait(barrier, n_seq - 1)
    gathers[0].own()
    rows_out = []
    for d in range(1, n_seq):
        copy = pltpu.make_async_remote_copy(
            src_ref=table_row,
            dst_ref=tab.at[s],
            send_sem=stab.at[d],
            recv_sem=rtab.at[d],
            device_id=(lax.rem(s + d, n_seq), hd),
            device_id_type=MESH,
        )
        copy.start()
        rows_out.append(copy)
    prepare(1)
    for copy in rows_out:
        copy.wait()
    plan(tab, turn[0], turn[1], s, x, z, sendm, lastm, itemm, info)
    lists = [
        pltpu.make_async_copy(src, dst, load.at[3 + i])
        for i, (src, dst) in enumerate(((sendm, sends), (itemm, items), (lastm, lasts)))
    ]
    for copy in lists:
        copy.start()
    loads[0].wait()
    for copy in lists:
        copy.wait()

    def fill(c, carry):
        col, u = c // 2, lax.rem(c, 2)
        j = sends[s, c] & (BD - 1)
        for h in range(HD):
            qs[col, h, u] = qv[j, :, h * DH : (h + 1) * DH]
        return carry

    lax.fori_loop(0, 8, fill, 0)
    for h in range(HD):
        for u in range(2):
            qrs[h][x, u] = qs[x, h, u]

    def q_move(h, d, src):
        return pltpu.make_async_remote_copy(
            src_ref=qs.at[src, h],
            dst_ref=qrs[h].at[x],
            send_sem=sqx.at[d, h],
            recv_sem=rqx.at[d, h],
            device_id=at_x(d),
            device_id_type=MESH,
        )

    def q_leave(h):
        for d in (1, 3, 2):
            start(q_move(h, d, xi(d)))

    q_leave(0)
    q_leave(1)

    def q_copy(up, kk, h, row):
        n = (Q_UP if up else Q_DOWN).index((kk, h))
        return pltpu.make_async_remote_copy(
            src_ref=qzs[h].at[row],
            dst_ref=qzs[h].at[row],
            send_sem=sq.at[0 if up else 1, n],
            recv_sem=rq.at[0 if up else 1, n],
            device_id=at_z(1 if up else -1),
            device_id_type=MESH,
        )

    def q_send(up, kk, h):
        if (kk, h) in (Q_UP if up else Q_DOWN):
            start(q_copy(up, kk, h, zi((-1 if up else 1) * (kk - 1))))

    def q_ready(h):
        for d in (1, 2, 3):
            src = xi(-d)
            pltpu.make_async_remote_copy(
                src_ref=qrs[h].at[src],
                dst_ref=qrs[h].at[src],
                send_sem=sqx.at[d, h],
                recv_sem=rqx.at[d, h],
                device_id=at_x(d),
                device_id_type=MESH,
            ).wait_recv()
        for c in range(TQ):
            w = items[4, c]
            qzs[h][z, c] = qrs[h][(w >> 1) & 3, w & 1]

    def q_begin(h):
        for up in (True, False):
            q_send(up, 1, h)

    def q_step(kk, h):
        for up in (True, False):
            if (kk, h) in (Q_UP if up else Q_DOWN):
                q_copy(up, kk, h, zi((-1 if up else 1) * kk)).wait_recv()
                q_send(up, kk + 1, h)

    nb = jnp.where(z == 0, W_ALL // UN // 4, W_ANY // UN // 4)

    def chunk(h, part):
        kv, qz = kvs[h], qzs[h]

        def words_of(n):
            return [items[h, n * UN + u] for u in range(UN)]

        def score(words):
            for u, w in enumerate(words):
                spot, tile = w & 63, (w >> 6) & 31
                sc[u] = lax.dot_general(
                    kv[tile >> 3, 0, tile & 7],
                    qz[spot >> 3, jnp.minimum(spot & 7, TQ - 1)],
                    (((1,), (1,)), ((), ())),
                    preferred_element_type=jnp.float32,
                )

        def batch(n, carry):
            m0, l0, o0 = st_m[...], st_l[...], st_o[...]
            words = words_of(n)
            scores = [sc[u] for u in range(UN)]
            tops, weights = [], []
            for val in scores:
                raw = jnp.max(val, axis=0, keepdims=True)
                tops.append(raw)
                weights.append(jnp.exp2((val - raw) * EXP2).astype(jnp.bfloat16))
            sums = []
            for w, p in zip(words, weights):
                tile = (w >> 6) & 31
                rows = jnp.concatenate([kv[tile >> 3, 1, tile & 7], ones], axis=0)
                sums.append(jnp.dot(rows, p, preferred_element_type=jnp.float32))
            score(words_of(n + 1))
            for u, w in enumerate(words):
                old = jnp.where((w >> 20) > 0, neg_big, m0)
                top = jnp.maximum(old, tops[u])
                f0, f1 = jnp.exp2((old - top) * EXP2), jnp.exp2((tops[u] - top) * EXP2)
                m0 = top
                l0 = l0 * f0 + sums[u][DH : DH + 1] * f1
                o0 = o0 * f0 + sums[u][:DH] * f1
                at = n * UN + u
                res[at] = o0
                rel[at] = jnp.concatenate([m0, l0], axis=0)
            st_m[...], st_l[...], st_o[...] = m0, l0, o0
            return carry

        ones = jnp.ones((16, B), jnp.bfloat16)
        if part == 0:
            score(words_of(0))
        lax.fori_loop(part * nb, (part + 1) * nb, batch, 0)

    def collect(h):
        for a in range(NZ * NS):
            w = jnp.clip(lasts[a, h * 8], 0, W_ALL)
            zp, i = (a >> 1) & 7, (a >> 4) * 2 + (a & 1)
            l = rel[w, 1:2]
            cos[h][zp, i] = (res[w] * (1.0 / l)).astype(jnp.bfloat16)
            cls[h][zp, i] = rel[w, 0:1] * score_scale + jnp.log(l)

    def m_copies(up, kk, h, src_o, src_l):
        n = (M_UP if up else M_DOWN).index((kk, h))
        side = 0 if up else 1
        return [
            pltpu.make_async_remote_copy(
                src_ref=src,
                dst_ref=dst.at[side, n],
                send_sem=sm.at[i, side, n],
                recv_sem=rm.at[i, side, n],
                device_id=at_z(1 if up else -1),
                device_id_type=MESH,
            )
            for i, (src, dst) in enumerate(((src_o, ro), (src_l, rl)))
        ]

    def m_arrived(up, kk, h):
        n = (M_UP if up else M_DOWN).index((kk, h))
        side = 0 if up else 1
        for copy in m_copies(up, kk, h, ro.at[side, n], rl.at[side, n]):
            copy.wait_recv()
        return side, n

    def m_step(kk, h):
        for up in (True, False):
            table = M_UP if up else M_DOWN
            if (kk, h) not in table:
                continue
            dest = zi(kk if up else -kk)
            if (kk + 1, h) not in table:
                for copy in m_copies(up, kk, h, cos[h].at[dest], cls[h].at[dest]):
                    start(copy)
                continue
            side, prev = m_arrived(up, kk + 1, h)
            n = table.index((kk, h))
            for i in range(NS):
                val, l = merged(cos[h][dest, i], cls[h][dest, i], ro[side, prev, i], rl[side, prev, i])
                mo[side, n, i] = val.astype(jnp.bfloat16)
                ml[side, n, i] = l
            for copy in m_copies(up, kk, h, mo.at[side, n], ml.at[side, n]):
                start(copy)

    def m_begin(h):
        m_step(4, h)
        for up in (True, False):
            table = M_UP if up else M_DOWN
            if (4, h) not in table:
                dest = zi(3 if up else -3)
                for copy in m_copies(up, 3, h, cos[h].at[dest], cls[h].at[dest]):
                    start(copy)

    def m_second(h):
        for up in (True, False):
            table = M_UP if up else M_DOWN
            if (4, h) in table:
                dest = zi(3 if up else -3)
                side, prev = m_arrived(up, 4, h)
                n = table.index((3, h))
                for i in range(NS):
                    val, l = merged(cos[h][dest, i], cls[h][dest, i], ro[side, prev, i], rl[side, prev, i])
                    mo[side, n, i] = val.astype(jnp.bfloat16)
                    ml[side, n, i] = l
                for copy in m_copies(up, 3, h, mo.at[side, n], ml.at[side, n]):
                    start(copy)

    def final(h, r, d):
        return pltpu.make_async_remote_copy(
            src_ref=fin.at[h, r],
            dst_ref=out.at[:, x, :, h * DH : (h + 1) * DH],
            send_sem=sx.at[h, r],
            recv_sem=rx.at[h, d],
            device_id=(r * NZ + z, hd),
            device_id_type=MESH,
        )

    rows = NS // 2

    def m_end(h):
        su, nu = m_arrived(True, 1, h)
        sd, nd = m_arrived(False, 1, h)
        for i in range(NS):
            a, la = merged(ro[su, nu, i], rl[su, nu, i], ro[sd, nd, i], rl[sd, nd, i])
            val, _ = merged(cos[h][z, i], cls[h][z, i], a, la)
            fin[h, i // 2, i % 2] = val.T.astype(jnp.bfloat16)
        for r in range(rows):

            @pl.when(x == r)
            def _(r=r):
                for u in range(2):
                    out[u, x, :, h * DH : (h + 1) * DH] = fin[h, r, u]

            for d in (1, 2, 3):

                @pl.when(lax.rem(x + d, NX) == r)
                def _(r=r, d=d):
                    final(h, r, d).start()

    @pl.when(x >= rows)
    def _():
        out[...] = jnp.zeros(out.shape, out.dtype)

    res[W_ALL] = jnp.zeros((DH, B), jnp.float32)
    rel[W_ALL, 0:1] = jnp.full((1, B), neg_big, jnp.float32)
    rel[W_ALL, 1:2] = jnp.ones((1, B), jnp.float32)
    st_o[...] = jnp.zeros((DH, B), jnp.float32)
    st_m[...] = jnp.full((1, B), neg_big, jnp.float32)
    st_l[...] = jnp.zeros((1, B), jnp.float32)

    gathers[0].forward()
    gathers[1].own()
    q_ready(0)
    q_begin(0)
    q_ready(1)
    q_begin(1)
    q_leave(2)
    q_leave(3)
    q_step(1, 0)
    prepare(2)
    q_step(1, 1)
    prepare(3)
    q_step(2, 0)
    gathers[1].forward()
    gathers[2].own()
    q_step(2, 1)
    q_step(3, 0)
    q_ready(2)
    q_step(3, 1)
    q_begin(2)
    q_ready(3)
    q_begin(3)
    q_step(4, 0)
    gathers[0].finish()
    chunk(0, 0)
    q_step(4, 1)
    q_step(1, 2)
    chunk(0, 1)
    gathers[2].forward()
    gathers[3].own()
    q_step(1, 3)
    chunk(0, 2)
    q_step(2, 2)
    chunk(0, 3)
    collect(0)
    gathers[1].finish()
    q_step(2, 3)
    chunk(1, 0)
    q_step(3, 2)
    gathers[3].forward()
    chunk(1, 1)
    q_step(3, 3)
    m_begin(0)
    chunk(1, 2)
    q_step(4, 2)
    chunk(1, 3)
    collect(1)
    m_begin(1)
    q_step(4, 3)
    gathers[2].finish()
    m_second(0)
    chunk(2, 0)
    m_second(1)
    chunk(2, 1)
    m_step(2, 0)
    chunk(2, 2)
    m_step(2, 1)
    chunk(2, 3)
    collect(2)
    m_begin(2)
    m_step(1, 0)
    gathers[3].finish()
    chunk(3, 0)
    m_step(1, 1)
    m_second(2)
    chunk(3, 1)
    m_end(0)
    chunk(3, 2)
    m_step(2, 2)
    m_end(1)
    chunk(3, 3)
    collect(3)
    m_begin(3)
    m_step(1, 2)
    m_second(3)
    m_end(2)
    m_step(2, 3)
    m_step(1, 3)
    m_end(3)

    for h in range(HD):
        for r in range(rows):

            @pl.when(x == r)
            def _(h=h, r=r):
                for d in (1, 2, 3):
                    src = lax.rem(x - d + NX, NX)
                    pltpu.make_async_remote_copy(
                        src_ref=fin.at[h, r],
                        dst_ref=out.at[:, src, :, h * DH : (h + 1) * DH],
                        send_sem=sx.at[h, r],
                        recv_sem=rx.at[h, d],
                        device_id=at_x(d),
                        device_id_type=MESH,
                    ).wait_recv()

            for d in (1, 2, 3):

                @pl.when(lax.rem(x + d, NX) == r)
                def _(h=h, r=r, d=d):
                    final(h, r, d).wait_send()

    for g in gathers:
        g.close()
    for copy in sent:
        copy.wait_send()


def main_step(turn, row, q, k, v):
    dma = pltpu.SemaphoreType.DMA
    any_spec = pl.BlockSpec(memory_space=pl.ANY)
    bf, f32 = jnp.bfloat16, jnp.float32
    i32 = jnp.int32
    out, info = pl.pallas_call(
        main_kernel,
        out_shape=[
            jax.ShapeDtypeStruct((2, NX, B, HD * DH), bf),
            jax.ShapeDtypeStruct((8, 128), i32),
        ],
        in_specs=[SMEM_SPEC, VMEM_SPEC] + [any_spec] * 3,
        out_specs=[VMEM_SPEC] * 2,
        scratch_shapes=[pltpu.VMEM((NX, 2, BD, B, DH), bf)] * HD
        + [pltpu.VMEM((NX, 2, B, DH), bf)] * HD
        + [pltpu.VMEM((NZ, TQ, B, DH), bf)] * HD
        + [pltpu.VMEM((NZ, NS, DH, B), bf)] * HD
        + [pltpu.VMEM((NZ, NS, 1, B), f32)] * HD
        + [
            pltpu.VMEM((BD, B, HD * DH), bf),
            pltpu.VMEM((BD * B, HD * DH), bf),
            pltpu.VMEM((BD * B, HD * DH), bf),
            pltpu.VMEM((NX, HD, 2, B, DH), bf),
            pltpu.VMEM((UN, B, B), f32),
            pltpu.VMEM((W_ALL + 1, DH, B), f32),
            pltpu.VMEM((W_ALL + 1, 2, B), f32),
            pltpu.VMEM((DH, B), f32),
            pltpu.VMEM((1, B), f32),
            pltpu.VMEM((1, B), f32),
            pltpu.VMEM((2, 14, NS, DH, B), bf),
            pltpu.VMEM((2, 14, NS, 1, B), f32),
            pltpu.VMEM((2, 14, NS, DH, B), bf),
            pltpu.VMEM((2, 14, NS, 1, B), f32),
            pltpu.VMEM((HD, NS // 2, 2, B, DH), bf),
            pltpu.VMEM((NX * NZ, 1, 128), i32),
            pltpu.VMEM((NX * NZ, 128), i32),
            pltpu.VMEM((32, 128), i32),
            pltpu.VMEM((8, 256), i32),
            pltpu.SMEM((NX * NZ, 128), i32),
            pltpu.SMEM((32, 128), i32),
            pltpu.SMEM((8, 256), i32),
        ]
        + [
            dma((6,)), dma((NX * NZ,)), dma((NX * NZ,)),
            dma((4, HD)), dma((4, HD)),
            dma((HD, 2, 2)), dma((HD, 2, 2)), dma((HD, 2, 2)), dma((HD, 2, 2)),
            dma((2, 14)), dma((2, 14)),
            dma((2, 2, 14)), dma((2, 2, 14)),
            dma((HD, NS // 2)), dma((HD, 4)),
        ],
        compiler_params=params(0, 58),
        name="main",
    )(turn, row, q, k, v)
    return out.reshape(BD * B, HD * DH), info[0, 0], info[1, 0]


def plan_kernel(tab, send_idx, items, counts, blk, slot):
    s, x, z, _ = place()
    blk_dev = BD
    n_blocks = NX * NZ * BD

    def one(i, carry):
        rank, used, start = carry
        home = i // blk_dev
        k = tab[home, 0, HD * blk_dev * R + lax.rem(i, blk_dev)]
        used = jnp.where(lax.rem(i, blk_dev) == 0, 0, used)
        start = jnp.where(i == s * blk_dev, rank, start)
        mine = (k > 0) & (lax.rem(rank, NX) == x)
        at = jnp.where(mine, rank // NX, 64)
        blk[at] = i
        slot[at] = lax.rem(home, NZ) * 8 + (home // NZ) * 2 + used
        return rank + k, used + jnp.where(mine, 1, 0), start

    total, _, start = lax.fori_loop(0, n_blocks, one, (0, 0, 0))

    for c in range(8):
        send_idx[c] = 0
    filled = [jnp.int32(0)] * NX
    rank = start
    for j in range(blk_dev):
        k = tab[s, 0, HD * blk_dev * R + j]
        col = lax.rem(rank, NX)
        at = jnp.int32(8)
        for c in range(NX):
            hit = (k > 0) & (col == c)
            at = jnp.where(hit, c * 2 + filled[c], at)
            filled[c] = filled[c] + jnp.where(hit, 1, 0)
        send_idx[at] = j
        rank = rank + k

    def query(a, cnt):
        i = blk[a]
        home = i // blk_dev
        base = lax.rem(i, blk_dev) * R
        pos = (lax.rem(a // 2, NZ)) * 8 + (a // 16) * 2 + lax.rem(a, 2)
        word = slot[a] * 64 + pos
        cnt = list(cnt)

        def add(h, t, ok):
            w = ((t // 64) * 8 + lax.rem(t, blk_dev)) * 4096 + word
            items[h * LCAP + cnt[h]] = w
            cnt[h] = cnt[h] + jnp.where(ok, 1, 0)

        for dt in (-1, 0, 1):
            t = i + dt
            ok = (t >= 0) & (t < n_blocks) & (lax.rem(t // blk_dev, NZ) == z)
            t = jnp.clip(t, 0, n_blocks - 1)
            for h in range(HD):
                add(h, t, ok)
        for g in range(G):
            for h in range(HD):
                add(h, jnp.int32(g), z == 0)
        for h in range(HD):
            for r in range(R):
                t = tab[home, 0, h * blk_dev * R + base + r]
                add(h, t, lax.rem(t // blk_dev, NZ) == z)
        return tuple(cnt)

    n_mine = (total - x + NX - 1) // NX
    cnt = lax.fori_loop(0, n_mine, query, (jnp.int32(0),) * HD)
    for h in range(HD):
        counts[h] = cnt[h]
        for u in range(4):
            items[h * LCAP + cnt[h] + u] = jnp.int32(64)


def planned(tab):
    return pl.pallas_call(
        plan_kernel,
        out_shape=[
            jax.ShapeDtypeStruct((16,), jnp.int32),
            jax.ShapeDtypeStruct((HD * LCAP,), jnp.int32),
            jax.ShapeDtypeStruct((8,), jnp.int32),
        ],
        in_specs=[SMEM_SPEC],
        out_specs=[SMEM_SPEC] * 3,
        scratch_shapes=[pltpu.SMEM((72,), jnp.int32), pltpu.SMEM((72,), jnp.int32)],
        compiler_params=params(None, 16),
        name="plan",
    )(tab)


RING = [(k, h) for k in (1, 2, 3) for h in range(HD)]
RING_UP = RING + [(4, 0), (4, 1)]
RING_DOWN = RING + [(4, 2), (4, 3)]


def spread_kernel(idx, q, k, v, kv, qz, qs, sx, rx, so, ro, sf, rf, su, ru, sd, rd):
    s, x, z, hd = place()

    def at_x(d):
        return (lax.rem(x + d, NX) * NZ + z, hd)

    def at_z(d):
        return (x * NZ + lax.rem(z + d + NZ, NZ), hd)

    def xi(d):
        return lax.rem(x + d + NX, NX)

    def zi(d):
        return lax.rem(z + d + NZ, NZ)

    barrier = pltpu.get_barrier_semaphore()
    for d in (1, 2, 3):
        pl.semaphore_signal(barrier, inc=1, device_id=at_x(d), device_id_type=MESH)
    for d in (1, -1):
        pl.semaphore_signal(barrier, inc=1, device_id=at_z(d), device_id_type=MESH)

    def fill(c, carry):
        col, u = c // 2, lax.rem(c, 2)
        j = idx[c]
        for h in range(HD):
            qs[col, h, u] = q[j, :, h * DH : (h + 1) * DH]
        return carry

    lax.fori_loop(0, 8, fill, 0)
    for h in range(HD):
        for u in range(2):
            qz[h, z, x, u] = qs[x, h, u]
    pl.semaphore_wait(barrier, 5)

    q_out = []
    for d in (1, 2, 3):
        copy = pltpu.make_async_remote_copy(
            src_ref=qs.at[xi(d)],
            dst_ref=qz.at[:, z, x],
            send_sem=sx.at[d],
            recv_sem=rx.at[d],
            device_id=at_x(d),
            device_id_type=MESH,
        )
        copy.start()
        q_out.append(copy)

    own = []
    for h in range(HD):

        def prep(b, carry):
            rows = pl.ds(pl.multiple_of(b * B, B), B)
            kv[h, x, 0, b] = k[rows, h * DH : (h + 1) * DH]
            kv[h, x, 1, b] = v[rows, h * DH : (h + 1) * DH].T
            return carry

        lax.fori_loop(0, BD, prep, 0)
        for side, d in ((0, 1), (1, 3)):
            copy = pltpu.make_async_remote_copy(
                src_ref=kv.at[h, x],
                dst_ref=kv.at[h, x],
                send_sem=so.at[side, h],
                recv_sem=ro.at[side, h],
                device_id=at_x(d),
                device_id_type=MESH,
            )
            copy.start()
            own.append(copy)

    for d in (1, 2, 3):
        src = xi(-d)
        pltpu.make_async_remote_copy(
            src_ref=qz.at[:, z, src],
            dst_ref=qz.at[:, z, src],
            send_sem=sx.at[d],
            recv_sem=rx.at[d],
            device_id=at_x(d),
            device_id_type=MESH,
        ).wait_recv()

    rings = []

    def ring_piece(up, n):
        kk, h = (RING_UP if up else RING_DOWN)[n]
        step = -1 if up else 1
        row = zi(step * (kk - 1))
        return pltpu.make_async_remote_copy(
            src_ref=qz.at[h, row],
            dst_ref=qz.at[h, row],
            send_sem=(su if up else sd).at[n],
            recv_sem=(ru if up else rd).at[n],
            device_id=at_z(1 if up else -1),
            device_id_type=MESH,
        )

    def ring_arrival(up, n):
        kk, h = (RING_UP if up else RING_DOWN)[n]
        row = zi((-1 if up else 1) * kk)
        return pltpu.make_async_remote_copy(
            src_ref=qz.at[h, row],
            dst_ref=qz.at[h, row],
            send_sem=(su if up else sd).at[n],
            recv_sem=(ru if up else rd).at[n],
            device_id=at_z(1 if up else -1),
            device_id_type=MESH,
        )

    for n in range(4):
        for up in (True, False):
            copy = ring_piece(up, n)
            copy.start()
            rings.append(copy)

    fwd = []

    def forward_x(h):
        for side, d, part in ((0, 1, 0), (1, 3, 1)):
            src = xi(-d)
            pltpu.make_async_remote_copy(
                src_ref=kv.at[h, src],
                dst_ref=kv.at[h, src],
                send_sem=so.at[side, h],
                recv_sem=ro.at[side, h],
                device_id=at_x(d),
                device_id_type=MESH,
            ).wait_recv()
            copy = pltpu.make_async_remote_copy(
                src_ref=kv.at[h, src, part],
                dst_ref=kv.at[h, src, part],
                send_sem=sf.at[side, h],
                recv_sem=rf.at[side, h],
                device_id=at_x(d),
                device_id_type=MESH,
            )
            copy.start()
            fwd.append(copy)

    for n in range(14):
        for up in (True, False):
            kk, h = (RING_UP if up else RING_DOWN)[n]
            ring_arrival(up, n).wait_recv()
            table = RING_UP if up else RING_DOWN
            if (kk + 1, h) in table:
                copy = ring_piece(up, table.index((kk + 1, h)))
                copy.start()
                rings.append(copy)
        if n % 2 == 1 and n // 2 < HD:
            forward_x(n // 2)

    far = xi(2)
    for h in range(HD):
        for side, d, part in ((0, 1, 0), (1, 3, 1)):
            pltpu.make_async_remote_copy(
                src_ref=kv.at[h, far, part],
                dst_ref=kv.at[h, far, part],
                send_sem=sf.at[side, h],
                recv_sem=rf.at[side, h],
                device_id=at_x(d),
                device_id_type=MESH,
            ).wait_recv()
    for copy in q_out + own + rings + fwd:
        copy.wait_send()


def spread_all(idx, q, k, v):
    dma = pltpu.SemaphoreType.DMA
    return pl.pallas_call(
        spread_kernel,
        out_shape=[
            jax.ShapeDtypeStruct((HD, NX, 2, BD, B, DH), jnp.bfloat16),
            jax.ShapeDtypeStruct((HD, NZ, NX, 2, B, DH), jnp.bfloat16),
        ],
        in_specs=[SMEM_SPEC] + [VMEM_SPEC] * 3,
        out_specs=[VMEM_SPEC] * 2,
        scratch_shapes=[
            pltpu.VMEM((NX, HD, 2, B, DH), jnp.bfloat16),
            dma((4,)),
            dma((4,)),
            dma((2, HD)),
            dma((2, HD)),
            dma((2, HD)),
            dma((2, HD)),
            dma((14,)),
            dma((14,)),
            dma((14,)),
            dma((14,)),
        ],
        compiler_params=params(2),
        name="spread",
    )(idx, q, k, v)


UNROLL = 4


def part_kernel(ns, items, counts, kv, qz, out, lse, acc, top, den):
    h = pl.program_id(0)
    n_acc = NZ * ns

    def clear(a, carry):
        acc[a] = jnp.zeros((DH, B), jnp.float32)
        top[a] = jnp.full((1, B), neg_big, jnp.float32)
        den[a] = jnp.zeros((1, B), jnp.float32)
        return carry

    lax.fori_loop(0, n_acc + 1, clear, 0)

    def batch(n, carry):
        found = []
        for u in range(UNROLL):
            w = items[h * LCAP + n * UNROLL + u]
            pos = lax.rem(w, 64)
            a = (pos // 8) * ns + lax.rem(pos, 8)
            a = jnp.where(n * UNROLL + u < counts[h], a, n_acc)
            spot = lax.rem(w // 64, 64)
            tile = w // 4096
            keys = kv[0, tile // 8, 0, lax.rem(tile, 8)]
            vals = kv[0, tile // 8, 1, lax.rem(tile, 8)]
            qt = qz[0, spot // 8, lax.rem(spot, 8) // 2, lax.rem(spot, 2)]
            scores = lax.dot_general(
                keys, qt, (((1,), (1,)), ((), ())), preferred_element_type=jnp.float32
            )
            scores = scores * score_scale
            m = jnp.max(scores, axis=0, keepdims=True)
            p = jnp.exp(scores - m).astype(jnp.bfloat16)
            l = jnp.sum(p.astype(jnp.float32), axis=0, keepdims=True)
            o = jnp.dot(vals, p, preferred_element_type=jnp.float32)
            found.append((a, m, l, o))
        for a, m, l, o in found:
            old = top[a]
            new = jnp.maximum(old, m)
            f0, f1 = jnp.exp(old - new), jnp.exp(m - new)
            acc[a] = acc[a] * f0 + o * f1
            den[a] = den[a] * f0 + l * f1
            top[a] = new
        return carry

    lax.fori_loop(0, (counts[h] + UNROLL - 1) // UNROLL, batch, 0)

    def finish(a, carry):
        l = den[a]
        some = l > 0
        safe = jnp.where(some, l, 1.0)
        out[0, a // ns, lax.rem(a, ns)] = (acc[a] / safe).astype(jnp.bfloat16)
        lse[0, a // ns, lax.rem(a, ns)] = jnp.where(some, top[a] + jnp.log(safe), neg_big)
        return carry

    lax.fori_loop(0, n_acc, finish, 0)


def parts_of(ns, items, counts, kv, qz):
    n_acc = NZ * ns
    return pl.pallas_call(
        functools.partial(part_kernel, ns),
        grid=(HD,),
        out_shape=[
            jax.ShapeDtypeStruct((HD, NZ, ns, DH, B), jnp.bfloat16),
            jax.ShapeDtypeStruct((HD, NZ, ns, 1, B), jnp.float32),
        ],
        in_specs=[
            SMEM_SPEC,
            SMEM_SPEC,
            pl.BlockSpec((1, NX, 2, BD, B, DH), lambda h: (h, 0, 0, 0, 0, 0)),
            pl.BlockSpec((1, NZ, NX, 2, B, DH), lambda h: (h, 0, 0, 0, 0, 0)),
        ],
        out_specs=[
            pl.BlockSpec((1, NZ, ns, DH, B), lambda h: (h, 0, 0, 0, 0)),
            pl.BlockSpec((1, NZ, ns, 1, B), lambda h: (h, 0, 0, 0, 0)),
        ],
        scratch_shapes=[
            pltpu.VMEM((n_acc + 1, DH, B), jnp.float32),
            pltpu.VMEM((n_acc + 1, 1, B), jnp.float32),
            pltpu.VMEM((n_acc + 1, 1, B), jnp.float32),
        ],
        compiler_params=params(None, 40),
        name="parts",
    )(items, counts, kv, qz)


HOME_UP = [(4, 2), (4, 3)] + [(k, h) for k in (3, 2, 1) for h in range(HD)]
HOME_DOWN = [(4, 0), (4, 1)] + [(k, h) for k in (3, 2, 1) for h in range(HD)]


def merged(o0, l0, o1, l1):
    top = jnp.maximum(l0, l1)
    f0, f1 = jnp.exp(l0 - top), jnp.exp(l1 - top)
    both = f0 + f1
    o = (o0.astype(jnp.float32) * f0 + o1.astype(jnp.float32) * f1) / both
    return o, top + jnp.log(both)


def join_kernel(
    ns, o, lse, out, sou, slu, rou, rlu, sod, sld, rod, rld, fin, ssu, rsu, ssd, rsd, sx, rx
):
    s, x, z, hd = place()

    def at_x(d):
        return (lax.rem(x + d, NX) * NZ + z, hd)

    def at_z(d):
        return (x * NZ + lax.rem(z + d + NZ, NZ), hd)

    def zi(d):
        return lax.rem(z + d + NZ, NZ)

    barrier = pltpu.get_barrier_semaphore()
    for d in (1, 2, 3):
        pl.semaphore_signal(barrier, inc=1, device_id=at_x(d), device_id_type=MESH)
    for d in (1, -1):
        pl.semaphore_signal(barrier, inc=1, device_id=at_z(d), device_id_type=MESH)
    pl.semaphore_wait(barrier, 5)

    sent = []

    def copies(up, n, src_o, src_l):
        ro, rl = (rou, rlu) if up else (rod, rld)
        ss, rs = (ssu, rsu) if up else (ssd, rsd)
        return [
            pltpu.make_async_remote_copy(
                src_ref=src,
                dst_ref=dst.at[n],
                send_sem=ss.at[i, n],
                recv_sem=rs.at[i, n],
                device_id=at_z(1 if up else -1),
                device_id_type=MESH,
            )
            for i, (src, dst) in enumerate(((src_o, ro), (src_l, rl)))
        ]

    def send(up, n, src_o, src_l):
        for copy in copies(up, n, src_o, src_l):
            copy.start()
            sent.append(copy)

    def arrived(up, n):
        ro, rl = (rou, rlu) if up else (rod, rld)
        for copy in copies(up, n, ro.at[n], rl.at[n]):
            copy.wait_recv()

    for n in range(14):
        for up in (True, False):
            table = HOME_UP if up else HOME_DOWN
            kk, h = table[n]
            dest = zi(kk if up else -kk)
            if (kk + 1, h) not in table:
                send(up, n, o.at[h, dest], lse.at[h, dest])
                continue
            prev = table.index((kk + 1, h))
            arrived(up, prev)
            ro, rl = (rou, rlu) if up else (rod, rld)
            so, sl = (sou, slu) if up else (sod, sld)

            def step(i, carry, ro=ro, rl=rl, so=so, sl=sl, prev=prev, n=n, h=h, dest=dest):
                val, l = merged(o[h, dest, i], lse[h, dest, i], ro[prev, i], rl[prev, i])
                so[n, i] = val.astype(jnp.bfloat16)
                sl[n, i] = l
                return carry

            lax.fori_loop(0, ns, step, 0)
            send(up, n, so.at[n], sl.at[n])

    for h in range(HD):
        n = 10 + h
        arrived(True, n)
        arrived(False, n)

        def last(i, carry, h=h, n=n):
            a, la = merged(rou[n, i], rlu[n, i], rod[n, i], rld[n, i])
            val, _ = merged(o[h, z, i], lse[h, z, i], a, la)
            fin[i // 2, lax.rem(i, 2), :, h * DH : (h + 1) * DH] = val.T.astype(jnp.bfloat16)
            return carry

        lax.fori_loop(0, ns, last, 0)

    rows = ns // 2
    for r in range(NX):
        if r >= rows:

            @pl.when(x == r)
            def _():
                out[...] = jnp.zeros(out.shape, out.dtype)

            continue

        @pl.when(x == r)
        def _(r=r):
            out[:, x] = fin[r]

    def final(r, d):
        return pltpu.make_async_remote_copy(
            src_ref=fin.at[r],
            dst_ref=out.at[:, x],
            send_sem=sx.at[r],
            recv_sem=rx.at[d],
            device_id=(r * NZ + z, hd),
            device_id_type=MESH,
        )

    for d in (1, 2, 3):
        for r in range(rows):

            @pl.when(lax.rem(x + d, NX) == r)
            def _(r=r, d=d):
                final(r, d).start()

    for r in range(rows):

        @pl.when(x == r)
        def _(r=r):
            for d in (1, 2, 3):
                src = lax.rem(x - d + NX, NX)
                pltpu.make_async_remote_copy(
                    src_ref=fin.at[r],
                    dst_ref=out.at[:, src],
                    send_sem=sx.at[r],
                    recv_sem=rx.at[d],
                    device_id=at_x(d),
                    device_id_type=MESH,
                ).wait_recv()

    for d in (1, 2, 3):
        for r in range(rows):

            @pl.when(lax.rem(x + d, NX) == r)
            def _(r=r, d=d):
                final(r, d).wait_send()

    for copy in sent:
        copy.wait_send()


def joined(ns, o, lse):
    dma = pltpu.SemaphoreType.DMA
    piece_o = pltpu.VMEM((14, ns, DH, B), jnp.bfloat16)
    piece_l = pltpu.VMEM((14, ns, 1, B), jnp.float32)
    out = pl.pallas_call(
        functools.partial(join_kernel, ns),
        out_shape=jax.ShapeDtypeStruct((2, NX, B, HD * DH), jnp.bfloat16),
        in_specs=[VMEM_SPEC] * 2,
        out_specs=VMEM_SPEC,
        scratch_shapes=[
            piece_o, piece_l, piece_o, piece_l, piece_o, piece_l, piece_o, piece_l,
            pltpu.VMEM((ns // 2, 2, B, HD * DH), jnp.bfloat16),
            dma((2, 14)), dma((2, 14)), dma((2, 14)), dma((2, 14)),
            dma((4,)), dma((4,)),
        ],
        compiler_params=params(3, 56),
        name="join%d" % ns,
    )(o, lse)
    return out.reshape(BD * B, HD * DH)


def body(queries, keys, values, random_holder, random_offset, keep):
    want = random_holder * BD + random_offset
    row = jnp.concatenate([want.reshape(-1), keep, jnp.zeros((24,), jnp.int32)]).reshape(1, 128)
    q = queries.reshape(BD, B, HD * DH)
    out, total, most = main_step(jnp.zeros((2,), jnp.int32), row, q, keys, values)
    parts = (most + TQ - 1) // TQ
    passes = (total + STEP - 1) // STEP * parts

    def more(out):
        def again(state):
            n, out = state
            turn = jnp.stack([n // parts, n % parts])
            new = main_step(turn, row, q, keys, values)[0]
            pairs = [(i, i + 2 * NZ) for i in range(2 * NZ)]
            new = jnp.where(turn[0] > 0, lax.ppermute(new, "seq", pairs), new)
            return n + 1, out + new

        return lax.while_loop(lambda state: state[0] < passes, again, (jnp.int32(1), out))[1]

    return lax.cond(passes > 1, more, lambda out: out, out)


def solution(mesh):
    in_specs = (
        P("seq", "head"),
        P("seq", "head"),
        P("seq", "head"),
        P("head", "seq", None),
        P("head", "seq", None),
        P("seq"),
    )
    out_specs = P("seq", "head")
    return jax.shard_map(body, mesh=mesh, in_specs=in_specs, out_specs=out_specs, check_vma=False)
```

```python
import math

import jax
import jax.numpy as jnp
from jax import lax
from jax.experimental import pallas as pl
from jax.experimental.pallas import tpu as pltpu
from jax.sharding import PartitionSpec as P

DH = 128
B = 128
G = 2
R = 3
NX = 4
NZ = 8
HD = 4
BD = 8
TQ = 6
NS = 4
HALF = NS // 2
UN = 8
W_ANY = 128
W_ALL = 192
STEP = 32 * NX

neg_big = -1e30
MESH = pl.DeviceIdType.MESH
SMEM_SPEC = pl.BlockSpec(memory_space=pltpu.SMEM)
VMEM_SPEC = pl.BlockSpec(memory_space=pltpu.VMEM)
score_scale = 1.0 / math.sqrt(DH)


def place():
    s = lax.axis_index("seq")
    return s, s // NZ, lax.rem(s, NZ), lax.axis_index("head")


def to_seq(s, h):
    return (s, h)


def params(cid=None, mib=48):
    if cid is None:
        return pltpu.CompilerParams(vmem_limit_bytes=mib << 20)
    return pltpu.CompilerParams(
        collective_id=cid, has_side_effects=True, vmem_limit_bytes=mib << 20
    )


class RowGather:
    def __init__(self, kv, sems, x, z, hd):
        self.kv, self.sems, self.x, self.z, self.hd = kv, sems, x, z, hd
        self.sent = []

    def piece(self, which, side, part, holder):
        sk, rk, sf, rf = self.sems
        ss, rs = (sk, rk) if which == 0 else (sf, rf)
        d = 1 if side == 0 else 3
        return pltpu.make_async_remote_copy(
            src_ref=self.kv.at[holder, part],
            dst_ref=self.kv.at[holder, part],
            send_sem=ss.at[side, part],
            recv_sem=rs.at[side, part],
            device_id=(lax.rem(self.x + d, NX) * NZ + self.z, self.hd),
            device_id_type=MESH,
        )

    def start(self, copy):
        copy.start()
        self.sent.append(copy)

    def own(self, orders=(0, 1)):
        for order in orders:
            for side in (0, 1):
                self.start(self.piece(0, side, order ^ side, self.x))

    def neighbour(self, side):
        return lax.rem(self.x + (3 if side == 0 else 1), NX)

    def forward(self):
        for side in (0, 1):
            self.piece(0, side, side, self.neighbour(side)).wait_recv()
            self.start(self.piece(1, side, side, self.neighbour(side)))

    def finish(self):
        for side in (0, 1):
            self.piece(0, side, 1 - side, self.neighbour(side)).wait_recv()
        for side in (0, 1):
            self.piece(1, side, side, lax.rem(self.x + 2, NX)).wait_recv()

    def close(self):
        for copy in self.sent:
            copy.wait_send()


def merged(o0, l0, o1, l1):
    top = jnp.maximum(l0, l1)
    f0, f1 = jnp.exp(l0 - top), jnp.exp(l1 - top)
    both = f0 + f1
    o = (o0.astype(jnp.float32) * f0 + o1.astype(jnp.float32) * f1) / both
    return o, top + jnp.log(both)


def plan(tab, window, part, s, x, z, sendm, lastm, itemm, info):
    n_home, wide = NX * NZ, 128
    flags = HD * BD * R
    f32, i32, bf = jnp.float32, jnp.int32, jnp.bfloat16

    def iota(rows, cols, axis):
        return lax.broadcasted_iota(i32, (rows, cols), axis)

    def times(a, b):
        return jnp.dot(a.astype(bf), b.astype(bf), preferred_element_type=f32)

    t = tab[:, 0, :]
    lane = iota(n_home, wide, 1)
    home = iota(n_home, wide, 0)
    kept = jnp.where((lane >= flags) & (lane < flags + BD), t, 0).astype(f32)
    in_row = times(kept, (iota(wide, wide, 0) < iota(wide, wide, 1)).astype(f32))
    count = jnp.broadcast_to(jnp.sum(kept, axis=1, keepdims=True), (n_home, wide))
    upper = times(iota(n_home, n_home, 1) < iota(n_home, n_home, 0), count)
    ranks = (in_row + upper).astype(i32)
    first_rank = upper.astype(i32)

    most = jnp.zeros((NZ, 1), f32)
    for c in range(NX):
        n = jnp.sum(jnp.where((ranks & (NX - 1)) == c, kept, 0.0), axis=1, keepdims=True)
        most = jnp.maximum(most, n[0:8] + n[8:16] + n[16:24] + n[24:32])
    most = jnp.max(most, axis=0, keepdims=True)
    total = jnp.sum(count[:, 0:1], axis=0, keepdims=True)
    row8 = iota(8, wide, 0)
    info[...] = jnp.where(
        row8 == 0, jnp.broadcast_to(total, (8, wide)), jnp.broadcast_to(most, (8, wide))
    ).astype(i32)

    row, line = home & (NZ - 1), home >> 3
    blocks = []
    mine_count = jnp.zeros((n_home, wide), f32)
    for b in range(BD):
        at = flags + b
        k = jnp.broadcast_to(kept[:, at : at + 1], (n_home, wide)) > 0
        r = jnp.broadcast_to(ranks[:, at : at + 1], (n_home, wide))
        here = k & ((r >> 7) == window)
        turn = jnp.where(((r - first_rank) >= 4) & (((r - 4) >> 7) == window), 1, 0)
        mine = here & ((r & (NX - 1)) == x)
        blocks.append((r, here, turn, mine))
        mine_count = mine_count + jnp.where(mine, 1.0, 0.0)
    same_row = (iota(n_home, n_home, 0) & (NZ - 1)) == (iota(n_home, n_home, 1) & (NZ - 1))
    cell = times(same_row & (iota(n_home, n_home, 1) < iota(n_home, n_home, 0)), mine_count)
    cell = cell.astype(i32) - part * TQ

    send = jnp.zeros((n_home, wide), i32)
    take = jnp.zeros((n_home, wide), i32)
    hots, data = [], []
    for b, (r, here, turn, mine) in enumerate(blocks):
        send = send + jnp.where(here & (lane == (r & (NX - 1)) * 2 + turn), b, 0)
        chosen = mine & (cell >= 0) & (cell < TQ)
        take = take + jnp.where(chosen & (row == z) & (lane == cell), line * 2 + turn, 0)
        hots.append(jnp.where(chosen & (((r >> 2) & 31) == lane), 1.0, 0.0))
        moved = t if b == 0 else pltpu.roll(t, wide - R * b, 1)
        moved = jnp.where(lane == 120, home * BD + b, moved)
        moved = jnp.where(lane == 121, row * 8 + cell, moved)
        data.append(jnp.where(lane == 122, 1, moved).astype(f32))
        cell = cell + jnp.where(mine, 1, 0)
    sendm[...] = send
    take = jnp.sum(take.astype(f32), axis=0, keepdims=True).astype(i32)

    hot = jnp.concatenate(hots, axis=0).astype(bf)
    known = jnp.concatenate(data, axis=0).astype(bf)
    of = lax.dot_general(hot, known, (((0,), (0,)), ((), ())), preferred_element_type=f32)
    of = of[:32]

    src, to = iota(wide, wide, 0), iota(wide, wide, 1)
    kind = to & 7
    wanted = jnp.where(kind < 3, 120, jnp.where(kind < 5, -1, (to >> 3) * (BD * R) + kind - 5))
    tile = times(of, (src == wanted).astype(f32)).astype(i32)
    spot = times(of, (src == 121).astype(f32)).astype(i32)
    valid = times(of, (src == 122).astype(f32)) > 0.5
    m = iota(32, wide, 1)
    kind = m & 7
    tile = tile + jnp.where(kind < 3, kind - 1, jnp.where(kind < 5, kind - 3, 0))
    ok = valid & (m < 32) & (tile >= 0) & (tile < n_home * BD)
    ok = ok & (((tile >> 3) & (NZ - 1)) == z)
    hit = jnp.where(ok, 1.0, 0.0)
    word = spot + ((((tile >> 6) & 3) * 8) + (tile & 7)) * 64
    same_head = (src >> 3) == (to >> 3)
    ahead = times(hit, (same_head & (src < to)).astype(f32))
    whole = times(hit, same_head.astype(f32))
    above = times(
        times(iota(32, 32, 1) < iota(32, 32, 0), hit), same_head.astype(f32)
    )
    order = jnp.where(ok, (ahead + above).astype(i32), -1)
    word = word + jnp.where(ahead < 0.5, 1 << 20, 0)
    lastm[...] = jnp.where(whole > 0.5, (above + whole).astype(i32) - 1, W_ALL)

    slots = iota(32, 2 * wide, 1)
    for h in range(HD):
        found = jnp.zeros((32, 2 * wide), i32)
        for k in range(8):
            c = h * 8 + k
            spots = jnp.broadcast_to(order[:, c : c + 1], (32, 2 * wide))
            words = jnp.broadcast_to(word[:, c : c + 1], (32, 2 * wide))
            found = found + jnp.where(spots == slots, words, 0)
        found = (found[0:8] + found[8:16]) + (found[16:24] + found[24:32])
        found = found[0:4] + found[4:8]
        found = found[0:2] + found[2:4]
        itemm[h : h + 1] = found[0:1] + found[1:2]
    itemm[4:5] = jnp.concatenate([take, take], axis=1)


EXP2 = score_scale * math.log2(math.e)
Q_UP = [(k, h) for h in range(HD) for k in (1, 2, 3)] + [(4, 0), (4, 2)]
Q_DOWN = [(k, h) for h in range(HD) for k in (1, 2, 3)] + [(4, 1), (4, 3)]
M_UP = [(k, h) for h in range(HD) for k in (3, 2, 1)] + [(4, 1), (4, 3)]
M_DOWN = [(k, h) for h in range(HD) for k in (3, 2, 1)] + [(4, 0), (4, 2)]


def main_kernel(turn, table_row, q_any, k_any, v_any, out, info, *rest):
    kvs, qrs, qzs, cos, cls = rest[0:4], rest[4:8], rest[8:12], rest[12:16], rest[16:20]
    (qv, kbuf, vbuf, qs, sc, res, rel, st_o, st_m, st_l, mo, ml, ro, rl, fin) = rest[20:35]
    (tab, sendm, lastm, itemm, sends, lasts, items) = rest[35:42]
    (load, stab, rtab, sqx, rqx, skv, rkv, sfw, rfw, sq, rq, sm, rm, sx, rx) = rest[42:]
    s, x, z, hd = place()
    n_seq = NX * NZ

    def at_x(d):
        return (lax.rem(x + d, NX) * NZ + z, hd)

    def at_z(d):
        return (x * NZ + lax.rem(z + d + NZ, NZ), hd)

    def xi(d):
        return lax.rem(x + d + NX, NX)

    def zi(d):
        return lax.rem(z + d + NZ, NZ)

    loads = [
        pltpu.make_async_copy(src, dst, load.at[i])
        for i, (src, dst) in enumerate(((q_any, qv), (k_any, kbuf), (v_any, vbuf)))
    ]
    for copy in loads:
        copy.start()
    barrier = pltpu.get_barrier_semaphore()
    for d in range(1, n_seq):
        pl.semaphore_signal(
            barrier, inc=1, device_id=(lax.rem(s + d, n_seq), hd), device_id_type=MESH
        )
    tab[s] = table_row[...]
    loads[1].wait()
    loads[2].wait()

    sent = []

    def start(copy):
        copy.start()
        sent.append(copy)

    gathers = []
    for h in range(HD):
        g = RowGather(kvs[h], (skv.at[h], rkv.at[h], sfw.at[h], rfw.at[h]), x, z, hd)
        gathers.append(g)

    def prepare(h):
        def prep(b, carry):
            rows = pl.ds(pl.multiple_of(b * B, B), B)
            kvs[h][x, 0, b] = kbuf[rows, h * DH : (h + 1) * DH]
            kvs[h][x, 1, b] = vbuf[rows, h * DH : (h + 1) * DH].T
            return carry

        lax.fori_loop(0, BD, prep, 0)


    prepare(0)
    pl.semaphore_wait(barrier, n_seq - 1)
    gathers[0].own((0,))
    rows_out = []
    for d in range(1, n_seq):
        copy = pltpu.make_async_remote_copy(
            src_ref=table_row,
            dst_ref=tab.at[s],
            send_sem=stab.at[d],
            recv_sem=rtab.at[d],
            device_id=(lax.rem(s + d, n_seq), hd),
            device_id_type=MESH,
        )
        copy.start()
        rows_out.append(copy)
    prepare(1)
    for copy in rows_out:
        copy.wait()
    plan(tab, turn[0], turn[1], s, x, z, sendm, lastm, itemm, info)
    lists = [
        pltpu.make_async_copy(src, dst, load.at[3 + i])
        for i, (src, dst) in enumerate(((sendm, sends), (itemm, items), (lastm, lasts)))
    ]
    for copy in lists:
        copy.start()
    loads[0].wait()
    for copy in lists:
        copy.wait()

    def fill(c, carry):
        col, u = c // 2, lax.rem(c, 2)
        j = sends[s, c] & (BD - 1)
        for h in range(HD):
            qs[col, h, u] = qv[j, :, h * DH : (h + 1) * DH]
        return carry

    lax.fori_loop(0, 8, fill, 0)
    for h in range(HD):
        for u in range(2):
            qrs[h][x, u] = qs[x, h, u]

    def q_move(h, d, src):
        return pltpu.make_async_remote_copy(
            src_ref=qs.at[src, h],
            dst_ref=qrs[h].at[x],
            send_sem=sqx.at[d, h],
            recv_sem=rqx.at[d, h],
            device_id=at_x(d),
            device_id_type=MESH,
        )

    def q_leave(h):
        for d in (1, 3, 2):
            start(q_move(h, d, xi(d)))

    q_leave(0)
    q_leave(1)
    gathers[0].own((1,))

    def q_copy(up, kk, h, row):
        n = (Q_UP if up else Q_DOWN).index((kk, h))
        return pltpu.make_async_remote_copy(
            src_ref=qzs[h].at[row],
            dst_ref=qzs[h].at[row],
            send_sem=sq.at[0 if up else 1, n],
            recv_sem=rq.at[0 if up else 1, n],
            device_id=at_z(1 if up else -1),
            device_id_type=MESH,
        )

    def q_send(up, kk, h):
        if (kk, h) in (Q_UP if up else Q_DOWN):
            start(q_copy(up, kk, h, zi((-1 if up else 1) * (kk - 1))))

    def q_ready(h):
        for d in (1, 2, 3):
            src = xi(-d)
            pltpu.make_async_remote_copy(
                src_ref=qrs[h].at[src],
                dst_ref=qrs[h].at[src],
                send_sem=sqx.at[d, h],
                recv_sem=rqx.at[d, h],
                device_id=at_x(d),
                device_id_type=MESH,
            ).wait_recv()
        for c in range(TQ):
            w = items[4, c]
            qzs[h][z, c] = qrs[h][(w >> 1) & 3, w & 1]

    def q_begin(h):
        for up in (True, False):
            q_send(up, 1, h)

    def q_step(kk, h):
        for up in (True, False):
            if (kk, h) in (Q_UP if up else Q_DOWN):
                q_copy(up, kk, h, zi((-1 if up else 1) * kk)).wait_recv()
                q_send(up, kk + 1, h)

    nb = jnp.where(z == 0, W_ALL // UN // 4, W_ANY // UN // 4)

    def chunk(h, part):
        kv, qz = kvs[h], qzs[h]

        def words_of(n):
            return [items[h, n * UN + u] for u in range(UN)]

        def score(words):
            for u, w in enumerate(words):
                spot, tile = w & 63, (w >> 6) & 31
                sc[u] = lax.dot_general(
                    kv[tile >> 3, 0, tile & 7],
                    qz[spot >> 3, jnp.minimum(spot & 7, TQ - 1)],
                    (((1,), (1,)), ((), ())),
                    preferred_element_type=jnp.float32,
                )

        def batch(n, carry):
            m0, l0, o0 = st_m[...], st_l[...], st_o[...]
            words = words_of(n)
            scores = [sc[u] for u in range(UN)]
            tops, weights = [], []
            for val in scores:
                raw = jnp.max(val, axis=0, keepdims=True)
                tops.append(raw)
                weights.append(jnp.exp2((val - raw) * EXP2).astype(jnp.bfloat16))
            sums = []
            for w, p in zip(words, weights):
                tile = (w >> 6) & 31
                rows = jnp.concatenate([kv[tile >> 3, 1, tile & 7], ones], axis=0)
                sums.append(jnp.dot(rows, p, preferred_element_type=jnp.float32))
            score(words_of(n + 1))
            for u, w in enumerate(words):
                old = jnp.where((w >> 20) > 0, neg_big, m0)
                top = jnp.maximum(old, tops[u])
                f0, f1 = jnp.exp2((old - top) * EXP2), jnp.exp2((tops[u] - top) * EXP2)
                m0 = top
                l0 = l0 * f0 + sums[u][DH : DH + 1] * f1
                o0 = o0 * f0 + sums[u][:DH] * f1
                at = n * UN + u
                res[at] = o0
                rel[at] = jnp.concatenate([m0, l0], axis=0)
            st_m[...], st_l[...], st_o[...] = m0, l0, o0
            return carry

        ones = jnp.ones((16, B), jnp.bfloat16)
        if part == 0:
            score(words_of(0))
        lax.fori_loop(part * nb, (part + 1) * nb, batch, 0)

    def collect(h):
        for a in range(NZ * NS):
            w = jnp.clip(lasts[a, h * 8], 0, W_ALL)
            zp, i = (a >> 1) & 7, (a >> 4) * 2 + (a & 1)
            l = rel[w, 1:2]
            cos[h][zp, i] = (res[w] * (1.0 / l)).astype(jnp.bfloat16)
            cls[h][zp, i] = rel[w, 0:1] * score_scale + jnp.log(l)

    def m_copies(up, kk, h, half, src_o, src_l):
        n = (M_UP if up else M_DOWN).index((kk, h))
        side = 0 if up else 1
        part = slice(half * HALF, (half + 1) * HALF)
        return [
            pltpu.make_async_remote_copy(
                src_ref=src.at[part],
                dst_ref=dst.at[side, n, part],
                send_sem=sm.at[i, half, side, n],
                recv_sem=rm.at[i, half, side, n],
                device_id=at_z(1 if up else -1),
                device_id_type=MESH,
            )
            for i, (src, dst) in enumerate(((src_o, ro), (src_l, rl)))
        ]

    def m_arrived(up, kk, h, half):
        n = (M_UP if up else M_DOWN).index((kk, h))
        side = 0 if up else 1
        for copy in m_copies(up, kk, h, half, ro.at[side, n], rl.at[side, n]):
            copy.wait_recv()
        return side, n

    def m_send(up, kk, h, half):
        table = M_UP if up else M_DOWN
        dest = zi(kk if up else -kk)
        if (kk + 1, h) not in table:
            for copy in m_copies(up, kk, h, half, cos[h].at[dest], cls[h].at[dest]):
                start(copy)
            return
        side, prev = m_arrived(up, kk + 1, h, half)
        n = table.index((kk, h))
        for i in range(half * HALF, (half + 1) * HALF):
            val, l = merged(cos[h][dest, i], cls[h][dest, i], ro[side, prev, i], rl[side, prev, i])
            mo[side, n, i] = val.astype(jnp.bfloat16)
            ml[side, n, i] = l
        for copy in m_copies(up, kk, h, half, mo.at[side, n], ml.at[side, n]):
            start(copy)

    def m_step(kk, h):
        for half in (0, 1):
            for up in (True, False):
                m_send(up, kk, h, half)

    def m_begin(h):
        for half in (0, 1):
            for up in (True, False):
                longest = (4, h) in (M_UP if up else M_DOWN)
                m_send(up, 4 if longest else 3, h, half)

    def m_second(h):
        for half in (0, 1):
            for up in (True, False):
                if (4, h) in (M_UP if up else M_DOWN):
                    m_send(up, 3, h, half)

    def final(h, r, d):
        return pltpu.make_async_remote_copy(
            src_ref=fin.at[h, r],
            dst_ref=out.at[:, x, :, h * DH : (h + 1) * DH],
            send_sem=sx.at[h, r],
            recv_sem=rx.at[h, d],
            device_id=(r * NZ + z, hd),
            device_id_type=MESH,
        )

    rows = NS // 2

    def m_end(h):
        for i in range(NS):
            if i % HALF == 0:
                su, nu = m_arrived(True, 1, h, i // HALF)
                sd, nd = m_arrived(False, 1, h, i // HALF)
            a, la = merged(ro[su, nu, i], rl[su, nu, i], ro[sd, nd, i], rl[sd, nd, i])
            val, _ = merged(cos[h][z, i], cls[h][z, i], a, la)
            fin[h, i // 2, i % 2] = val.T.astype(jnp.bfloat16)
            if i % 2 == 1:
                leave(h, i // 2)

    def leave(h, r):
        @pl.when(x == r)
        def _():
            for u in range(2):
                out[u, x, :, h * DH : (h + 1) * DH] = fin[h, r, u]

        for d in (1, 2, 3):

            @pl.when(lax.rem(x + d, NX) == r)
            def _(d=d):
                final(h, r, d).start()

    @pl.when(x >= rows)
    def _():
        out[...] = jnp.zeros(out.shape, out.dtype)

    res[W_ALL] = jnp.zeros((DH, B), jnp.float32)
    rel[W_ALL, 0:1] = jnp.full((1, B), neg_big, jnp.float32)
    rel[W_ALL, 1:2] = jnp.ones((1, B), jnp.float32)
    st_o[...] = jnp.zeros((DH, B), jnp.float32)
    st_m[...] = jnp.full((1, B), neg_big, jnp.float32)
    st_l[...] = jnp.zeros((1, B), jnp.float32)

    gathers[0].forward()
    gathers[1].own()
    q_ready(0)
    q_begin(0)
    q_ready(1)
    q_begin(1)
    q_leave(2)
    q_leave(3)
    q_step(1, 0)
    prepare(2)
    q_step(1, 1)
    prepare(3)
    q_step(2, 0)
    gathers[1].forward()
    gathers[2].own()
    q_step(2, 1)
    q_step(3, 0)
    q_ready(2)
    q_step(3, 1)
    q_begin(2)
    q_ready(3)
    q_begin(3)
    q_step(4, 0)
    gathers[0].finish()
    chunk(0, 0)
    q_step(4, 1)
    q_step(1, 2)
    chunk(0, 1)
    gathers[2].forward()
    gathers[3].own()
    q_step(1, 3)
    chunk(0, 2)
    q_step(2, 2)
    chunk(0, 3)
    collect(0)
    m_begin(0)
    gathers[1].finish()
    q_step(2, 3)
    chunk(1, 0)
    q_step(3, 2)
    m_second(0)
    gathers[3].forward()
    chunk(1, 1)
    q_step(3, 3)
    m_step(2, 0)
    chunk(1, 2)
    q_step(4, 2)
    chunk(1, 3)
    collect(1)
    m_begin(1)
    q_step(4, 3)
    m_step(1, 0)
    gathers[2].finish()
    chunk(2, 0)
    m_second(1)
    chunk(2, 1)
    m_end(0)
    m_step(2, 1)
    chunk(2, 2)
    chunk(2, 3)
    collect(2)
    m_begin(2)
    gathers[3].finish()
    chunk(3, 0)
    chunk(3, 1)
    m_step(1, 1)
    m_second(2)
    chunk(3, 2)
    chunk(3, 3)
    collect(3)
    m_begin(3)
    m_step(2, 2)
    m_end(1)
    m_second(3)
    m_step(1, 2)
    m_step(2, 3)
    m_end(2)
    m_step(1, 3)
    m_end(3)

    for h in range(HD):
        for r in range(rows):

            @pl.when(x == r)
            def _(h=h, r=r):
                for d in (1, 2, 3):
                    src = lax.rem(x - d + NX, NX)
                    pltpu.make_async_remote_copy(
                        src_ref=fin.at[h, r],
                        dst_ref=out.at[:, src, :, h * DH : (h + 1) * DH],
                        send_sem=sx.at[h, r],
                        recv_sem=rx.at[h, d],
                        device_id=at_x(d),
                        device_id_type=MESH,
                    ).wait_recv()

            for d in (1, 2, 3):

                @pl.when(lax.rem(x + d, NX) == r)
                def _(h=h, r=r, d=d):
                    final(h, r, d).wait_send()

    for g in gathers:
        g.close()
    for copy in sent:
        copy.wait_send()


def main_step(turn, row, q, k, v):
    dma = pltpu.SemaphoreType.DMA
    any_spec = pl.BlockSpec(memory_space=pl.ANY)
    bf, f32 = jnp.bfloat16, jnp.float32
    i32 = jnp.int32
    out, info = pl.pallas_call(
        main_kernel,
        out_shape=[
            jax.ShapeDtypeStruct((2, NX, B, HD * DH), bf),
            jax.ShapeDtypeStruct((8, 128), i32),
        ],
        in_specs=[SMEM_SPEC, VMEM_SPEC] + [any_spec] * 3,
        out_specs=[VMEM_SPEC] * 2,
        scratch_shapes=[pltpu.VMEM((NX, 2, BD, B, DH), bf)] * HD
        + [pltpu.VMEM((NX, 2, B, DH), bf)] * HD
        + [pltpu.VMEM((NZ, TQ, B, DH), bf)] * HD
        + [pltpu.VMEM((NZ, NS, DH, B), bf)] * HD
        + [pltpu.VMEM((NZ, NS, 1, B), f32)] * HD
        + [
            pltpu.VMEM((BD, B, HD * DH), bf),
            pltpu.VMEM((BD * B, HD * DH), bf),
            pltpu.VMEM((BD * B, HD * DH), bf),
            pltpu.VMEM((NX, HD, 2, B, DH), bf),
            pltpu.VMEM((UN, B, B), f32),
            pltpu.VMEM((W_ALL + 1, DH, B), f32),
            pltpu.VMEM((W_ALL + 1, 2, B), f32),
            pltpu.VMEM((DH, B), f32),
            pltpu.VMEM((1, B), f32),
            pltpu.VMEM((1, B), f32),
            pltpu.VMEM((2, 14, NS, DH, B), bf),
            pltpu.VMEM((2, 14, NS, 1, B), f32),
            pltpu.VMEM((2, 14, NS, DH, B), bf),
            pltpu.VMEM((2, 14, NS, 1, B), f32),
            pltpu.VMEM((HD, NS // 2, 2, B, DH), bf),
            pltpu.VMEM((NX * NZ, 1, 128), i32),
            pltpu.VMEM((NX * NZ, 128), i32),
            pltpu.VMEM((32, 128), i32),
            pltpu.VMEM((8, 256), i32),
            pltpu.SMEM((NX * NZ, 128), i32),
            pltpu.SMEM((32, 128), i32),
            pltpu.SMEM((8, 256), i32),
        ]
        + [
            dma((6,)), dma((NX * NZ,)), dma((NX * NZ,)),
            dma((4, HD)), dma((4, HD)),
            dma((HD, 2, 2)), dma((HD, 2, 2)), dma((HD, 2, 2)), dma((HD, 2, 2)),
            dma((2, 14)), dma((2, 14)),
            dma((2, 2, 2, 14)), dma((2, 2, 2, 14)),
            dma((HD, NS // 2)), dma((HD, 4)),
        ],
        compiler_params=params(0, 58),
        name="main",
    )(turn, row, q, k, v)
    return out.reshape(BD * B, HD * DH), info[0, 0], info[1, 0]


def plan_kernel(tab, send_idx, items, counts, blk, slot):
    s, x, z, _ = place()
    blk_dev = BD
    n_blocks = NX * NZ * BD

    def one(i, carry):
        rank, used, start = carry
        home = i // blk_dev
        k = tab[home, 0, HD * blk_dev * R + lax.rem(i, blk_dev)]
        used = jnp.where(lax.rem(i, blk_dev) == 0, 0, used)
        start = jnp.where(i == s * blk_dev, rank, start)
        mine = (k > 0) & (lax.rem(rank, NX) == x)
        at = jnp.where(mine, rank // NX, 64)
        blk[at] = i
        slot[at] = lax.rem(home, NZ) * 8 + (home // NZ) * 2 + used
        return rank + k, used + jnp.where(mine, 1, 0), start

    total, _, start = lax.fori_loop(0, n_blocks, one, (0, 0, 0))

    for c in range(8):
        send_idx[c] = 0
    filled = [jnp.int32(0)] * NX
    rank = start
    for j in range(blk_dev):
        k = tab[s, 0, HD * blk_dev * R + j]
        col = lax.rem(rank, NX)
        at = jnp.int32(8)
        for c in range(NX):
            hit = (k > 0) & (col == c)
            at = jnp.where(hit, c * 2 + filled[c], at)
            filled[c] = filled[c] + jnp.where(hit, 1, 0)
        send_idx[at] = j
        rank = rank + k

    def query(a, cnt):
        i = blk[a]
        home = i // blk_dev
        base = lax.rem(i, blk_dev) * R
        pos = (lax.rem(a // 2, NZ)) * 8 + (a // 16) * 2 + lax.rem(a, 2)
        word = slot[a] * 64 + pos
        cnt = list(cnt)

        def add(h, t, ok):
            w = ((t // 64) * 8 + lax.rem(t, blk_dev)) * 4096 + word
            items[h * LCAP + cnt[h]] = w
            cnt[h] = cnt[h] + jnp.where(ok, 1, 0)

        for dt in (-1, 0, 1):
            t = i + dt
            ok = (t >= 0) & (t < n_blocks) & (lax.rem(t // blk_dev, NZ) == z)
            t = jnp.clip(t, 0, n_blocks - 1)
            for h in range(HD):
                add(h, t, ok)
        for g in range(G):
            for h in range(HD):
                add(h, jnp.int32(g), z == 0)
        for h in range(HD):
            for r in range(R):
                t = tab[home, 0, h * blk_dev * R + base + r]
                add(h, t, lax.rem(t // blk_dev, NZ) == z)
        return tuple(cnt)

    n_mine = (total - x + NX - 1) // NX
    cnt = lax.fori_loop(0, n_mine, query, (jnp.int32(0),) * HD)
    for h in range(HD):
        counts[h] = cnt[h]
        for u in range(4):
            items[h * LCAP + cnt[h] + u] = jnp.int32(64)


def planned(tab):
    return pl.pallas_call(
        plan_kernel,
        out_shape=[
            jax.ShapeDtypeStruct((16,), jnp.int32),
            jax.ShapeDtypeStruct((HD * LCAP,), jnp.int32),
            jax.ShapeDtypeStruct((8,), jnp.int32),
        ],
        in_specs=[SMEM_SPEC],
        out_specs=[SMEM_SPEC] * 3,
        scratch_shapes=[pltpu.SMEM((72,), jnp.int32), pltpu.SMEM((72,), jnp.int32)],
        compiler_params=params(None, 16),
        name="plan",
    )(tab)


RING = [(k, h) for k in (1, 2, 3) for h in range(HD)]
RING_UP = RING + [(4, 0), (4, 1)]
RING_DOWN = RING + [(4, 2), (4, 3)]


def spread_kernel(idx, q, k, v, kv, qz, qs, sx, rx, so, ro, sf, rf, su, ru, sd, rd):
    s, x, z, hd = place()

    def at_x(d):
        return (lax.rem(x + d, NX) * NZ + z, hd)

    def at_z(d):
        return (x * NZ + lax.rem(z + d + NZ, NZ), hd)

    def xi(d):
        return lax.rem(x + d + NX, NX)

    def zi(d):
        return lax.rem(z + d + NZ, NZ)

    barrier = pltpu.get_barrier_semaphore()
    for d in (1, 2, 3):
        pl.semaphore_signal(barrier, inc=1, device_id=at_x(d), device_id_type=MESH)
    for d in (1, -1):
        pl.semaphore_signal(barrier, inc=1, device_id=at_z(d), device_id_type=MESH)

    def fill(c, carry):
        col, u = c // 2, lax.rem(c, 2)
        j = idx[c]
        for h in range(HD):
            qs[col, h, u] = q[j, :, h * DH : (h + 1) * DH]
        return carry

    lax.fori_loop(0, 8, fill, 0)
    for h in range(HD):
        for u in range(2):
            qz[h, z, x, u] = qs[x, h, u]
    pl.semaphore_wait(barrier, 5)

    q_out = []
    for d in (1, 2, 3):
        copy = pltpu.make_async_remote_copy(
            src_ref=qs.at[xi(d)],
            dst_ref=qz.at[:, z, x],
            send_sem=sx.at[d],
            recv_sem=rx.at[d],
            device_id=at_x(d),
            device_id_type=MESH,
        )
        copy.start()
        q_out.append(copy)

    own = []
    for h in range(HD):

        def prep(b, carry):
            rows = pl.ds(pl.multiple_of(b * B, B), B)
            kv[h, x, 0, b] = k[rows, h * DH : (h + 1) * DH]
            kv[h, x, 1, b] = v[rows, h * DH : (h + 1) * DH].T
            return carry

        lax.fori_loop(0, BD, prep, 0)
        for side, d in ((0, 1), (1, 3)):
            copy = pltpu.make_async_remote_copy(
                src_ref=kv.at[h, x],
                dst_ref=kv.at[h, x],
                send_sem=so.at[side, h],
                recv_sem=ro.at[side, h],
                device_id=at_x(d),
                device_id_type=MESH,
            )
            copy.start()
            own.append(copy)

    for d in (1, 2, 3):
        src = xi(-d)
        pltpu.make_async_remote_copy(
            src_ref=qz.at[:, z, src],
            dst_ref=qz.at[:, z, src],
            send_sem=sx.at[d],
            recv_sem=rx.at[d],
            device_id=at_x(d),
            device_id_type=MESH,
        ).wait_recv()

    rings = []

    def ring_piece(up, n):
        kk, h = (RING_UP if up else RING_DOWN)[n]
        step = -1 if up else 1
        row = zi(step * (kk - 1))
        return pltpu.make_async_remote_copy(
            src_ref=qz.at[h, row],
            dst_ref=qz.at[h, row],
            send_sem=(su if up else sd).at[n],
            recv_sem=(ru if up else rd).at[n],
            device_id=at_z(1 if up else -1),
            device_id_type=MESH,
        )

    def ring_arrival(up, n):
        kk, h = (RING_UP if up else RING_DOWN)[n]
        row = zi((-1 if up else 1) * kk)
        return pltpu.make_async_remote_copy(
            src_ref=qz.at[h, row],
            dst_ref=qz.at[h, row],
            send_sem=(su if up else sd).at[n],
            recv_sem=(ru if up else rd).at[n],
            device_id=at_z(1 if up else -1),
            device_id_type=MESH,
        )

    for n in range(4):
        for up in (True, False):
            copy = ring_piece(up, n)
            copy.start()
            rings.append(copy)

    fwd = []

    def forward_x(h):
        for side, d, part in ((0, 1, 0), (1, 3, 1)):
            src = xi(-d)
            pltpu.make_async_remote_copy(
                src_ref=kv.at[h, src],
                dst_ref=kv.at[h, src],
                send_sem=so.at[side, h],
                recv_sem=ro.at[side, h],
                device_id=at_x(d),
                device_id_type=MESH,
            ).wait_recv()
            copy = pltpu.make_async_remote_copy(
                src_ref=kv.at[h, src, part],
                dst_ref=kv.at[h, src, part],
                send_sem=sf.at[side, h],
                recv_sem=rf.at[side, h],
                device_id=at_x(d),
                device_id_type=MESH,
            )
            copy.start()
            fwd.append(copy)

    for n in range(14):
        for up in (True, False):
            kk, h = (RING_UP if up else RING_DOWN)[n]
            ring_arrival(up, n).wait_recv()
            table = RING_UP if up else RING_DOWN
            if (kk + 1, h) in table:
                copy = ring_piece(up, table.index((kk + 1, h)))
                copy.start()
                rings.append(copy)
        if n % 2 == 1 and n // 2 < HD:
            forward_x(n // 2)

    far = xi(2)
    for h in range(HD):
        for side, d, part in ((0, 1, 0), (1, 3, 1)):
            pltpu.make_async_remote_copy(
                src_ref=kv.at[h, far, part],
                dst_ref=kv.at[h, far, part],
                send_sem=sf.at[side, h],
                recv_sem=rf.at[side, h],
                device_id=at_x(d),
                device_id_type=MESH,
            ).wait_recv()
    for copy in q_out + own + rings + fwd:
        copy.wait_send()


def spread_all(idx, q, k, v):
    dma = pltpu.SemaphoreType.DMA
    return pl.pallas_call(
        spread_kernel,
        out_shape=[
            jax.ShapeDtypeStruct((HD, NX, 2, BD, B, DH), jnp.bfloat16),
            jax.ShapeDtypeStruct((HD, NZ, NX, 2, B, DH), jnp.bfloat16),
        ],
        in_specs=[SMEM_SPEC] + [VMEM_SPEC] * 3,
        out_specs=[VMEM_SPEC] * 2,
        scratch_shapes=[
            pltpu.VMEM((NX, HD, 2, B, DH), jnp.bfloat16),
            dma((4,)),
            dma((4,)),
            dma((2, HD)),
            dma((2, HD)),
            dma((2, HD)),
            dma((2, HD)),
            dma((14,)),
            dma((14,)),
            dma((14,)),
            dma((14,)),
        ],
        compiler_params=params(2),
        name="spread",
    )(idx, q, k, v)


UNROLL = 4


def part_kernel(ns, items, counts, kv, qz, out, lse, acc, top, den):
    h = pl.program_id(0)
    n_acc = NZ * ns

    def clear(a, carry):
        acc[a] = jnp.zeros((DH, B), jnp.float32)
        top[a] = jnp.full((1, B), neg_big, jnp.float32)
        den[a] = jnp.zeros((1, B), jnp.float32)
        return carry

    lax.fori_loop(0, n_acc + 1, clear, 0)

    def batch(n, carry):
        found = []
        for u in range(UNROLL):
            w = items[h * LCAP + n * UNROLL + u]
            pos = lax.rem(w, 64)
            a = (pos // 8) * ns + lax.rem(pos, 8)
            a = jnp.where(n * UNROLL + u < counts[h], a, n_acc)
            spot = lax.rem(w // 64, 64)
            tile = w // 4096
            keys = kv[0, tile // 8, 0, lax.rem(tile, 8)]
            vals = kv[0, tile // 8, 1, lax.rem(tile, 8)]
            qt = qz[0, spot // 8, lax.rem(spot, 8) // 2, lax.rem(spot, 2)]
            scores = lax.dot_general(
                keys, qt, (((1,), (1,)), ((), ())), preferred_element_type=jnp.float32
            )
            scores = scores * score_scale
            m = jnp.max(scores, axis=0, keepdims=True)
            p = jnp.exp(scores - m).astype(jnp.bfloat16)
            l = jnp.sum(p.astype(jnp.float32), axis=0, keepdims=True)
            o = jnp.dot(vals, p, preferred_element_type=jnp.float32)
            found.append((a, m, l, o))
        for a, m, l, o in found:
            old = top[a]
            new = jnp.maximum(old, m)
            f0, f1 = jnp.exp(old - new), jnp.exp(m - new)
            acc[a] = acc[a] * f0 + o * f1
            den[a] = den[a] * f0 + l * f1
            top[a] = new
        return carry

    lax.fori_loop(0, (counts[h] + UNROLL - 1) // UNROLL, batch, 0)

    def finish(a, carry):
        l = den[a]
        some = l > 0
        safe = jnp.where(some, l, 1.0)
        out[0, a // ns, lax.rem(a, ns)] = (acc[a] / safe).astype(jnp.bfloat16)
        lse[0, a // ns, lax.rem(a, ns)] = jnp.where(some, top[a] + jnp.log(safe), neg_big)
        return carry

    lax.fori_loop(0, n_acc, finish, 0)


def parts_of(ns, items, counts, kv, qz):
    n_acc = NZ * ns
    return pl.pallas_call(
        functools.partial(part_kernel, ns),
        grid=(HD,),
        out_shape=[
            jax.ShapeDtypeStruct((HD, NZ, ns, DH, B), jnp.bfloat16),
            jax.ShapeDtypeStruct((HD, NZ, ns, 1, B), jnp.float32),
        ],
        in_specs=[
            SMEM_SPEC,
            SMEM_SPEC,
            pl.BlockSpec((1, NX, 2, BD, B, DH), lambda h: (h, 0, 0, 0, 0, 0)),
            pl.BlockSpec((1, NZ, NX, 2, B, DH), lambda h: (h, 0, 0, 0, 0, 0)),
        ],
        out_specs=[
            pl.BlockSpec((1, NZ, ns, DH, B), lambda h: (h, 0, 0, 0, 0)),
            pl.BlockSpec((1, NZ, ns, 1, B), lambda h: (h, 0, 0, 0, 0)),
        ],
        scratch_shapes=[
            pltpu.VMEM((n_acc + 1, DH, B), jnp.float32),
            pltpu.VMEM((n_acc + 1, 1, B), jnp.float32),
            pltpu.VMEM((n_acc + 1, 1, B), jnp.float32),
        ],
        compiler_params=params(None, 40),
        name="parts",
    )(items, counts, kv, qz)


HOME_UP = [(4, 2), (4, 3)] + [(k, h) for k in (3, 2, 1) for h in range(HD)]
HOME_DOWN = [(4, 0), (4, 1)] + [(k, h) for k in (3, 2, 1) for h in range(HD)]


def merged(o0, l0, o1, l1):
    top = jnp.maximum(l0, l1)
    f0, f1 = jnp.exp(l0 - top), jnp.exp(l1 - top)
    both = f0 + f1
    o = (o0.astype(jnp.float32) * f0 + o1.astype(jnp.float32) * f1) / both
    return o, top + jnp.log(both)


def join_kernel(
    ns, o, lse, out, sou, slu, rou, rlu, sod, sld, rod, rld, fin, ssu, rsu, ssd, rsd, sx, rx
):
    s, x, z, hd = place()

    def at_x(d):
        return (lax.rem(x + d, NX) * NZ + z, hd)

    def at_z(d):
        return (x * NZ + lax.rem(z + d + NZ, NZ), hd)

    def zi(d):
        return lax.rem(z + d + NZ, NZ)

    barrier = pltpu.get_barrier_semaphore()
    for d in (1, 2, 3):
        pl.semaphore_signal(barrier, inc=1, device_id=at_x(d), device_id_type=MESH)
    for d in (1, -1):
        pl.semaphore_signal(barrier, inc=1, device_id=at_z(d), device_id_type=MESH)
    pl.semaphore_wait(barrier, 5)

    sent = []

    def copies(up, n, src_o, src_l):
        ro, rl = (rou, rlu) if up else (rod, rld)
        ss, rs = (ssu, rsu) if up else (ssd, rsd)
        return [
            pltpu.make_async_remote_copy(
                src_ref=src,
                dst_ref=dst.at[n],
                send_sem=ss.at[i, n],
                recv_sem=rs.at[i, n],
                device_id=at_z(1 if up else -1),
                device_id_type=MESH,
            )
            for i, (src, dst) in enumerate(((src_o, ro), (src_l, rl)))
        ]

    def send(up, n, src_o, src_l):
        for copy in copies(up, n, src_o, src_l):
            copy.start()
            sent.append(copy)

    def arrived(up, n):
        ro, rl = (rou, rlu) if up else (rod, rld)
        for copy in copies(up, n, ro.at[n], rl.at[n]):
            copy.wait_recv()

    for n in range(14):
        for up in (True, False):
            table = HOME_UP if up else HOME_DOWN
            kk, h = table[n]
            dest = zi(kk if up else -kk)
            if (kk + 1, h) not in table:
                send(up, n, o.at[h, dest], lse.at[h, dest])
                continue
            prev = table.index((kk + 1, h))
            arrived(up, prev)
            ro, rl = (rou, rlu) if up else (rod, rld)
            so, sl = (sou, slu) if up else (sod, sld)

            def step(i, carry, ro=ro, rl=rl, so=so, sl=sl, prev=prev, n=n, h=h, dest=dest):
                val, l = merged(o[h, dest, i], lse[h, dest, i], ro[prev, i], rl[prev, i])
                so[n, i] = val.astype(jnp.bfloat16)
                sl[n, i] = l
                return carry

            lax.fori_loop(0, ns, step, 0)
            send(up, n, so.at[n], sl.at[n])

    for h in range(HD):
        n = 10 + h
        arrived(True, n)
        arrived(False, n)

        def last(i, carry, h=h, n=n):
            a, la = merged(rou[n, i], rlu[n, i], rod[n, i], rld[n, i])
            val, _ = merged(o[h, z, i], lse[h, z, i], a, la)
            fin[i // 2, lax.rem(i, 2), :, h * DH : (h + 1) * DH] = val.T.astype(jnp.bfloat16)
            return carry

        lax.fori_loop(0, ns, last, 0)

    rows = ns // 2
    for r in range(NX):
        if r >= rows:

            @pl.when(x == r)
            def _():
                out[...] = jnp.zeros(out.shape, out.dtype)

            continue

        @pl.when(x == r)
        def _(r=r):
            out[:, x] = fin[r]

    def final(r, d):
        return pltpu.make_async_remote_copy(
            src_ref=fin.at[r],
            dst_ref=out.at[:, x],
            send_sem=sx.at[r],
            recv_sem=rx.at[d],
            device_id=(r * NZ + z, hd),
            device_id_type=MESH,
        )

    for d in (1, 2, 3):
        for r in range(rows):

            @pl.when(lax.rem(x + d, NX) == r)
            def _(r=r, d=d):
                final(r, d).start()

    for r in range(rows):

        @pl.when(x == r)
        def _(r=r):
            for d in (1, 2, 3):
                src = lax.rem(x - d + NX, NX)
                pltpu.make_async_remote_copy(
                    src_ref=fin.at[r],
                    dst_ref=out.at[:, src],
                    send_sem=sx.at[r],
                    recv_sem=rx.at[d],
                    device_id=at_x(d),
                    device_id_type=MESH,
                ).wait_recv()

    for d in (1, 2, 3):
        for r in range(rows):

            @pl.when(lax.rem(x + d, NX) == r)
            def _(r=r, d=d):
                final(r, d).wait_send()

    for copy in sent:
        copy.wait_send()


def joined(ns, o, lse):
    dma = pltpu.SemaphoreType.DMA
    piece_o = pltpu.VMEM((14, ns, DH, B), jnp.bfloat16)
    piece_l = pltpu.VMEM((14, ns, 1, B), jnp.float32)
    out = pl.pallas_call(
        functools.partial(join_kernel, ns),
        out_shape=jax.ShapeDtypeStruct((2, NX, B, HD * DH), jnp.bfloat16),
        in_specs=[VMEM_SPEC] * 2,
        out_specs=VMEM_SPEC,
        scratch_shapes=[
            piece_o, piece_l, piece_o, piece_l, piece_o, piece_l, piece_o, piece_l,
            pltpu.VMEM((ns // 2, 2, B, HD * DH), jnp.bfloat16),
            dma((2, 14)), dma((2, 14)), dma((2, 14)), dma((2, 14)),
            dma((4,)), dma((4,)),
        ],
        compiler_params=params(3, 56),
        name="join%d" % ns,
    )(o, lse)
    return out.reshape(BD * B, HD * DH)


def body(queries, keys, values, random_holder, random_offset, keep):
    want = random_holder * BD + random_offset
    row = jnp.concatenate([want.reshape(-1), keep, jnp.zeros((24,), jnp.int32)]).reshape(1, 128)
    q = queries.reshape(BD, B, HD * DH)
    out, total, most = main_step(jnp.zeros((2,), jnp.int32), row, q, keys, values)
    parts = (most + TQ - 1) // TQ
    passes = (total + STEP - 1) // STEP * parts

    def more(out):
        def again(state):
            n, out = state
            turn = jnp.stack([n // parts, n % parts])
            new = main_step(turn, row, q, keys, values)[0]
            pairs = [(i, i + 2 * NZ) for i in range(2 * NZ)]
            new = jnp.where(turn[0] > 0, lax.ppermute(new, "seq", pairs), new)
            return n + 1, out + new

        return lax.while_loop(lambda state: state[0] < passes, again, (jnp.int32(1), out))[1]

    return lax.cond(passes > 1, more, lambda out: out, out)


def solution(mesh):
    in_specs = (
        P("seq", "head"),
        P("seq", "head"),
        P("seq", "head"),
        P("head", "seq", None),
        P("head", "seq", None),
        P("seq"),
    )
    out_specs = P("seq", "head")
    return jax.shard_map(body, mesh=mesh, in_specs=in_specs, out_specs=out_specs, check_vma=False)
```
